256 devices in a mesh: sub: 64 (over z, y, core), panel: 4 (over x).
Axes of the slice: x: 4, y: 4, z: 8, core: 2. Of those that a mesh axis runs over, the one named last changes fastest.
Arguments:
- interior_factor: float32 [512, 512, 512], P('sub'), may hold values from -1 to 3, as said below
- coupling: bfloat16 [512, 512, 2048], P('sub', None, 'panel'), may hold values from -1 to 1
- interface_diag: float32 [65536], P(('sub', 'panel')), may hold values from 0.5 to 4
- interface_column: float32 [65536, 128], P(('sub', 'panel')), may hold values from -1.8 to 1.8
- block_map: int32 [512, 16], replicated, may hold values from 0 to 511, as said below
- pair_pattern: int32 [512, 8], P('sub'), may hold values 0 or 1
Outputs:
- assembled: float32 [65536, 1024], P(('sub', 'panel'))
- factored: float32 [65536, 1024], P(('sub', 'panel'))
The draws below stay inside these ranges and needn't reach their ends.
Inputs may be any that keep to these rules, and one draw needn't show every extreme that they name: Local block a of a subdomain has its owner block_map // 8 and its position block_map % 8 among that owner's blocks, one of the 2 positions from (a // 4) * 2. Blocks a and b of one subdomain with a % 4 == b % 4 have the same owner. The 32 block groups of the subdomains of one index of sub go at most 1 to one owner, and some owner gets exactly 1 of them. `interior_factor`: lower triangular; the diagonal lies between 1 and 3.
All inputs are finite; a program needn't handle non-finite values. No bound on the sum of `pair_pattern` on one device may be relied on, other than what follows from the above.
Results may differ from the reference program's by a relative error of at most 0.0006.
Values may be sent and summed in bfloat16 or wider, within the bound.
A program may use at most 128 MiB of HBM per device.

```python
import math
import jax
import jax.numpy as jnp
from jax import lax

BLK = 128
NS = 2048
NIN = 512
SUB_DEV = 8
OWN = 8
NLOC = 16
GRP = 4
R = 2
RPO = 1
SUBDOMAINS = 512
NBLK = 512
N_SUB = 64
N_PANEL = 4


def draw_interior_factor(key, part):
    key_diag, key_lower = jax.random.split(jax.random.fold_in(key, 7))
    diagonal = jnp.exp(jax.random.uniform(key_diag, (SUBDOMAINS, NIN), jnp.float32, 0.0, math.log(2.0)))
    lower = 1.5 * jnp.clip(jax.random.normal(key_lower, (SUBDOMAINS, NIN, NIN), jnp.float32), -3.5, 3.5)
    strict = jnp.tril(lower, -1) / math.sqrt(NIN)
    return strict + diagonal[:, :, None] * jnp.eye(NIN, dtype=jnp.float32)[None]


def draw_coupling(key, part):
    key_base, key_shift = jax.random.split(jax.random.fold_in(key, 11))
    base = jnp.clip(jax.random.normal(key_base, (SUBDOMAINS, NIN, NS), jnp.float32), -3.0, 3.0)
    shift = 0.25 * jnp.clip(jax.random.normal(key_shift, (SUBDOMAINS, NIN, 1), jnp.float32), -3.0, 3.0)
    return ((base + shift) / math.sqrt(NIN)).astype(jnp.bfloat16)


def draw_block_map(key, part):
    key_rank, key_noise, key_order, key_rows = jax.random.split(jax.random.fold_in(key, 23), 4)
    item_total = N_SUB * RPO
    popularity = jax.random.permutation(key_rank, N_SUB).astype(jnp.int32)
    owner_of_item = jnp.arange(item_total, dtype=jnp.int32) // RPO
    noise = jax.random.randint(key_noise, (N_SUB, item_total), 0, 1024, dtype=jnp.int32)
    score = noise + popularity[owner_of_item][None, :] * (2048 // N_SUB)
    distinct = score * item_total + jnp.arange(item_total, dtype=jnp.int32)[None, :]
    chosen = lax.top_k(distinct, GRP * SUB_DEV)[1].astype(jnp.int32)
    shuffle = jax.vmap(lambda sub_key: jax.random.permutation(sub_key, GRP * SUB_DEV))(jax.random.split(key_order, N_SUB))
    chosen = jnp.take_along_axis(chosen, shuffle.astype(jnp.int32), axis=1)
    owners = owner_of_item[chosen].reshape(SUBDOMAINS, GRP)
    rows = jax.random.randint(key_rows, (SUBDOMAINS, N_PANEL, GRP), 0, R, dtype=jnp.int32)
    panels = jnp.arange(N_PANEL, dtype=jnp.int32)[None, :, None]
    blocks = owners[:, None, :] * OWN + panels * R + rows
    return blocks.reshape(SUBDOMAINS, N_PANEL * GRP)


def set_ends(drawn, key, least, high):
    longest = drawn.shape.index(max(drawn.shape))
    spots = []
    for shift in (0, 1):
        where = [jax.random.randint(jax.random.fold_in(key, axis), (), 0, length) for axis, length in enumerate(drawn.shape)]
        where[longest] = (where[longest] + shift) % drawn.shape[longest]
        spots.append(tuple(where))
    return drawn.at[spots[0]].set(least).at[spots[1]].set(high)


def steps_of(stream_key, extent, pieces, least, high):
    def one(position, shards_of):
        draws = jax.random.uniform(jax.random.fold_in(jax.random.fold_in(stream_key, 6), position), (shards_of,), jnp.float32, least / len(pieces), high / len(pieces))
        return jnp.repeat(jnp.exp(draws), extent[position] // shards_of).reshape((-1,) + (1,) * (len(extent) - position - 1))

    gain = one(*pieces[0])
    for cut in pieces[1:]:
        gain = gain * one(*cut)
    return gain


def scatter_about(key, extent, width, most, pieces=(), kind=jnp.bfloat16):
    drawn = width * jax.random.normal(key, extent, jnp.float32)
    if pieces:
        drawn = drawn * steps_of(key, extent, pieces, -0.22, 0.18)
    return jnp.clip(drawn, -most, most).astype(kind)


def setup_inputs(seed: int = 0) -> dict:
    splits = jax.random.split(jax.random.key(seed), 7)
    interior_factor = draw_interior_factor(jax.random.fold_in(splits[6], 71), 0)
    coupling = draw_coupling(jax.random.fold_in(splits[6], 71), 0)
    interface_diag = jnp.clip(jnp.exp(math.log(4.0) - 2.0794415 * jax.random.uniform(splits[2], (NBLK * BLK,), jnp.float32) ** steps_of(splits[2], (NBLK * BLK,), ((0, 256),), -0.2, 0.2)), 0.5, 4.0)
    interface_column = scatter_about(splits[3], (NBLK * BLK, BLK), 0.3, 1.8, ((0, 256),), jnp.float32)
    block_map = draw_block_map(jax.random.fold_in(splits[6], 71), 0)
    pair_pattern = set_ends((jax.random.randint(splits[5], (SUBDOMAINS, NLOC // 2), 0, 4) < 3).astype(jnp.int32), jax.random.fold_in(splits[5], 1), 0, 1)
    return {"interior_factor": interior_factor, "coupling": coupling, "interface_diag": interface_diag, "interface_column": interface_column, "block_map": block_map, "pair_pattern": pair_pattern}


def local_tiles(factor, couple, pattern):
    solved = lax.linalg.triangular_solve(factor, couple.astype(jnp.float32), left_side=True, lower=True)
    rounded = lax.optimization_barrier(solved.astype(jnp.bfloat16))
    blocks = rounded.astype(jnp.float32).reshape(NIN, NLOC, BLK)
    partner = jnp.roll(blocks, -(NLOC // 2), axis=1)
    diagonal = jnp.einsum('kai,kaj->aij', blocks, blocks)
    cross_tiles = jnp.einsum('kai,kaj->aij', blocks, partner)
    linked = jnp.concatenate([pattern, pattern]).astype(jnp.float32)
    return (diagonal, cross_tiles * linked[:, None, None])

def factor_step(square):
    column = square[:, :BLK]
    pivot = jnp.linalg.cholesky(column[:BLK])
    solved = lax.linalg.triangular_solve(pivot, column.T, left_side=True, lower=True).T
    lower_col = jnp.concatenate([pivot, solved[BLK:]], axis=0)
    update = jnp.dot(lower_col, lower_col.T, precision=lax.Precision.HIGHEST)
    row_ids = jnp.arange(square.shape[0], dtype=jnp.int32)[:, None]
    updated = jnp.where(row_ids < BLK, square, square - update)
    return jnp.concatenate([lower_col, updated[:, BLK:]], axis=1)

def reference(interior_factor, coupling, interface_diag, interface_column, block_map, pair_pattern):

    def add_one(total, items):
        factor, couple, blocks, pattern = items
        diagonal, cross_tiles = local_tiles(factor, couple, pattern)
        partner_blocks = jnp.roll(blocks, -(NLOC // 2))
        total = total.at[blocks, blocks % OWN].add(diagonal)
        total = total.at[blocks, partner_blocks % OWN].add(cross_tiles)
        return (total, None)
    start = jnp.zeros((NBLK, OWN, BLK, BLK), jnp.float32)
    total, unused = lax.scan(add_one, start, (interior_factor, coupling, block_map, pair_pattern))
    diag_values = interface_diag.reshape(NBLK, BLK)
    identity = jnp.eye(BLK, dtype=jnp.float32)
    index = jnp.arange(NBLK, dtype=jnp.int32)
    total = total.at[index, index % OWN].add(diag_values[:, :, None] * identity[None])
    off_pivot = (index % OWN != 0).astype(jnp.float32)
    column_tiles = interface_column.reshape(NBLK, BLK, BLK) * off_pivot[:, None, None]
    total = total.at[:, 0].add(column_tiles)
    assembled = total.transpose(0, 2, 1, 3).reshape(NBLK * BLK, OWN * BLK)
    squares = assembled.reshape(N_SUB, OWN * BLK, OWN * BLK)
    factored = lax.map(factor_step, squares)
    return (assembled, factored.reshape(NBLK * BLK, OWN * BLK))
```

```python
import functools

import jax
import jax.numpy as jnp
from jax import lax
from jax.experimental import pallas as pl
from jax.experimental.pallas import tpu as pltpu
from jax.sharding import PartitionSpec as P

BLK = 128
HALF = BLK // 2
OWN = 8
BASE = 32
EXTRA = 8
F32 = jnp.float32
BF16 = jnp.bfloat16
VMEM = pltpu.VMEM


def split(x):
    hi = x.astype(BF16)
    return hi, (x - hi.astype(F32)).astype(BF16)


def mm(a, b):
    return jnp.dot(a, b, preferred_element_type=F32)


def mm_nt(a, b):
    return lax.dot_general(a, b, (((1,), (1,)), ((), ())), preferred_element_type=F32)


def mm_tn(a, b):
    return lax.dot_general(a, b, (((0,), (0,)), ((), ())), preferred_element_type=F32)


def wide(dot, a, b):
    ah, al = split(a)
    bh, bl = split(b)
    return dot(ah, bh) + (dot(ah, bl) + dot(al, bh))


def iota(shape, axis):
    return lax.broadcasted_iota(jnp.int32, shape, axis)


def base_inverses(f_ref, s_ref, a_ref, x_ref):
    subs, order, _ = f_ref.shape
    tiles = order // BLK
    per_tile = BLK // BASE
    count = subs * order // BASE

    def gather(l, carry):
        for t in range(tiles):
            for q in range(per_tile):
                row = t * BLK + q * BASE
                block = f_ref[l, row : row + BASE, t * BLK : (t + 1) * BLK]
                if q:
                    block = pltpu.roll(block, BLK - q * BASE, 1)
                s_ref[pl.ds(pl.multiple_of(l * order + row, BASE), BASE), :] = block
        return carry

    lax.fori_loop(0, subs, gather, 0)

    def lanes(i, carry):
        a_ref[i] = s_ref[pl.ds(i, count, stride=BASE), :].T[:BASE]
        return carry

    lax.fori_loop(0, BASE, lanes, 0, unroll=4)
    rows = iota((BASE, BLK), 0)
    for i in range(BASE):
        top = 8 * (i // 8 + 1)
        total = jnp.where(rows[:top] == i, 1.0, 0.0).astype(F32)
        parts = [total[8 * g : 8 * g + 8] for g in range(top // 8)]
        for k in range(i):
            factor = a_ref[i, k : k + 1, :]
            for g in range(k // 8 + 1):
                parts[g] = parts[g] - factor * x_ref[k, 8 * g : 8 * g + 8, :]
        scale = 1.0 / a_ref[i, i : i + 1, :]
        for g in range(BASE // 8):
            x_ref[i, 8 * g : 8 * g + 8, :] = (
                parts[g] * scale if g < len(parts) else jnp.zeros((8, BLK), F32)
            )

    def back(i, carry):
        padded = jnp.concatenate([x_ref[i], jnp.zeros((BLK - BASE, BLK), F32)], axis=0)
        s_ref[pl.ds(i, count, stride=BASE), :] = padded.T
        return carry

    lax.fori_loop(0, BASE, back, 0, unroll=4)


def full_inverse(l, f_ref, s_ref):
    order = f_ref.shape[1]
    tiles = order // BLK
    row = iota((BLK, BLK), 0)
    col = iota((BLK, BLK), 1)
    inverse = []
    for t in range(tiles):
        pieces = []
        for q in range(BLK // BASE):
            start = pl.multiple_of(l * order + t * BLK + q * BASE, BASE)
            block = s_ref[pl.ds(start, BASE), :]
            pieces.append(pltpu.roll(block, q * BASE, 1) if q else block)
        inverse.append(jnp.concatenate(pieces, axis=0))
    size = BASE
    while size < BLK:
        below = jnp.logical_and(row // size % 2 == 1, col // size == row // size - 1)
        for t in range(tiles):
            tile = f_ref[l, t * BLK : (t + 1) * BLK, t * BLK : (t + 1) * BLK]
            strip = wide(mm, jnp.where(below, tile, 0.0), inverse[t])
            inverse[t] = inverse[t] - wide(mm, inverse[t], strip)
        size *= 2
    while len(inverse) > 1:
        size = inverse[0].shape[0]
        merged = []
        for t in range(0, len(inverse), 2):
            below = f_ref[l, (t + 1) * size : (t + 2) * size, t * size : (t + 1) * size]
            corner = -wide(mm, inverse[t + 1], wide(mm, below, inverse[t]))
            if len(inverse) > 2:
                merged.append(
                    jnp.concatenate(
                        [
                            jnp.concatenate([inverse[t], jnp.zeros((size, size), F32)], axis=1),
                            jnp.concatenate([corner, inverse[t + 1]], axis=1),
                        ],
                        axis=0,
                    )
                )
            else:
                return inverse[0], corner, inverse[1]
        inverse = merged


def apply_inverse(hi_ref, lo_ref, right):
    half = hi_ref.shape[1] // 2
    top = mm(hi_ref[0, :half, :half], right[:half]) + mm(lo_ref[0, :half, :half], right[:half])
    low = mm(hi_ref[0, half:, :], right) + mm(lo_ref[0, half:, :], right)
    return jnp.concatenate([top.astype(BF16), low.astype(BF16)], axis=0)


def solve_kernel(slot_ref, upper_ref, f_ref, c_ref, hi_ref, lo_ref, w_ref, d_ref, s_ref, a_ref, x_ref):
    l = pl.program_id(0)
    order = f_ref.shape[1]
    half = order // 2
    groups = c_ref.shape[2] // BLK

    @pl.when(l == 0)
    def _():
        d_ref[...] = jnp.zeros_like(d_ref)
        base_inverses(f_ref, s_ref, a_ref, x_ref)

    left, corner, right = full_inverse(l, f_ref, s_ref)
    for part, rows, cols in ((left, 0, 0), (corner, half, 0), (right, half, half)):
        hi, lo = split(part)
        hi_ref[0, rows : rows + half, cols : cols + half] = hi
        lo_ref[0, rows : rows + half, cols : cols + half] = lo
    hi_ref[0, :half, half:] = jnp.zeros((half, half), BF16)
    lo_ref[0, :half, half:] = jnp.zeros((half, half), BF16)
    solved = apply_inverse(hi_ref, lo_ref, c_ref[0])
    width = solved.shape[1] // 2
    w_ref[0] = jnp.where(upper_ref[0] == 0, solved[:, :width], solved[:, width:])
    row = iota((HALF, BLK), 0)
    lane = iota((HALF, BLK), 1)
    from_low = lane - HALF < row
    eye = iota((BLK, BLK), 0) == iota((BLK, BLK), 1)
    extra_row = iota((EXTRA, BLK), 0)
    for r in range(groups):
        block = solved[:, r * BLK : (r + 1) * BLK]
        tile = mm_tn(block, block)
        folded = jnp.where(from_low, tile[HALF:], pltpu.roll(tile[:HALF], HALF, 1))
        diag = jnp.sum(jnp.where(eye, tile, 0.0), axis=0, keepdims=True)
        first = diag.astype(BF16).astype(F32)
        second = (diag - first).astype(BF16).astype(F32)
        third = diag - first - second
        extra = jnp.where(
            extra_row == 0,
            first,
            jnp.where(extra_row == 1, second, jnp.where(extra_row == 2, third, 0.0)),
        )
        slot = slot_ref[l * groups + r]
        d_ref[slot] = jnp.concatenate([folded, extra], axis=0).astype(BF16)


def cross_kernel(pat_ref, upper_ref, hi_ref, lo_ref, c_ref, w_ref, keep_ref, send_ref):
    l = pl.program_id(0)
    upper = upper_ref[0] == 0
    solved = apply_inverse(hi_ref, lo_ref, c_ref[0])
    for r in range(c_ref.shape[2] // BLK):
        own = w_ref[0, :, r * BLK : (r + 1) * BLK]
        other = solved[:, r * BLK : (r + 1) * BLK]
        tile = mm_tn(jnp.where(upper, own, other), jnp.where(upper, other, own))
        tile = tile * pat_ref[l * 2 + r].astype(F32)
        keep_ref[0, r] = jnp.where(upper, tile[:HALF], tile[HALF:]).astype(BF16)
        send_ref[0, r] = jnp.where(upper, tile[HALF:], tile[:HALF]).astype(BF16)


def place_kernel(slot_ref, keep_ref, got_ref, out_ref):
    out_ref[...] = jnp.zeros_like(out_ref)
    count = keep_ref.shape[0]

    def one(i, carry):
        out_ref[slot_ref[i]] = keep_ref[i]
        out_ref[slot_ref[count + i]] = got_ref[i]
        return carry

    lax.fori_loop(0, count, one, 0, unroll=2)


def diag_kernel(index_ref, recv_ref, own_diag_ref, out_ref, acc_ref):
    acc_ref[...] = jnp.zeros_like(acc_ref)

    def one(s, carry):
        i = index_ref[s]
        acc_ref[i] = acc_ref[i] + recv_ref[s].astype(F32)
        return carry

    lax.fori_loop(0, recv_ref.shape[0], one, 0, unroll=4)
    row = iota((HALF, BLK), 0)
    lane = iota((HALF, BLK), 1)
    eye = iota((BLK, BLK), 0) == iota((BLK, BLK), 1)
    for r in range(out_ref.shape[0]):
        folded = acc_ref[r + 1, :HALF, :]
        low = jnp.where(lane - HALF < row, folded, 0.0)
        high = jnp.where(
            jnp.logical_and(lane > row, lane < HALF), pltpu.roll(folded, HALF, 1), 0.0
        )
        strict = jnp.concatenate([high, low], axis=0)
        diag = jnp.sum(acc_ref[r + 1, HALF:, :], axis=0, keepdims=True) + own_diag_ref[r : r + 1, :]
        out_ref[r] = strict + strict.T + jnp.where(eye, diag, 0.0)


def cross_sum_kernel(index_ref, recv_ref, out_ref, acc_ref):
    acc_ref[...] = jnp.zeros_like(acc_ref)

    def one(s, carry):
        i = index_ref[s]
        acc_ref[i] = acc_ref[i] + recv_ref[s].astype(F32)
        return carry

    lax.fori_loop(0, recv_ref.shape[0], one, 0, unroll=4)
    out_ref[...] = acc_ref[1:]


def cholesky_kernel(tile_ref, p_ref, inv_ref, t_ref):
    groups = BLK // 8
    rows = [tile_ref[8 * g : 8 * g + 8, :] for g in range(groups)]
    lane = iota((8, BLK), 1)
    sub = iota((8, BLK), 0)
    lane1 = iota((1, BLK), 1)
    right = [jnp.where(lane == sub + 8 * g, 1.0, 0.0).astype(F32) for g in range(groups)]
    for j in range(BLK):
        g, s = divmod(j, 8)
        pivot_row = rows[g][s : s + 1, :]
        right_row = right[g][s : s + 1, :]
        pivot = jnp.broadcast_to(pivot_row[:, j : j + 1], (1, BLK))
        root = 1.0 / jnp.sqrt(pivot)
        scaled = pivot_row / pivot
        t_ref[j : j + 1, :] = jnp.where(lane1 >= j, pivot_row * root, 0.0)
        inv_ref[j : j + 1, :] = right_row * root
        right_scaled = right_row / pivot
        for h in range(g, groups):
            if h == g and s == 7:
                continue
            column = jnp.broadcast_to(rows[h][:, j : j + 1], (8, BLK))
            if h == g:
                column = jnp.where(sub > s, column, 0.0)
            rows[h] = rows[h] - column * scaled
            right[h] = right[h] - column * right_scaled
    p_ref[...] = t_ref[...].T


def final_kernel(panel_ref, diag_ref, half_ref, icol_ref, first_ref, p_ref, inv_ref, asm_ref, fac_ref, l_ref):
    panel = panel_ref[0]
    lower = panel < 2
    base = panel % 2
    other = (panel + 2) % 4
    asm_ref[...] = jnp.zeros_like(asm_ref)
    for r in range(2):
        at = pl.multiple_of((panel * 2 + r) * BLK, BLK)
        asm_ref[r * BLK : (r + 1) * BLK, pl.ds(at, BLK)] = diag_ref[r]
    for a in range(2):
        for b in range(2):
            whole = jnp.concatenate(
                [half_ref[base, a * 2 + b], half_ref[base + 2, a * 2 + b]], axis=0
            )
            tile = jnp.where(lower, whole, whole.T)
            row = pl.multiple_of(jnp.where(lower, a, b) * BLK, BLK)
            at = pl.multiple_of((other * 2 + jnp.where(lower, b, a)) * BLK, BLK)
            asm_ref[pl.ds(row, BLK), pl.ds(at, BLK)] = tile
    own = pl.multiple_of(panel * 2 * BLK, BLK)
    off = jnp.logical_or(panel > 0, iota((2 * BLK, BLK), 0) >= BLK)
    asm_ref[:, :BLK] = asm_ref[:, :BLK] + jnp.where(off, icol_ref[pl.ds(own, 2 * BLK), :], 0.0)
    inv_hi, inv_lo = split(inv_ref[...])
    l_ref[:BLK, :] = p_ref[...]
    for r in range(1, OWN):
        key = icol_ref[r * BLK : (r + 1) * BLK, :]
        if r in (4, 5):
            key = key + jnp.concatenate([half_ref[0, r - 4], half_ref[2, r - 4]], axis=0).T
        kh, kl = split(key)
        l_ref[r * BLK : (r + 1) * BLK, :] = mm_nt(kh, inv_hi) + (
            mm_nt(kh, inv_lo) + mm_nt(kl, inv_hi)
        )
    mine = l_ref[pl.ds(own, 2 * BLK), :]
    mh, ml = split(mine)
    fac_ref[:, :BLK] = mine
    for c in range(1, OWN):
        lh, ll = split(l_ref[c * BLK : (c + 1) * BLK, :])
        update = mm_nt(mh, lh) + (mm_nt(mh, ll) + mm_nt(ml, lh))
        fac_ref[:, c * BLK : (c + 1) * BLK] = asm_ref[:, c * BLK : (c + 1) * BLK] - jnp.where(
            off, update, 0.0
        )


def cost(flops, nbytes):
    return pl.CostEstimate(flops=flops, bytes_accessed=nbytes, transcendentals=0)


def whole(count):
    return [pl.BlockSpec(memory_space=VMEM)] * count


SMEM = pl.BlockSpec(memory_space=pltpu.SMEM)


def partner(value, panels):
    pairs = [(source, (source + panels // 2) % panels) for source in range(panels)]
    return lax.ppermute(value, "panel", pairs)


def per_device(
    interior_factor, coupling, interface_diag, interface_column, block_map, pair_pattern
):
    subs, order, width = coupling.shape
    owners_total = lax.axis_size("sub")
    panels = lax.axis_size("panel")
    sub = lax.axis_index("sub")
    panel = lax.axis_index("panel")
    upper = (panel >= panels // 2).astype(jnp.int32)
    upper_s = upper.reshape(1)
    panel_s = panel.astype(jnp.int32).reshape(1)
    groups = width // BLK
    half_width = width // 2

    outgoing = lax.dynamic_slice_in_dim(coupling, (1 - upper) * half_width, half_width, 2)
    incoming = partner(outgoing, panels)
    columns = lax.all_gather(interface_column, "panel", axis=0, tiled=True)

    maps = block_map.reshape(owners_total, subs, panels, groups)
    owner = maps[:, :, 0, :] // OWN
    match = (owner == sub).astype(jnp.int32)
    place = maps % 2
    base = panel % 2
    own_place = lax.dynamic_index_in_dim(place, panel, 2, keepdims=False)
    low_place = lax.dynamic_index_in_dim(place, base, 2, keepdims=False)
    high_place = lax.dynamic_index_in_dim(place, base + 2, 2, keepdims=False)
    diag_index = jnp.sum(match * (1 + own_place), axis=(1, 2))
    cross_index = jnp.sum(match * (1 + 2 * low_place + high_place), axis=(1, 2))
    slots = lax.dynamic_index_in_dim(owner, sub, 0, keepdims=False)
    by_half = slots.reshape(subs, 2, 2)
    keep_slots = lax.dynamic_index_in_dim(by_half, upper, 1, keepdims=False).reshape(-1)
    got_slots = lax.dynamic_index_in_dim(by_half, 1 - upper, 1, keepdims=False).reshape(-1)
    pattern = lax.dynamic_slice_in_dim(pair_pattern, base * groups + upper * 2, 2, 1).reshape(-1)

    hi, lo, w_half, diag_send = pl.pallas_call(
        solve_kernel,
        grid=(subs,),
        in_specs=[
            SMEM,
            SMEM,
            pl.BlockSpec((subs, order, order), lambda l: (0, 0, 0)),
            pl.BlockSpec((1, order, width), lambda l: (l, 0, 0)),
        ],
        out_specs=[
            pl.BlockSpec((1, order, order), lambda l: (l, 0, 0)),
            pl.BlockSpec((1, order, order), lambda l: (l, 0, 0)),
            pl.BlockSpec((1, order, half_width), lambda l: (l, 0, 0)),
            pl.BlockSpec((owners_total, HALF + EXTRA, BLK), lambda l: (0, 0, 0)),
        ],
        out_shape=[
            jax.ShapeDtypeStruct((subs, order, order), BF16),
            jax.ShapeDtypeStruct((subs, order, order), BF16),
            jax.ShapeDtypeStruct((subs, order, half_width), BF16),
            jax.ShapeDtypeStruct((owners_total, HALF + EXTRA, BLK), BF16),
        ],
        scratch_shapes=[
            VMEM((subs * order, BLK), F32),
            VMEM((BASE, BASE, BLK), F32),
            VMEM((BASE, BASE, BLK), F32),
        ],
        compiler_params=pltpu.CompilerParams(vmem_limit_bytes=48 * 2**20),
        cost_estimate=cost(2 * 10**10, 2**25),
        name="solve",
    )(slots.reshape(-1), upper_s, interior_factor, coupling)

    diag_got = lax.all_to_all(diag_send, "sub", split_axis=0, concat_axis=0, tiled=True)

    keep, send = pl.pallas_call(
        cross_kernel,
        grid=(subs,),
        in_specs=[
            SMEM,
            SMEM,
            pl.BlockSpec((1, order, order), lambda l: (l, 0, 0)),
            pl.BlockSpec((1, order, order), lambda l: (l, 0, 0)),
            pl.BlockSpec((1, order, half_width), lambda l: (l, 0, 0)),
            pl.BlockSpec((1, order, half_width), lambda l: (l, 0, 0)),
        ],
        out_specs=[pl.BlockSpec((1, 2, HALF, BLK), lambda l: (l, 0, 0, 0))] * 2,
        out_shape=[jax.ShapeDtypeStruct((subs, 2, HALF, BLK), BF16)] * 2,
        cost_estimate=cost(4 * 10**9, 2**24),
        name="cross",
    )(pattern, upper_s, hi, lo, incoming, w_half)
    got = partner(send, panels)

    count = subs * 2
    cross_send = pl.pallas_call(
        place_kernel,
        in_specs=[SMEM] + whole(2),
        out_specs=pl.BlockSpec(memory_space=VMEM),
        out_shape=jax.ShapeDtypeStruct((owners_total, HALF, BLK), BF16),
        cost_estimate=cost(10**9, 2**21),
        name="place",
    )(
        jnp.concatenate([keep_slots, got_slots]),
        keep.reshape(count, HALF, BLK),
        got.reshape(count, HALF, BLK),
    )
    cross_got = lax.all_to_all(cross_send, "sub", split_axis=0, concat_axis=0, tiled=True)

    rows = OWN // panels
    diag_tiles = pl.pallas_call(
        diag_kernel,
        in_specs=[SMEM] + whole(2),
        out_specs=pl.BlockSpec(memory_space=VMEM),
        out_shape=jax.ShapeDtypeStruct((rows, BLK, BLK), F32),
        scratch_shapes=[VMEM((rows + 1, HALF + EXTRA, BLK), F32)],
        cost_estimate=cost(10**9, 2**21),
        name="diag_sum",
    )(diag_index, diag_got, interface_diag.reshape(rows, BLK))
    first = lax.all_gather(diag_tiles[0], "panel", axis=0)[0]
    pivot, pivot_inverse = pl.pallas_call(
        cholesky_kernel,
        in_specs=whole(1),
        out_specs=whole(2),
        out_shape=[jax.ShapeDtypeStruct((BLK, BLK), F32)] * 2,
        scratch_shapes=[VMEM((BLK, BLK), F32)],
        cost_estimate=cost(10**10, 2**18),
        name="pivot",
    )(first)

    halves = pl.pallas_call(
        cross_sum_kernel,
        in_specs=[SMEM] + whole(1),
        out_specs=pl.BlockSpec(memory_space=VMEM),
        out_shape=jax.ShapeDtypeStruct((rows * rows, HALF, BLK), F32),
        scratch_shapes=[VMEM((rows * rows + 1, HALF, BLK), F32)],
        cost_estimate=cost(10**9, 2**21),
        name="cross_sum",
    )(cross_index, cross_got)
    all_halves = lax.all_gather(halves, "panel", axis=0)
    return pl.pallas_call(
        final_kernel,
        in_specs=[SMEM] + whole(6),
        out_specs=whole(2),
        out_shape=[jax.ShapeDtypeStruct((rows * BLK, OWN * BLK), F32)] * 2,
        scratch_shapes=[VMEM((OWN * BLK, BLK), F32)],
        cost_estimate=cost(10**9, 2**22),
        name="final",
    )(panel_s, diag_tiles, all_halves, columns, first, pivot, pivot_inverse)


def solution(mesh):
    return jax.shard_map(
        per_device,
        mesh=mesh,
        in_specs=(
            P("sub", None, None),
            P("sub", None, "panel"),
            P(("sub", "panel")),
            P(("sub", "panel"), None),
            P(),
            P("sub", None),
        ),
        out_specs=(P(("sub", "panel"), None), P(("sub", "panel"), None)),
        check_vma=False,
    )
```

```python
import functools

import jax
import jax.numpy as jnp
from jax import lax
from jax.experimental import pallas as pl
from jax.experimental.pallas import tpu as pltpu
from jax.sharding import PartitionSpec as P

BLK = 128
HALF = BLK // 2
OWN = 8
BASE = 32
EXTRA = 8
EARLY = 5
F32 = jnp.float32
BF16 = jnp.bfloat16
VMEM = pltpu.VMEM


def split(x):
    hi = x.astype(BF16)
    return hi, (x - hi.astype(F32)).astype(BF16)


def mm(a, b):
    return jnp.dot(a, b, preferred_element_type=F32)


def mm_nt(a, b):
    return lax.dot_general(a, b, (((1,), (1,)), ((), ())), preferred_element_type=F32)


def mm_tn(a, b):
    return lax.dot_general(a, b, (((0,), (0,)), ((), ())), preferred_element_type=F32)


def wide(dot, a, b):
    ah, al = split(a)
    bh, bl = split(b)
    return dot(ah, bh) + (dot(ah, bl) + dot(al, bh))


def iota(shape, axis):
    return lax.broadcasted_iota(jnp.int32, shape, axis)


def base_inverses(f_ref, s_ref, a_ref, x_ref):
    subs, order, _ = f_ref.shape
    tiles = order // BLK
    per_tile = BLK // BASE
    count = subs * order // BASE

    def gather(l, carry):
        for t in range(tiles):
            for q in range(per_tile):
                row = t * BLK + q * BASE
                block = f_ref[l, row : row + BASE, t * BLK : (t + 1) * BLK]
                if q:
                    block = pltpu.roll(block, BLK - q * BASE, 1)
                s_ref[pl.ds(pl.multiple_of(l * order + row, BASE), BASE), :] = block
        return carry

    lax.fori_loop(0, subs, gather, 0)

    def lanes(i, carry):
        a_ref[i] = s_ref[pl.ds(i, count, stride=BASE), :].T[:BASE]
        return carry

    lax.fori_loop(0, BASE, lanes, 0, unroll=4)
    rows = iota((BASE, BLK), 0)
    for i in range(BASE):
        top = 8 * (i // 8 + 1)
        total = jnp.where(rows[:top] == i, 1.0, 0.0).astype(F32)
        parts = [total[8 * g : 8 * g + 8] for g in range(top // 8)]
        for k in range(i):
            factor = a_ref[i, k : k + 1, :]
            for g in range(k // 8 + 1):
                parts[g] = parts[g] - factor * x_ref[k, 8 * g : 8 * g + 8, :]
        scale = 1.0 / a_ref[i, i : i + 1, :]
        for g in range(BASE // 8):
            x_ref[i, 8 * g : 8 * g + 8, :] = (
                parts[g] * scale if g < len(parts) else jnp.zeros((8, BLK), F32)
            )

    def back(i, carry):
        padded = jnp.concatenate([x_ref[i], jnp.zeros((BLK - BASE, BLK), F32)], axis=0)
        s_ref[pl.ds(i, count, stride=BASE), :] = padded.T
        return carry

    lax.fori_loop(0, BASE, back, 0, unroll=4)


def full_inverse(l, f_ref, s_ref):
    order = f_ref.shape[1]
    tiles = order // BLK
    row = iota((BLK, BLK), 0)
    col = iota((BLK, BLK), 1)
    inverse = []
    for t in range(tiles):
        pieces = []
        for q in range(BLK // BASE):
            start = pl.multiple_of(l * order + t * BLK + q * BASE, BASE)
            block = s_ref[pl.ds(start, BASE), :]
            pieces.append(pltpu.roll(block, q * BASE, 1) if q else block)
        inverse.append(jnp.concatenate(pieces, axis=0))
    size = BASE
    while size < BLK:
        below = jnp.logical_and(row // size % 2 == 1, col // size == row // size - 1)
        for t in range(tiles):
            tile = f_ref[l, t * BLK : (t + 1) * BLK, t * BLK : (t + 1) * BLK]
            strip = wide(mm, jnp.where(below, tile, 0.0), inverse[t])
            inverse[t] = inverse[t] - wide(mm, inverse[t], strip)
        size *= 2
    while len(inverse) > 1:
        size = inverse[0].shape[0]
        merged = []
        for t in range(0, len(inverse), 2):
            below = f_ref[l, (t + 1) * size : (t + 2) * size, t * size : (t + 1) * size]
            corner = -wide(mm, inverse[t + 1], wide(mm, below, inverse[t]))
            if len(inverse) > 2:
                merged.append(
                    jnp.concatenate(
                        [
                            jnp.concatenate([inverse[t], jnp.zeros((size, size), F32)], axis=1),
                            jnp.concatenate([corner, inverse[t + 1]], axis=1),
                        ],
                        axis=0,
                    )
                )
            else:
                return inverse[0], corner, inverse[1]
        inverse = merged


def apply_inverse(hi, lo, right):
    half = hi.shape[0] // 2
    top = mm(hi[:half, :half], right[:half]) + mm(lo[:half, :half], right[:half])
    low = mm(hi[half:], right) + mm(lo[half:], right)
    return jnp.concatenate([top.astype(BF16), low.astype(BF16)], axis=0)


def solve_kernel(upper_ref, f_ref, c_ref, hi_ref, lo_ref, w_ref, d_ref, s_ref, a_ref, x_ref):
    l = pl.program_id(0)
    order = f_ref.shape[1]
    half = order // 2
    groups = c_ref.shape[2] // BLK

    @pl.when(l == 0)
    def _():
        d_ref[...] = jnp.zeros_like(d_ref)
        base_inverses(f_ref, s_ref, a_ref, x_ref)

    left, corner, right = full_inverse(l, f_ref, s_ref)
    for part, rows, cols in ((left, 0, 0), (corner, half, 0), (right, half, half)):
        hi, lo = split(part)
        hi_ref[0, rows : rows + half, cols : cols + half] = hi
        lo_ref[0, rows : rows + half, cols : cols + half] = lo
    hi_ref[0, :half, half:] = jnp.zeros((half, half), BF16)
    lo_ref[0, :half, half:] = jnp.zeros((half, half), BF16)
    solved = apply_inverse(hi_ref[0], lo_ref[0], c_ref[0])
    width = solved.shape[1] // 2
    w_ref[0] = jnp.where(upper_ref[0] == 0, solved[:, :width], solved[:, width:])
    row = iota((HALF, BLK), 0)
    lane = iota((HALF, BLK), 1)
    from_low = lane - HALF < row
    eye = iota((BLK, BLK), 0) == iota((BLK, BLK), 1)
    extra_row = iota((EXTRA, BLK), 0)
    for r in range(groups):
        block = solved[:, r * BLK : (r + 1) * BLK]
        tile = mm_tn(block, block)
        folded = jnp.where(from_low, tile[HALF:], pltpu.roll(tile[:HALF], HALF, 1))
        diag = jnp.sum(jnp.where(eye, tile, 0.0), axis=0, keepdims=True)
        first = diag.astype(BF16).astype(F32)
        second = (diag - first).astype(BF16).astype(F32)
        third = diag - first - second
        extra = jnp.where(
            extra_row == 0,
            first,
            jnp.where(extra_row == 1, second, jnp.where(extra_row == 2, third, 0.0)),
        )
        d_ref[l * groups + r] = jnp.concatenate([folded, extra], axis=0).astype(BF16)


MESH = pl.DeviceIdType.MESH
SUB_SHAPE = (8, 4, 2)


def sub_peer(step):
    z_total, y_total, cores = SUB_SHAPE
    me = lax.axis_index("sub")
    z, y, core = me // (y_total * cores), (me // cores) % y_total, me % cores
    m = step % z_total
    dz = z_total // 2 + (1 - 2 * (m % 2)) * ((m + 1) // 2)
    rest = step // z_total
    return (
        ((z + dz) % z_total) * y_total + (y + rest // cores) % y_total
    ) * cores + (core + rest) % cores


def all_peers(total, act):
    skip = SUB_SHAPE[0] - 1

    def one(step, carry):
        act(sub_peer(step))
        return carry

    lax.fori_loop(0, skip, one, 0)
    lax.fori_loop(skip + 1, total, one, 0)


def greet(total, panels):
    barrier = pltpu.get_barrier_semaphore()
    panel = lax.axis_index("panel")

    def signal(peer):
        pl.semaphore_signal(barrier, inc=1, device_id={"sub": peer}, device_id_type=MESH)

    all_peers(total, signal)
    for away in range(1, panels):
        pl.semaphore_signal(
            barrier, inc=1, device_id={"panel": (panel + away) % panels}, device_id_type=MESH
        )
    return lambda: pl.semaphore_wait(barrier, total - 1 + panels - 1)


def to_panel(src, dst, send, recv, away):
    panels = lax.axis_size("panel")
    peer = (lax.axis_index("panel") + away) % panels
    return pltpu.make_async_remote_copy(
        src_ref=src,
        dst_ref=dst,
        send_sem=send,
        recv_sem=recv,
        device_id={"panel": peer},
        device_id_type=MESH,
    )


def await_bytes(ref, sem):
    pltpu.make_async_copy(ref, ref, sem).wait()


def scatter_slots(total, src_ref, tiles_ref, send_ref, recv_ref):
    me = lax.axis_index("sub")

    def one(s, carry):
        send_ref[s] = tiles_ref[src_ref[s]]
        return carry

    lax.fori_loop(0, total, one, 0, unroll=2)
    recv_ref[me] = tiles_ref[src_ref[me]]


def start_slots(total, send_ref, recv_ref, send, recv):
    me = lax.axis_index("sub")

    def go(peer):
        pltpu.make_async_remote_copy(
            src_ref=send_ref.at[peer],
            dst_ref=recv_ref.at[me],
            send_sem=send,
            recv_sem=recv,
            device_id={"sub": peer},
            device_id_type=MESH,
        ).start()

    all_peers(total, go)


def cross_products(first, count, pat_ref, hi_ref, lo_ref, c_ref, w_ref, x_ref, out_ref, send, recv):
    panels = lax.axis_size("panel")
    upper = lax.axis_index("panel") // (panels // 2)
    low = upper == 0
    width = c_ref.shape[2] // BLK

    def one(i, carry):
        solved = apply_inverse(hi_ref[i], lo_ref[i], c_ref[i])
        for r in range(width):
            own = w_ref[i, :, r * BLK : (r + 1) * BLK]
            other = solved[:, r * BLK : (r + 1) * BLK]
            tile = mm_tn(jnp.where(low, own, other), jnp.where(low, other, own))
            tile = tile * pat_ref[(first + i) * width + r].astype(F32)
            group = (first + i) * 2 * width + width * upper + r
            x_ref[group] = jnp.where(low, tile[:HALF], tile[HALF:]).astype(BF16)
            out_ref[i * width + r] = jnp.where(low, tile[HALF:], tile[:HALF]).astype(BF16)
            to_panel(
                out_ref.at[i * width + r], x_ref.at[group], send, recv, panels // 2
            ).start()
        return carry

    lax.fori_loop(0, count, one, 0)


def fetch(pairs, sem):
    copies = [pltpu.make_async_copy(src, dst, sem.at[k]) for k, (src, dst) in enumerate(pairs)]
    for copy in copies:
        copy.start()
    return copies


def first_kernel(
    count, src_ref, pat_ref, d_ref, icol_ref, hi_any, lo_any, c_any, w_any,
    got_ref, x_ref, cols_ref,
    dsend_ref, out_ref, hi_ref, lo_ref, c_ref, w_ref, local, slot_send, slot_recv, half_send, half_recv, col_send, col_recv,
):
    total = lax.axis_size("sub")
    panels = lax.axis_size("panel")
    panel = lax.axis_index("panel")
    rows = icol_ref.shape[0]
    ready = greet(total, panels)
    copies = fetch(
        [
            (hi_any.at[pl.ds(0, count)], hi_ref),
            (lo_any.at[pl.ds(0, count)], lo_ref),
            (c_any, c_ref),
            (w_any.at[pl.ds(0, count)], w_ref),
        ],
        local,
    )
    scatter_slots(total, src_ref, d_ref, dsend_ref, got_ref)
    ready()
    start_slots(total, dsend_ref, got_ref, slot_send, slot_recv)
    mine = cols_ref.at[pl.ds(pl.multiple_of(panel * rows, rows), rows)]
    column_copies = [
        to_panel(icol_ref, mine, col_send.at[away - 1], col_recv, away) for away in range(1, panels)
    ]
    for copy in column_copies:
        copy.start()
    cols_ref[pl.ds(pl.multiple_of(panel * rows, rows), rows), :] = icol_ref[...]
    for copy in copies:
        copy.wait()
    cross_products(0, count, pat_ref, hi_ref, lo_ref, c_ref, w_ref, x_ref, out_ref, half_send, half_recv)
    await_bytes(out_ref, half_send)
    await_bytes(out_ref, half_recv)
    for copy in column_copies:
        copy.wait_send()
    await_bytes(cols_ref.at[pl.ds(0, (panels - 1) * rows)], col_recv)
    await_bytes(dsend_ref.at[pl.ds(0, total - 1)], slot_send)
    await_bytes(got_ref.at[pl.ds(0, total - 1)], slot_recv)


def second_kernel(
    done, src_ref, pat_ref, dindex_ref, xindex_ref, dgot_ref, xin_ref, own_diag_ref, hi_any, lo_any, c_any, w_any,
    diag_ref, p_ref, inv_ref, pair_ref, col_ref,
    x_ref, xsend_ref, xgot_ref, out_ref, hi_ref, lo_ref, c_ref, w_ref, first_ref, a_ref, b_ref, t_ref,
    local, slot_send, slot_recv, half_send, half_recv, first_send, first_recv, pair_send, pair_recv, col_send, col_recv,
):
    total = lax.axis_size("sub")
    panels = lax.axis_size("panel")
    panel = lax.axis_index("panel")
    upper = panel // (panels // 2)
    count = c_ref.shape[0]
    ready = greet(total, panels)
    copies = fetch(
        [
            (hi_any.at[pl.ds(done, count)], hi_ref),
            (lo_any.at[pl.ds(done, count)], lo_ref),
            (c_any, c_ref),
            (w_any.at[pl.ds(done, count)], w_ref),
        ],
        local,
    )
    groups = xin_ref.shape[0]
    x_ref[:groups] = xin_ref[...]
    x_ref[x_ref.shape[0] - 1] = jnp.zeros(x_ref.shape[1:], BF16)
    ready()
    for copy in copies:
        copy.wait()
    cross_products(done, count, pat_ref, hi_ref, lo_ref, c_ref, w_ref, x_ref, out_ref, half_send, half_recv)
    await_bytes(out_ref, half_send)
    await_bytes(out_ref, half_recv)
    scatter_slots(total, src_ref, x_ref, xsend_ref, xgot_ref)
    start_slots(total, xsend_ref, xgot_ref, slot_send, slot_recv)

    sum_diagonal(dindex_ref, dgot_ref, own_diag_ref, diag_ref)

    @pl.when(panel == 0)
    def _():
        first_ref[...] = diag_ref[0]
        sends = [
            to_panel(first_ref, first_ref, first_send.at[away - 1], first_recv, away)
            for away in range(1, panels)
        ]
        for copy in sends:
            copy.start()
        for copy in sends:
            copy.wait_send()

    @pl.when(panel != 0)
    def _():
        await_bytes(first_ref, first_recv)

    factor_pivot(first_ref, p_ref, inv_ref, a_ref, b_ref, t_ref)
    await_bytes(xsend_ref.at[pl.ds(0, total - 1)], slot_send)
    await_bytes(xgot_ref.at[pl.ds(0, total - 1)], slot_recv)
    sum_cross(xindex_ref, xgot_ref, pair_ref, upper)
    pair = to_panel(pair_ref.at[upper], pair_ref.at[upper], pair_send, pair_recv, panels // 2)
    pair.start()

    @pl.when(panel % 2 == 0)
    def _():
        key = pair_ref.at[upper, pl.ds(0, 2)]
        sends = [
            to_panel(key, col_ref.at[upper], col_send.at[k], col_recv, away)
            for k, away in enumerate((1, panels - 1))
        ]
        for copy in sends:
            copy.start()
        for copy in sends:
            copy.wait_send()
        pair.wait()
        col_ref[...] = pair_ref[:, :2]

    @pl.when(panel % 2 == 1)
    def _():
        pair.wait()
        await_bytes(col_ref, col_recv)


def sum_diagonal(index_ref, recv_ref, own_diag_ref, out_ref):
    count, height, _ = recv_ref.shape
    places = out_ref.shape[0]

    def one(s, sums):
        value = recv_ref[s].astype(F32)
        at = index_ref[s]
        return tuple(
            total + jnp.where(at == r + 1, value, 0.0) for r, total in enumerate(sums)
        )

    start = tuple(jnp.zeros((height, BLK), F32) for _ in range(places))
    sums = lax.fori_loop(0, count, one, start, unroll=2)
    row = iota((HALF, BLK), 0)
    lane = iota((HALF, BLK), 1)
    eye = iota((BLK, BLK), 0) == iota((BLK, BLK), 1)
    for r in range(places):
        folded = sums[r][:HALF]
        low = jnp.where(lane - HALF < row, folded, 0.0)
        high = jnp.where(
            jnp.logical_and(lane > row, lane < HALF), pltpu.roll(folded, HALF, 1), 0.0
        )
        strict = jnp.concatenate([high, low], axis=0)
        diag = jnp.sum(sums[r][HALF:], axis=0, keepdims=True) + own_diag_ref[r : r + 1, :]
        out_ref[r] = strict + strict.T + jnp.where(eye, diag, 0.0)


def sum_cross(index_ref, recv_ref, out_ref, slot):
    count = recv_ref.shape[0]
    places = out_ref.shape[1]

    def one(s, sums):
        value = recv_ref[s].astype(F32)
        at = index_ref[s]
        return tuple(
            total + jnp.where(at == r + 1, value, 0.0) for r, total in enumerate(sums)
        )

    start = tuple(jnp.zeros((HALF, BLK), F32) for _ in range(places))
    sums = lax.fori_loop(0, count, one, start, unroll=2)
    for r in range(places):
        out_ref[slot, r] = sums[r]


def factor_pivot(tile_ref, p_ref, inv_ref, a_ref, b_ref, t_ref):
    step = 8
    a_ref[...] = tile_ref[...]
    b_ref[...] = jnp.where(iota((BLK, BLK), 0) == iota((BLK, BLK), 1), 1.0, 0.0)
    row = iota((BLK, BLK), 0)
    sub = iota((step, BLK), 0)
    lane = iota((step, BLK), 1)

    def group(g, carry):
        at = pl.ds(pl.multiple_of(g * step, step), step)
        a, b = a_ref[...], b_ref[...]
        rows, right = a_ref[at, :], b_ref[at, :]
        factor_rows, inverse_rows = [], []
        for s in range(step):
            pivot_row, right_row = rows[s : s + 1], right[s : s + 1]
            pivot = jnp.broadcast_to(pivot_row[:, s : s + 1], (1, BLK))
            root = 1.0 / jnp.sqrt(pivot)
            inverse = 1.0 / pivot
            factor_rows.append(pivot_row * root)
            inverse_rows.append(right_row * root)
            scaled, right_scaled = pivot_row * inverse, right_row * inverse
            near = jnp.where(sub > s, rows[:, s : s + 1], 0.0)
            far = jnp.where(row > g * step + s, a[:, s : s + 1], 0.0)
            rows, right = rows - near * scaled, right - near * right_scaled
            a, b = a - far * scaled, b - far * right_scaled
        a_ref[...] = pltpu.roll(a, BLK - step, 1)
        b_ref[...] = b
        block = jnp.concatenate(factor_rows, axis=0)
        block = jnp.where(jnp.logical_and(lane >= sub, lane < BLK - g * step), block, 0.0)
        t_ref[at, :] = pltpu.roll(block, g * step, 1)
        inv_ref[at, :] = jnp.concatenate(inverse_rows, axis=0)
        return carry

    lax.fori_loop(0, BLK // step, group, 0)
    p_ref[...] = t_ref[...].T


def final_kernel(panel_ref, diag_ref, pair_ref, col_ref, icol_ref, p_ref, inv_ref, asm_ref, fac_ref, l_ref):
    panel = panel_ref[0]
    lower = panel < 2
    other = (panel + 2) % 4
    asm_ref[...] = jnp.zeros_like(asm_ref)
    for r in range(2):
        at = pl.multiple_of((panel * 2 + r) * BLK, BLK)
        asm_ref[r * BLK : (r + 1) * BLK, pl.ds(at, BLK)] = diag_ref[r]
    for a in range(2):
        for b in range(2):
            tile = jnp.concatenate([pair_ref[0, a * 2 + b], pair_ref[1, a * 2 + b]], axis=0)
            tile = jnp.where(lower, tile, tile.T)
            row = pl.multiple_of(jnp.where(lower, a, b) * BLK, BLK)
            at = pl.multiple_of((other * 2 + jnp.where(lower, b, a)) * BLK, BLK)
            asm_ref[pl.ds(row, BLK), pl.ds(at, BLK)] = tile
    own = pl.multiple_of(panel * 2 * BLK, BLK)
    off = jnp.logical_or(panel > 0, iota((2 * BLK, BLK), 0) >= BLK)
    asm_ref[:, :BLK] = asm_ref[:, :BLK] + jnp.where(off, icol_ref[pl.ds(own, 2 * BLK), :], 0.0)
    inv_hi, inv_lo = split(inv_ref[...])
    l_ref[:BLK, :] = p_ref[...]
    for r in range(1, OWN):
        key = icol_ref[r * BLK : (r + 1) * BLK, :]
        if r in (4, 5):
            key = key + jnp.concatenate([col_ref[0, r - 4], col_ref[1, r - 4]], axis=0).T
        kh, kl = split(key)
        l_ref[r * BLK : (r + 1) * BLK, :] = mm_nt(kh, inv_hi) + (
            mm_nt(kh, inv_lo) + mm_nt(kl, inv_hi)
        )
    mine = l_ref[pl.ds(own, 2 * BLK), :]
    mh, ml = split(mine)
    fac_ref[:, :BLK] = mine
    for c in range(1, OWN):
        lh, ll = split(l_ref[c * BLK : (c + 1) * BLK, :])
        update = mm_nt(mh, lh) + (mm_nt(mh, ll) + mm_nt(ml, lh))
        fac_ref[:, c * BLK : (c + 1) * BLK] = asm_ref[:, c * BLK : (c + 1) * BLK] - jnp.where(
            off, update, 0.0
        )


def cost(flops, nbytes):
    return pl.CostEstimate(flops=flops, bytes_accessed=nbytes, transcendentals=0)


def whole(count):
    return [pl.BlockSpec(memory_space=VMEM)] * count


SMEM = pl.BlockSpec(memory_space=pltpu.SMEM)


def partner(value, panels):
    pairs = [(source, (source + panels // 2) % panels) for source in range(panels)]
    return lax.ppermute(value, "panel", pairs)


def per_device(
    interior_factor, coupling, interface_diag, interface_column, block_map, pair_pattern
):
    subs, order, width = coupling.shape
    owners_total = lax.axis_size("sub")
    panels = lax.axis_size("panel")
    sub = lax.axis_index("sub")
    panel = lax.axis_index("panel")
    upper = (panel >= panels // 2).astype(jnp.int32)
    upper_s = upper.reshape(1)
    panel_s = panel.astype(jnp.int32).reshape(1)
    groups = width // BLK
    half_width = width // 2

    outgoing = lax.dynamic_slice_in_dim(coupling, (1 - upper) * half_width, half_width, 2)
    incoming = [partner(outgoing[:EARLY], panels), partner(outgoing[EARLY:], panels)]

    maps = block_map.reshape(owners_total, subs, panels, groups)
    owner = maps[:, :, 0, :] // OWN
    match = (owner == sub).astype(jnp.int32)
    place = maps % 2
    base = panel % 2
    own_place = lax.dynamic_index_in_dim(place, panel, 2, keepdims=False)
    low_place = lax.dynamic_index_in_dim(place, base, 2, keepdims=False)
    high_place = lax.dynamic_index_in_dim(place, base + 2, 2, keepdims=False)
    diag_index = jnp.sum(match * (1 + own_place), axis=(1, 2))
    cross_index = jnp.sum(match * (1 + 2 * low_place + high_place), axis=(1, 2))
    slots = lax.dynamic_index_in_dim(owner, sub, 0, keepdims=False).reshape(-1)
    tiles = subs * groups
    filled = (slots[None, :] == jnp.arange(owners_total, dtype=jnp.int32)[:, None]).astype(jnp.int32)
    source = tiles + jnp.sum(
        filled * (jnp.arange(tiles, dtype=jnp.int32) - tiles)[None, :], axis=1
    )
    pattern = lax.dynamic_slice_in_dim(pair_pattern, base * groups + upper * 2, 2, 1).reshape(-1)

    hi, lo, w_half, diag_tiles = pl.pallas_call(
        solve_kernel,
        grid=(subs,),
        in_specs=[
            SMEM,
            pl.BlockSpec((subs, order, order), lambda l: (0, 0, 0)),
            pl.BlockSpec((1, order, width), lambda l: (l, 0, 0)),
        ],
        out_specs=[
            pl.BlockSpec((1, order, order), lambda l: (l, 0, 0)),
            pl.BlockSpec((1, order, order), lambda l: (l, 0, 0)),
            pl.BlockSpec((1, order, half_width), lambda l: (l, 0, 0)),
            pl.BlockSpec((tiles + 1, HALF + EXTRA, BLK), lambda l: (0, 0, 0)),
        ],
        out_shape=[
            jax.ShapeDtypeStruct((subs, order, order), BF16),
            jax.ShapeDtypeStruct((subs, order, order), BF16),
            jax.ShapeDtypeStruct((subs, order, half_width), BF16),
            jax.ShapeDtypeStruct((tiles + 1, HALF + EXTRA, BLK), BF16),
        ],
        scratch_shapes=[
            VMEM((subs * order, BLK), F32),
            VMEM((BASE, BASE, BLK), F32),
            VMEM((BASE, BASE, BLK), F32),
        ],
        compiler_params=pltpu.CompilerParams(vmem_limit_bytes=48 * 2**20),
        cost_estimate=cost(2 * 10**10, 2**25),
        name="solve",
    )(upper_s, interior_factor, coupling)

    anywhere = pl.BlockSpec(memory_space=pl.ANY)
    dma = pltpu.SemaphoreType.DMA

    def staged(count):
        return [
            VMEM((count, order, order), BF16),
            VMEM((count, order, order), BF16),
            VMEM((count, order, half_width), BF16),
            VMEM((count, order, half_width), BF16),
        ]

    diag_got, cross_early, columns = pl.pallas_call(
        functools.partial(first_kernel, EARLY),
        in_specs=[SMEM] * 2 + whole(2) + [anywhere] * 4,
        out_specs=whole(3),
        out_shape=[
            jax.ShapeDtypeStruct((owners_total, HALF + EXTRA, BLK), BF16),
            jax.ShapeDtypeStruct((EARLY * groups, HALF, BLK), BF16),
            jax.ShapeDtypeStruct((OWN * BLK, BLK), F32),
        ],
        scratch_shapes=[
            VMEM((owners_total, HALF + EXTRA, BLK), BF16),
            VMEM((EARLY * 2, HALF, BLK), BF16),
            *staged(EARLY),
            dma((4,)),
            dma,
            dma,
            dma,
            dma,
            dma((panels - 1,)),
            dma,
        ],
        compiler_params=pltpu.CompilerParams(
            collective_id=1, has_side_effects=True, vmem_limit_bytes=48 * 2**20
        ),
        cost_estimate=cost(10**10, 2**24),
        name="first",
    )(source, pattern, diag_tiles, interface_column, hi, lo, incoming[0], w_half)

    rows = OWN // panels
    late = subs - EARLY
    diag, pivot, pivot_inverse, pair, col = pl.pallas_call(
        functools.partial(second_kernel, EARLY),
        in_specs=[SMEM] * 4 + whole(3) + [anywhere] * 4,
        out_specs=whole(5),
        out_shape=[
            jax.ShapeDtypeStruct((rows, BLK, BLK), F32),
            jax.ShapeDtypeStruct((BLK, BLK), F32),
            jax.ShapeDtypeStruct((BLK, BLK), F32),
            jax.ShapeDtypeStruct((2, rows * rows, HALF, BLK), F32),
            jax.ShapeDtypeStruct((2, 2, HALF, BLK), F32),
        ],
        scratch_shapes=[
            VMEM((tiles + 1, HALF, BLK), BF16),
            VMEM((owners_total, HALF, BLK), BF16),
            VMEM((owners_total, HALF, BLK), BF16),
            VMEM((late * 2, HALF, BLK), BF16),
            *staged(late),
            VMEM((BLK, BLK), F32),
            VMEM((BLK, BLK), F32),
            VMEM((BLK, BLK), F32),
            VMEM((BLK, BLK), F32),
            dma((4,)),
            dma,
            dma,
            dma,
            dma,
            dma((panels - 1,)),
            dma,
            dma,
            dma,
            dma((2,)),
            dma,
        ],
        compiler_params=pltpu.CompilerParams(
            collective_id=2, has_side_effects=True, vmem_limit_bytes=48 * 2**20
        ),
        cost_estimate=cost(10**10, 2**24),
        name="second",
    )(
        source, pattern, diag_index, cross_index, diag_got, cross_early,
        interface_diag.reshape(rows, BLK), hi, lo, incoming[1], w_half,
    )
    return pl.pallas_call(
        final_kernel,
        in_specs=[SMEM] + whole(6),
        out_specs=whole(2),
        out_shape=[jax.ShapeDtypeStruct((rows * BLK, OWN * BLK), F32)] * 2,
        scratch_shapes=[VMEM((OWN * BLK, BLK), F32)],
        cost_estimate=cost(10**9, 2**22),
        name="final",
    )(panel_s, diag, pair, col, columns, pivot, pivot_inverse)


def solution(mesh):
    return jax.shard_map(
        per_device,
        mesh=mesh,
        in_specs=(
            P("sub", None, None),
            P("sub", None, "panel"),
            P(("sub", "panel")),
            P(("sub", "panel"), None),
            P(),
            P("sub", None),
        ),
        out_specs=(P(("sub", "panel"), None), P(("sub", "panel"), None)),
        check_vma=False,
    )
```

```python
import functools

import jax
import jax.numpy as jnp
from jax import lax
from jax.experimental import pallas as pl
from jax.experimental.pallas import tpu as pltpu
from jax.sharding import PartitionSpec as P

BLK = 128
HALF = BLK // 2
OWN = 8
BASE = 32
EXTRA = 8
EARLY = 5
F32 = jnp.float32
BF16 = jnp.bfloat16
VMEM = pltpu.VMEM


def split(x):
    hi = x.astype(BF16)
    return hi, (x - hi.astype(F32)).astype(BF16)


def mm(a, b):
    return jnp.dot(a, b, preferred_element_type=F32)


def mm_nt(a, b):
    return lax.dot_general(a, b, (((1,), (1,)), ((), ())), preferred_element_type=F32)


def mm_tn(a, b):
    return lax.dot_general(a, b, (((0,), (0,)), ((), ())), preferred_element_type=F32)


def wide(dot, a, b):
    ah, al = split(a)
    bh, bl = split(b)
    return dot(ah, bh) + (dot(ah, bl) + dot(al, bh))


def iota(shape, axis):
    return lax.broadcasted_iota(jnp.int32, shape, axis)


def base_inverses(f_ref, s_ref, a_ref, x_ref):
    subs, order, _ = f_ref.shape
    tiles = order // BLK
    per_tile = BLK // BASE
    count = subs * order // BASE

    def gather(l, carry):
        for t in range(tiles):
            for q in range(per_tile):
                row = t * BLK + q * BASE
                block = f_ref[l, row : row + BASE, t * BLK : (t + 1) * BLK]
                if q:
                    block = pltpu.roll(block, BLK - q * BASE, 1)
                s_ref[pl.ds(pl.multiple_of(l * order + row, BASE), BASE), :] = block
        return carry

    lax.fori_loop(0, subs, gather, 0)

    def lanes(i, carry):
        a_ref[i] = s_ref[pl.ds(i, count, stride=BASE), :].T[:BASE]
        return carry

    lax.fori_loop(0, BASE, lanes, 0, unroll=4)
    rows = iota((BASE, BLK), 0)
    for i in range(BASE):
        top = 8 * (i // 8 + 1)
        total = jnp.where(rows[:top] == i, 1.0, 0.0).astype(F32)
        parts = [total[8 * g : 8 * g + 8] for g in range(top // 8)]
        for k in range(i):
            factor = a_ref[i, k : k + 1, :]
            for g in range(k // 8 + 1):
                parts[g] = parts[g] - factor * x_ref[k, 8 * g : 8 * g + 8, :]
        scale = 1.0 / a_ref[i, i : i + 1, :]
        for g in range(BASE // 8):
            x_ref[i, 8 * g : 8 * g + 8, :] = (
                parts[g] * scale if g < len(parts) else jnp.zeros((8, BLK), F32)
            )

    def back(i, carry):
        padded = jnp.concatenate([x_ref[i], jnp.zeros((BLK - BASE, BLK), F32)], axis=0)
        s_ref[pl.ds(i, count, stride=BASE), :] = padded.T
        return carry

    lax.fori_loop(0, BASE, back, 0, unroll=4)


def full_inverse(l, f_ref, s_ref):
    order = f_ref.shape[1]
    tiles = order // BLK
    row = iota((BLK, BLK), 0)
    col = iota((BLK, BLK), 1)
    inverse = []
    for t in range(tiles):
        pieces = []
        for q in range(BLK // BASE):
            start = pl.multiple_of(l * order + t * BLK + q * BASE, BASE)
            block = s_ref[pl.ds(start, BASE), :]
            pieces.append(pltpu.roll(block, q * BASE, 1) if q else block)
        inverse.append(jnp.concatenate(pieces, axis=0))
    size = BASE
    while size < BLK:
        below = jnp.logical_and(row // size % 2 == 1, col // size == row // size - 1)
        for t in range(tiles):
            tile = f_ref[l, t * BLK : (t + 1) * BLK, t * BLK : (t + 1) * BLK]
            strip = wide(mm, jnp.where(below, tile, 0.0), inverse[t])
            inverse[t] = inverse[t] - wide(mm, inverse[t], strip)
        size *= 2
    while len(inverse) > 1:
        size = inverse[0].shape[0]
        merged = []
        for t in range(0, len(inverse), 2):
            below = f_ref[l, (t + 1) * size : (t + 2) * size, t * size : (t + 1) * size]
            corner = -wide(mm, inverse[t + 1], wide(mm, below, inverse[t]))
            if len(inverse) > 2:
                merged.append(
                    jnp.concatenate(
                        [
                            jnp.concatenate([inverse[t], jnp.zeros((size, size), F32)], axis=1),
                            jnp.concatenate([corner, inverse[t + 1]], axis=1),
                        ],
                        axis=0,
                    )
                )
            else:
                return inverse[0], corner, inverse[1]
        inverse = merged


def apply_inverse(hi, lo, right):
    half = hi.shape[0] // 2
    top = mm(hi[:half, :half], right[:half]) + mm(lo[:half, :half], right[:half])
    low = mm(hi[half:], right) + mm(lo[half:], right)
    return jnp.concatenate([top.astype(BF16), low.astype(BF16)], axis=0)


def solve_kernel(upper_ref, f_ref, c_ref, hi_ref, lo_ref, w_ref, d_ref, s_ref, a_ref, x_ref):
    l = pl.program_id(0)
    order = f_ref.shape[1]
    half = order // 2
    groups = c_ref.shape[2] // BLK

    @pl.when(l == 0)
    def _():
        d_ref[...] = jnp.zeros_like(d_ref)
        base_inverses(f_ref, s_ref, a_ref, x_ref)

    left, corner, right = full_inverse(l, f_ref, s_ref)
    for part, rows, cols in ((left, 0, 0), (corner, half, 0), (right, half, half)):
        hi, lo = split(part)
        hi_ref[0, rows : rows + half, cols : cols + half] = hi
        lo_ref[0, rows : rows + half, cols : cols + half] = lo
    hi_ref[0, :half, half:] = jnp.zeros((half, half), BF16)
    lo_ref[0, :half, half:] = jnp.zeros((half, half), BF16)
    solved = apply_inverse(hi_ref[0], lo_ref[0], c_ref[0])
    width = solved.shape[1] // 2
    w_ref[0] = jnp.where(upper_ref[0] == 0, solved[:, :width], solved[:, width:])
    row = iota((HALF, BLK), 0)
    lane = iota((HALF, BLK), 1)
    from_low = lane - HALF < row
    eye = iota((BLK, BLK), 0) == iota((BLK, BLK), 1)
    extra_row = iota((EXTRA, BLK), 0)
    for r in range(groups):
        block = solved[:, r * BLK : (r + 1) * BLK]
        tile = mm_tn(block, block)
        folded = jnp.where(from_low, tile[HALF:], pltpu.roll(tile[:HALF], HALF, 1))
        diag = jnp.sum(jnp.where(eye, tile, 0.0), axis=0, keepdims=True)
        first = diag.astype(BF16).astype(F32)
        second = (diag - first).astype(BF16).astype(F32)
        third = diag - first - second
        extra = jnp.where(
            extra_row == 0,
            first,
            jnp.where(extra_row == 1, second, jnp.where(extra_row == 2, third, 0.0)),
        )
        d_ref[l * groups + r] = jnp.concatenate([folded, extra], axis=0).astype(BF16)


MESH = pl.DeviceIdType.MESH
SUB_SHAPE = (8, 4, 2)


def sub_peer(step):
    z_total, y_total, cores = SUB_SHAPE
    me = lax.axis_index("sub")
    z, y, core = me // (y_total * cores), (me // cores) % y_total, me % cores
    m = step % z_total
    dz = z_total // 2 + (1 - 2 * (m % 2)) * ((m + 1) // 2)
    rest = step // z_total
    return (
        ((z + dz) % z_total) * y_total + (y + rest // cores) % y_total
    ) * cores + (core + rest) % cores


def all_peers(total, act):
    skip = SUB_SHAPE[0] - 1

    def one(step, carry):
        act(sub_peer(step))
        return carry

    lax.fori_loop(0, skip, one, 0)
    lax.fori_loop(skip + 1, total, one, 0)


def greet(total, panels):
    barrier = pltpu.get_barrier_semaphore()
    panel = lax.axis_index("panel")

    def signal(peer):
        pl.semaphore_signal(barrier, inc=1, device_id={"sub": peer}, device_id_type=MESH)

    all_peers(total, signal)
    for away in range(1, panels):
        pl.semaphore_signal(
            barrier, inc=1, device_id={"panel": (panel + away) % panels}, device_id_type=MESH
        )
    return lambda: pl.semaphore_wait(barrier, total - 1 + panels - 1)


def to_panel(src, dst, send, recv, away):
    panels = lax.axis_size("panel")
    peer = (lax.axis_index("panel") + away) % panels
    return pltpu.make_async_remote_copy(
        src_ref=src,
        dst_ref=dst,
        send_sem=send,
        recv_sem=recv,
        device_id={"panel": peer},
        device_id_type=MESH,
    )


def await_bytes(ref, sem):
    pltpu.make_async_copy(ref, ref, sem).wait()


def scatter_slots(total, src_ref, tiles_ref, send_ref, recv_ref):
    me = lax.axis_index("sub")

    def one(s, carry):
        send_ref[s] = tiles_ref[src_ref[s]]
        return carry

    lax.fori_loop(0, total, one, 0, unroll=2)
    recv_ref[me] = tiles_ref[src_ref[me]]


def start_slots(total, send_ref, recv_ref, send, recv):
    me = lax.axis_index("sub")

    def go(peer):
        pltpu.make_async_remote_copy(
            src_ref=send_ref.at[peer],
            dst_ref=recv_ref.at[me],
            send_sem=send,
            recv_sem=recv,
            device_id={"sub": peer},
            device_id_type=MESH,
        ).start()

    all_peers(total, go)


def cross_product(l, i, pat_ref, hi_ref, lo_ref, c_ref, w_ref, x_ref, out_ref, send, recv):
    panels = lax.axis_size("panel")
    upper = lax.axis_index("panel") // (panels // 2)
    low = upper == 0
    width = c_ref.shape[2] // BLK
    solved = apply_inverse(hi_ref[l], lo_ref[l], c_ref[i])
    for r in range(width):
        own = w_ref[l, :, r * BLK : (r + 1) * BLK]
        other = solved[:, r * BLK : (r + 1) * BLK]
        tile = mm_tn(jnp.where(low, own, other), jnp.where(low, other, own))
        tile = tile * pat_ref[l * width + r].astype(F32)
        group = l * 2 * width + width * upper + r
        x_ref[group] = jnp.where(low, tile[:HALF], tile[HALF:]).astype(BF16)
        out_ref[l * width + r] = jnp.where(low, tile[HALF:], tile[:HALF]).astype(BF16)
        to_panel(
            out_ref.at[l * width + r], x_ref.at[group], send, recv, panels // 2
        ).start()


def exchange_kernel(
    src_ref, pat_ref, dindex_ref, xindex_ref, d_ref, icol_ref, own_diag_ref,
    hi_ref, lo_ref, early_ref, w_ref, c_any,
    diag_ref, p_ref, inv_ref, pair_ref, col_ref, cols_ref,
    dsend_ref, dgot_ref, x_ref, out_ref, xsend_ref, xgot_ref,
    late_ref, first_ref, a_ref, b_ref, t_ref,
    late_send, late_recv, dslot_send, dslot_recv, slot_send, slot_recv, half_send, half_recv,
    cols_send, cols_recv, first_send, first_recv, pair_send, pair_recv, col_send, col_recv,
):
    total = lax.axis_size("sub")
    panels = lax.axis_size("panel")
    panel = lax.axis_index("panel")
    upper = panel // (panels // 2)
    early, late = early_ref.shape[0], late_ref.shape[0]
    half_width = late_ref.shape[2]
    rows = icol_ref.shape[0]
    ready = greet(total, panels)
    scatter_slots(total, src_ref, d_ref, dsend_ref, dgot_ref)
    ready()
    at = pl.multiple_of((1 - upper) * half_width, half_width)
    late_copies = [
        to_panel(
            c_any.at[early + i, :, pl.ds(at, half_width)],
            late_ref.at[i],
            late_send.at[i],
            late_recv.at[i],
            panels // 2,
        )
        for i in range(late)
    ]
    for copy in late_copies:
        copy.start()
    start_slots(total, dsend_ref, dgot_ref, dslot_send, dslot_recv)
    mine = pl.ds(pl.multiple_of(panel * rows, rows), rows)
    column_copies = [
        to_panel(icol_ref, cols_ref.at[mine], cols_send.at[away - 1], cols_recv, away)
        for away in range(1, panels)
    ]
    for copy in column_copies:
        copy.start()
    cols_ref[mine, :] = icol_ref[...]

    def cross_early(i, carry):
        cross_product(
            i, i, pat_ref, hi_ref, lo_ref, early_ref, w_ref, x_ref, out_ref, half_send, half_recv
        )
        return carry

    lax.fori_loop(0, early, cross_early, 0)
    for i in range(late):
        late_copies[i].wait()
        cross_product(
            early + i, i, pat_ref, hi_ref, lo_ref, late_ref, w_ref, x_ref, out_ref, half_send, half_recv
        )
    x_ref[x_ref.shape[0] - 1] = jnp.zeros(x_ref.shape[1:], BF16)
    await_bytes(out_ref, half_send)
    await_bytes(out_ref, half_recv)
    scatter_slots(total, src_ref, x_ref, xsend_ref, xgot_ref)
    start_slots(total, xsend_ref, xgot_ref, slot_send, slot_recv)

    await_bytes(dsend_ref.at[pl.ds(0, total - 1)], dslot_send)
    await_bytes(dgot_ref.at[pl.ds(0, total - 1)], dslot_recv)
    sum_diagonal(dindex_ref, dgot_ref, own_diag_ref, diag_ref)

    @pl.when(panel == 0)
    def _():
        first_ref[...] = diag_ref[0]
        sends = [
            to_panel(first_ref, first_ref, first_send.at[away - 1], first_recv, away)
            for away in range(1, panels)
        ]
        for copy in sends:
            copy.start()
        for copy in sends:
            copy.wait_send()

    @pl.when(panel != 0)
    def _():
        await_bytes(first_ref, first_recv)

    factor_pivot(first_ref, p_ref, inv_ref, a_ref, b_ref, t_ref)
    for copy in column_copies:
        copy.wait_send()
    await_bytes(cols_ref.at[pl.ds(0, (panels - 1) * rows)], cols_recv)
    await_bytes(xsend_ref.at[pl.ds(0, total - 1)], slot_send)
    await_bytes(xgot_ref.at[pl.ds(0, total - 1)], slot_recv)
    sum_cross(xindex_ref, xgot_ref, pair_ref, upper)
    pair = to_panel(pair_ref.at[upper], pair_ref.at[upper], pair_send, pair_recv, panels // 2)
    pair.start()

    @pl.when(panel % 2 == 0)
    def _():
        key = pair_ref.at[upper, pl.ds(0, 2)]
        sends = [
            to_panel(key, col_ref.at[upper], col_send.at[k], col_recv, away)
            for k, away in enumerate((1, panels - 1))
        ]
        for copy in sends:
            copy.start()
        for copy in sends:
            copy.wait_send()
        pair.wait()
        col_ref[...] = pair_ref[:, :2]

    @pl.when(panel % 2 == 1)
    def _():
        pair.wait()
        await_bytes(col_ref, col_recv)


def sum_diagonal(index_ref, recv_ref, own_diag_ref, out_ref):
    count, height, _ = recv_ref.shape
    places = out_ref.shape[0]

    def one(s, sums):
        value = recv_ref[s].astype(F32)
        at = index_ref[s]
        return tuple(
            total + jnp.where(at == r + 1, value, 0.0) for r, total in enumerate(sums)
        )

    start = tuple(jnp.zeros((height, BLK), F32) for _ in range(places))
    sums = lax.fori_loop(0, count, one, start, unroll=2)
    row = iota((HALF, BLK), 0)
    lane = iota((HALF, BLK), 1)
    eye = iota((BLK, BLK), 0) == iota((BLK, BLK), 1)
    for r in range(places):
        folded = sums[r][:HALF]
        low = jnp.where(lane - HALF < row, folded, 0.0)
        high = jnp.where(
            jnp.logical_and(lane > row, lane < HALF), pltpu.roll(folded, HALF, 1), 0.0
        )
        strict = jnp.concatenate([high, low], axis=0)
        diag = jnp.sum(sums[r][HALF:], axis=0, keepdims=True) + own_diag_ref[r : r + 1, :]
        out_ref[r] = strict + strict.T + jnp.where(eye, diag, 0.0)


def sum_cross(index_ref, recv_ref, out_ref, slot):
    count = recv_ref.shape[0]
    places = out_ref.shape[1]

    def one(s, sums):
        value = recv_ref[s].astype(F32)
        at = index_ref[s]
        return tuple(
            total + jnp.where(at == r + 1, value, 0.0) for r, total in enumerate(sums)
        )

    start = tuple(jnp.zeros((HALF, BLK), F32) for _ in range(places))
    sums = lax.fori_loop(0, count, one, start, unroll=2)
    for r in range(places):
        out_ref[slot, r] = sums[r]


def factor_pivot(tile_ref, p_ref, inv_ref, a_ref, b_ref, t_ref):
    step = 8
    a_ref[...] = tile_ref[...]
    b_ref[...] = jnp.where(iota((BLK, BLK), 0) == iota((BLK, BLK), 1), 1.0, 0.0)
    row = iota((BLK, BLK), 0)
    sub = iota((step, BLK), 0)
    lane = iota((step, BLK), 1)

    def group(g, carry):
        at = pl.ds(pl.multiple_of(g * step, step), step)
        a, b = a_ref[...], b_ref[...]
        rows, right = a_ref[at, :], b_ref[at, :]
        factor_rows, inverse_rows = [], []
        for s in range(step):
            pivot_row, right_row = rows[s : s + 1], right[s : s + 1]
            pivot = jnp.broadcast_to(pivot_row[:, s : s + 1], (1, BLK))
            root = 1.0 / jnp.sqrt(pivot)
            inverse = 1.0 / pivot
            factor_rows.append(pivot_row * root)
            inverse_rows.append(right_row * root)
            scaled, right_scaled = pivot_row * inverse, right_row * inverse
            near = jnp.where(sub > s, rows[:, s : s + 1], 0.0)
            far = jnp.where(row > g * step + s, a[:, s : s + 1], 0.0)
            rows, right = rows - near * scaled, right - near * right_scaled
            a, b = a - far * scaled, b - far * right_scaled
        a_ref[...] = pltpu.roll(a, BLK - step, 1)
        b_ref[...] = b
        block = jnp.concatenate(factor_rows, axis=0)
        block = jnp.where(jnp.logical_and(lane >= sub, lane < BLK - g * step), block, 0.0)
        t_ref[at, :] = pltpu.roll(block, g * step, 1)
        inv_ref[at, :] = jnp.concatenate(inverse_rows, axis=0)
        return carry

    lax.fori_loop(0, BLK // step, group, 0)
    p_ref[...] = t_ref[...].T


def final_kernel(panel_ref, diag_ref, pair_ref, col_ref, icol_ref, p_ref, inv_ref, asm_ref, fac_ref, l_ref):
    panel = panel_ref[0]
    lower = panel < 2
    other = (panel + 2) % 4
    asm_ref[...] = jnp.zeros_like(asm_ref)
    for r in range(2):
        at = pl.multiple_of((panel * 2 + r) * BLK, BLK)
        asm_ref[r * BLK : (r + 1) * BLK, pl.ds(at, BLK)] = diag_ref[r]
    for a in range(2):
        for b in range(2):
            tile = jnp.concatenate([pair_ref[0, a * 2 + b], pair_ref[1, a * 2 + b]], axis=0)
            tile = jnp.where(lower, tile, tile.T)
            row = pl.multiple_of(jnp.where(lower, a, b) * BLK, BLK)
            at = pl.multiple_of((other * 2 + jnp.where(lower, b, a)) * BLK, BLK)
            asm_ref[pl.ds(row, BLK), pl.ds(at, BLK)] = tile
    own = pl.multiple_of(panel * 2 * BLK, BLK)
    off = jnp.logical_or(panel > 0, iota((2 * BLK, BLK), 0) >= BLK)
    asm_ref[:, :BLK] = asm_ref[:, :BLK] + jnp.where(off, icol_ref[pl.ds(own, 2 * BLK), :], 0.0)
    inv_hi, inv_lo = split(inv_ref[...])
    l_ref[:BLK, :] = p_ref[...]
    for r in range(1, OWN):
        key = icol_ref[r * BLK : (r + 1) * BLK, :]
        if r in (4, 5):
            key = key + jnp.concatenate([col_ref[0, r - 4], col_ref[1, r - 4]], axis=0).T
        kh, kl = split(key)
        l_ref[r * BLK : (r + 1) * BLK, :] = mm_nt(kh, inv_hi) + (
            mm_nt(kh, inv_lo) + mm_nt(kl, inv_hi)
        )
    mine = l_ref[pl.ds(own, 2 * BLK), :]
    mh, ml = split(mine)
    fac_ref[:, :BLK] = mine
    for c in range(1, OWN):
        lh, ll = split(l_ref[c * BLK : (c + 1) * BLK, :])
        update = mm_nt(mh, lh) + (mm_nt(mh, ll) + mm_nt(ml, lh))
        fac_ref[:, c * BLK : (c + 1) * BLK] = asm_ref[:, c * BLK : (c + 1) * BLK] - jnp.where(
            off, update, 0.0
        )


def cost(flops, nbytes):
    return pl.CostEstimate(flops=flops, bytes_accessed=nbytes, transcendentals=0)


def whole(count):
    return [pl.BlockSpec(memory_space=VMEM)] * count


SMEM = pl.BlockSpec(memory_space=pltpu.SMEM)


def partner(value, panels):
    pairs = [(source, (source + panels // 2) % panels) for source in range(panels)]
    return lax.ppermute(value, "panel", pairs)


def per_device(
    interior_factor, coupling, interface_diag, interface_column, block_map, pair_pattern
):
    subs, order, width = coupling.shape
    owners_total = lax.axis_size("sub")
    panels = lax.axis_size("panel")
    sub = lax.axis_index("sub")
    panel = lax.axis_index("panel")
    upper = (panel >= panels // 2).astype(jnp.int32)
    upper_s = upper.reshape(1)
    panel_s = panel.astype(jnp.int32).reshape(1)
    groups = width // BLK
    half_width = width // 2

    outgoing = lax.dynamic_slice(
        coupling, (0, 0, (1 - upper) * half_width), (EARLY, order, half_width)
    )
    incoming = partner(outgoing, panels)

    maps = block_map.reshape(owners_total, subs, panels, groups)
    owner = maps[:, :, 0, :] // OWN
    match = (owner == sub).astype(jnp.int32)
    place = maps % 2
    base = panel % 2
    own_place = lax.dynamic_index_in_dim(place, panel, 2, keepdims=False)
    low_place = lax.dynamic_index_in_dim(place, base, 2, keepdims=False)
    high_place = lax.dynamic_index_in_dim(place, base + 2, 2, keepdims=False)
    diag_index = jnp.sum(match * (1 + own_place), axis=(1, 2))
    cross_index = jnp.sum(match * (1 + 2 * low_place + high_place), axis=(1, 2))
    slots = lax.dynamic_index_in_dim(owner, sub, 0, keepdims=False).reshape(-1)
    tiles = subs * groups
    filled = (slots[None, :] == jnp.arange(owners_total, dtype=jnp.int32)[:, None]).astype(jnp.int32)
    source = tiles + jnp.sum(
        filled * (jnp.arange(tiles, dtype=jnp.int32) - tiles)[None, :], axis=1
    )
    pattern = lax.dynamic_slice_in_dim(pair_pattern, base * groups + upper * 2, 2, 1).reshape(-1)

    hi, lo, w_half, diag_tiles = pl.pallas_call(
        solve_kernel,
        grid=(subs,),
        in_specs=[
            SMEM,
            pl.BlockSpec((subs, order, order), lambda l: (0, 0, 0)),
            pl.BlockSpec((1, order, width), lambda l: (l, 0, 0)),
        ],
        out_specs=[
            pl.BlockSpec((1, order, order), lambda l: (l, 0, 0)),
            pl.BlockSpec((1, order, order), lambda l: (l, 0, 0)),
            pl.BlockSpec((1, order, half_width), lambda l: (l, 0, 0)),
            pl.BlockSpec((tiles + 1, HALF + EXTRA, BLK), lambda l: (0, 0, 0)),
        ],
        out_shape=[
            jax.ShapeDtypeStruct((subs, order, order), BF16),
            jax.ShapeDtypeStruct((subs, order, order), BF16),
            jax.ShapeDtypeStruct((subs, order, half_width), BF16),
            jax.ShapeDtypeStruct((tiles + 1, HALF + EXTRA, BLK), BF16),
        ],
        scratch_shapes=[
            VMEM((subs * order, BLK), F32),
            VMEM((BASE, BASE, BLK), F32),
            VMEM((BASE, BASE, BLK), F32),
        ],
        compiler_params=pltpu.CompilerParams(vmem_limit_bytes=40 * 2**20),
        cost_estimate=cost(2 * 10**10, 2**25),
        name="solve",
    )(upper_s, interior_factor, coupling)

    anywhere = pl.BlockSpec(memory_space=pl.ANY)
    dma = pltpu.SemaphoreType.DMA

    rows = OWN // panels
    late = subs - EARLY
    slot_shape = (owners_total, HALF, BLK)
    slot_shape_d = (owners_total, HALF + EXTRA, BLK)
    diag, pivot, pivot_inverse, pair, col, columns = pl.pallas_call(
        exchange_kernel,
        in_specs=[SMEM] * 4 + whole(7) + [anywhere],
        out_specs=whole(6),
        out_shape=[
            jax.ShapeDtypeStruct((rows, BLK, BLK), F32),
            jax.ShapeDtypeStruct((BLK, BLK), F32),
            jax.ShapeDtypeStruct((BLK, BLK), F32),
            jax.ShapeDtypeStruct((2, rows * rows, HALF, BLK), F32),
            jax.ShapeDtypeStruct((2, 2, HALF, BLK), F32),
            jax.ShapeDtypeStruct((OWN * BLK, BLK), F32),
        ],
        scratch_shapes=[
            VMEM(slot_shape_d, BF16),
            VMEM(slot_shape_d, BF16),
            VMEM((tiles + 1, HALF, BLK), BF16),
            VMEM((tiles // 2, HALF, BLK), BF16),
            VMEM(slot_shape, BF16),
            VMEM(slot_shape, BF16),
            VMEM((late, order, half_width), BF16),
            *[VMEM((BLK, BLK), F32)] * 4,
            dma((late,)),
            dma((late,)),
            *[dma] * 6,
            dma((panels - 1,)),
            dma,
            dma((panels - 1,)),
            *[dma] * 3,
            dma((2,)),
            dma,
        ],
        compiler_params=pltpu.CompilerParams(
            collective_id=1, has_side_effects=True, vmem_limit_bytes=26 * 2**20
        ),
        cost_estimate=cost(10**10, 2**24),
        name="exchange",
    )(
        source, pattern, diag_index, cross_index, diag_tiles, interface_column,
        interface_diag.reshape(rows, BLK), hi, lo, incoming, w_half, coupling,
    )
    return pl.pallas_call(
        final_kernel,
        in_specs=[SMEM] + whole(6),
        out_specs=whole(2),
        out_shape=[jax.ShapeDtypeStruct((rows * BLK, OWN * BLK), F32)] * 2,
        scratch_shapes=[VMEM((OWN * BLK, BLK), F32)],
        compiler_params=pltpu.CompilerParams(vmem_limit_bytes=16 * 2**20),
        cost_estimate=cost(10**9, 2**22),
        name="final",
    )(panel_s, diag, pair, col, columns, pivot, pivot_inverse)


def solution(mesh):
    return jax.shard_map(
        per_device,
        mesh=mesh,
        in_specs=(
            P("sub", None, None),
            P("sub", None, "panel"),
            P(("sub", "panel")),
            P(("sub", "panel"), None),
            P(),
            P("sub", None),
        ),
        out_specs=(P(("sub", "panel"), None), P(("sub", "panel"), None)),
        check_vma=False,
    )
```

```python
import functools

import jax
import jax.numpy as jnp
from jax import lax
from jax.experimental import pallas as pl
from jax.experimental.pallas import tpu as pltpu
from jax.sharding import PartitionSpec as P

BLK = 128
HALF = BLK // 2
OWN = 8
BASE = 32
LEVELS = 32760.0
STEP = 2
F32 = jnp.float32
BF16 = jnp.bfloat16
I16 = jnp.int16
VMEM = pltpu.VMEM


def split(x):
    hi = x.astype(BF16)
    return hi, (x - hi.astype(F32)).astype(BF16)


def mm(a, b):
    return jnp.dot(a, b, preferred_element_type=F32)


def mm_nt(a, b):
    return lax.dot_general(a, b, (((1,), (1,)), ((), ())), preferred_element_type=F32)


def mm_tn(a, b):
    return lax.dot_general(a, b, (((0,), (0,)), ((), ())), preferred_element_type=F32)


def wide(dot, a, b):
    ah, al = split(a)
    bh, bl = split(b)
    return dot(ah, bh) + (dot(ah, bl) + dot(al, bh))


def packed(a, b):
    size = b.shape[1]
    right = jnp.concatenate(split(b), axis=1)
    both = mm(jnp.concatenate(split(a), axis=1), jnp.concatenate([right, right], axis=0))
    return both[:, :size] + both[:, size:]


def to_levels(tile):
    most = jnp.max(jnp.max(jnp.abs(tile), axis=0, keepdims=True), axis=1, keepdims=True)
    level = jnp.maximum(most, 1e-30) / LEVELS
    levels = jnp.round(tile * (1.0 / level)).astype(jnp.int32).astype(I16)
    return levels, jnp.broadcast_to(level, (1, BLK))


def from_levels(levels, row):
    return levels.astype(jnp.int32).astype(F32) * row


def iota(shape, axis):
    return lax.broadcasted_iota(jnp.int32, shape, axis)


def base_inverses(f_ref, s_ref, a_ref, x_ref):
    order = f_ref.shape[1]
    subs = f_ref.shape[0] // order
    tiles = order // BLK
    per_tile = BLK // BASE
    quarter = iota((BASE, BLK), 1) // BASE

    def pick(parts, where):
        total = parts[-1]
        for q in range(per_tile - 1):
            total = jnp.where(where == q, parts[q], total)
        return total

    def gather(l, carry):
        for t in range(tiles):
            parts = [
                f_ref[
                    pl.ds(pl.multiple_of(l * order + t * BLK + q * BASE, BASE), BASE),
                    t * BLK : (t + 1) * BLK,
                ]
                for q in range(per_tile)
            ]
            start = pl.multiple_of((t * subs + l) * BASE, BASE)
            s_ref[pl.ds(start, BASE), :] = pick(parts, quarter)
        return carry

    lax.fori_loop(0, subs, gather, 0)

    def lanes(g, carry):
        rows = [
            s_ref[pl.ds(g * per_tile + k, subs * tiles, stride=BASE), :] for k in range(per_tile)
        ]
        turned = jnp.concatenate(rows, axis=0).T
        for k in range(per_tile):
            parts = [
                pltpu.roll(turned[q * BASE : (q + 1) * BASE], (q - k) * BASE % BLK, 1)
                if q != k
                else turned[q * BASE : (q + 1) * BASE]
                for q in range(per_tile)
            ]
            a_ref[g * per_tile + k] = pick(parts, quarter)
        return carry

    lax.fori_loop(0, BASE // per_tile, lanes, 0)
    rows = iota((BASE, BLK), 0)
    x_ref[...] = jnp.where(
        iota((BASE, BASE, BLK), 0) == iota((BASE, BASE, BLK), 1), 1.0, 0.0
    ).astype(F32)
    scales = [1.0 / a_ref[i, i : i + 1, :] for i in range(BASE)]
    for k in range(BASE):
        top = 8 * (k // 8 + 1)
        solved = x_ref[k, :top] * scales[k]
        x_ref[k, :top] = solved
        if k + 1 < BASE:
            x_ref[k + 1 :, :top] = x_ref[k + 1 :, :top] - a_ref[k + 1 :, k : k + 1, :] * solved[None]

    def back(g, carry):
        rows = []
        for q in range(per_tile):
            parts = [x_ref[g * per_tile + k] for k in range(per_tile)]
            parts = [
                pltpu.roll(part, (k - q) * BASE % BLK, 1) if q != k else part
                for k, part in enumerate(parts)
            ]
            rows.append(pick(parts, quarter))
        turned = jnp.concatenate(rows, axis=0).T
        for k in range(per_tile):
            s_ref[pl.ds(g * per_tile + k, subs * tiles, stride=BASE), :] = turned[
                k * BASE : (k + 1) * BASE
            ]
        return carry

    lax.fori_loop(0, BASE // per_tile, back, 0)


def full_inverses(first, count, f_ref, s_ref):
    order = f_ref.shape[1]
    subs = f_ref.shape[0] // order
    tiles = order // BLK
    row = iota((BLK, BLK), 0)
    col = iota((BLK, BLK), 1)
    quarter = iota((BASE, BLK), 1) // BASE
    where = [(first + i, t * BLK) for i in range(count) for t in range(tiles)]
    inverse = []
    for l, at in where:
        start = pl.multiple_of((at // BLK * subs + l) * BASE, BASE)
        block = s_ref[pl.ds(start, BASE), :]
        pieces = [jnp.where(quarter == q, block, 0.0) for q in range(BLK // BASE)]
        inverse.append(jnp.concatenate(pieces, axis=0))

    def rows_of(l, start, size):
        return pl.ds(pl.multiple_of(l * order + start, BASE), size)

    size = BASE
    while size < BLK:
        odd = range(size, BLK, 2 * size)
        wanted = jnp.logical_and(row // size % 2 == 1, col // size == row // size - 1)
        mask = jnp.concatenate([wanted[start : start + size] for start in odd], axis=0)
        zero = jnp.zeros((size, BLK), F32)
        strips = []
        for (l, at), known in zip(where, inverse):
            tile = jnp.concatenate(
                [f_ref[rows_of(l, at + start, size), at : at + BLK] for start in odd], axis=0
            )
            strips.append(packed(jnp.where(mask, tile, 0.0), known))
        changes = []
        for strip, known in zip(strips, inverse):
            spread, rows = [], []
            for k, start in enumerate(odd):
                spread += [zero, strip[k * size : (k + 1) * size]]
                rows.append(known[start : start + size])
            changes.append(packed(jnp.concatenate(rows, axis=0), jnp.concatenate(spread, axis=0)))
        for n, (change, known) in enumerate(zip(changes, inverse)):
            pieces = []
            for k, start in enumerate(odd):
                pieces += [
                    known[start - size : start],
                    known[start : start + size] - change[k * size : (k + 1) * size],
                ]
            inverse[n] = jnp.concatenate(pieces, axis=0)
        size *= 2
    while size < order:
        product = packed if size == BLK else functools.partial(wide, mm)
        strips = []
        for n in range(0, len(inverse), 2):
            l, at = where[n]
            below = f_ref[rows_of(l, at + size, size), at : at + size]
            strips.append(product(below, inverse[n]))
        corners = [-product(inverse[2 * n + 1], strip) for n, strip in enumerate(strips)]
        if 2 * size == order:
            return [(inverse[2 * i], corners[i], inverse[2 * i + 1]) for i in range(count)]
        zero = jnp.zeros((size, size), F32)
        inverse = [
            jnp.concatenate(
                [
                    jnp.concatenate([inverse[2 * n], zero], axis=1),
                    jnp.concatenate([corner, inverse[2 * n + 1]], axis=1),
                ],
                axis=0,
            )
            for n, corner in enumerate(corners)
        ]
        where = where[::2]
        size *= 2


def apply_inverse(hi_ref, lo_ref, l, right):
    half = hi_ref.shape[1] // 2
    top = mm(hi_ref[l, :half, :half], right[:half]) + mm(lo_ref[l, :half, :half], right[:half])
    low = mm(hi_ref[l, half:], right) + mm(lo_ref[l, half:], right)
    return jnp.concatenate([top.astype(BF16), low.astype(BF16)], axis=0)


def solve_pair(first, count, f_ref, s_ref, c_ref, hi_ref, lo_ref, w_ref, d_ref, dside_ref):
    order = hi_ref.shape[1]
    half = order // 2
    panels = lax.axis_size("panel")
    upper = lax.axis_index("panel") // (panels // 2)
    groups = c_ref.shape[2] // BLK
    row = iota((HALF, BLK), 0)
    lane = iota((HALF, BLK), 1)
    from_low = lane - HALF < row
    eye = iota((BLK, BLK), 0) == iota((BLK, BLK), 1)
    for i, blocks in enumerate(full_inverses(first, count, f_ref, s_ref)):
        for part, rows, cols in zip(blocks, (0, half, half), (0, 0, half)):
            hi, lo = split(part)
            hi_ref[first + i, rows : rows + half, cols : cols + half] = hi
            lo_ref[first + i, rows : rows + half, cols : cols + half] = lo
    for i in range(count):
        l = first + i
        solved = apply_inverse(hi_ref, lo_ref, l, c_ref[l])
        width = solved.shape[1] // 2
        w_ref[l] = jnp.where(upper == 0, solved[:, :width], solved[:, width:])
        for r in range(groups):
            block = solved[:, r * BLK : (r + 1) * BLK]
            tile = mm_tn(block, block)
            diag = jnp.sum(jnp.where(eye, tile, 0.0), axis=0, keepdims=True)
            tile = jnp.where(eye, 0.0, tile)
            folded = jnp.where(from_low, tile[HALF:], pltpu.roll(tile[:HALF], HALF, 1))
            levels, level = to_levels(folded)
            d_ref[l * groups + r] = levels
            dside_ref[l * groups + r] = jnp.concatenate([diag, level], axis=0)


MESH = pl.DeviceIdType.MESH
SUB_SHAPE = (8, 4, 2)


def sub_peer(step):
    z_total, y_total, cores = SUB_SHAPE
    me = lax.axis_index("sub")
    z, y, core = me // (y_total * cores), (me // cores) % y_total, me % cores
    m = step % z_total
    dz = z_total // 2 + (1 - 2 * (m % 2)) * ((m + 1) // 2)
    rest = step // z_total
    return (
        ((z + dz) % z_total) * y_total + (y + rest // cores) % y_total
    ) * cores + (core + rest) % cores


def all_peers(total, act):
    skip = SUB_SHAPE[0] - 1

    def one(step, carry):
        act(sub_peer(step))
        return carry

    lax.fori_loop(0, skip, one, 0)
    lax.fori_loop(skip + 1, total, one, 0)


def greet(total, panels):
    barrier = pltpu.get_barrier_semaphore()
    panel = lax.axis_index("panel")

    def signal(peer):
        pl.semaphore_signal(barrier, inc=1, device_id={"sub": peer}, device_id_type=MESH)

    all_peers(total, signal)
    for away in range(1, panels):
        pl.semaphore_signal(
            barrier, inc=1, device_id={"panel": (panel + away) % panels}, device_id_type=MESH
        )
    return lambda: pl.semaphore_wait(barrier, total - 1 + panels - 1)


def to_panel(src, dst, send, recv, away):
    panels = lax.axis_size("panel")
    peer = (lax.axis_index("panel") + away) % panels
    return pltpu.make_async_remote_copy(
        src_ref=src,
        dst_ref=dst,
        send_sem=send,
        recv_sem=recv,
        device_id={"panel": peer},
        device_id_type=MESH,
    )


def await_bytes(ref, sem):
    pltpu.make_async_copy(ref, ref, sem).wait()


def scatter_slots(total, src_ref, pairs):
    me = lax.axis_index("sub")

    def one(s, carry):
        at = src_ref[s]
        for tiles_ref, send_ref, _ in pairs:
            send_ref[s] = tiles_ref[at]
        return carry

    lax.fori_loop(0, total, one, 0, unroll=2)
    for tiles_ref, _, recv_ref in pairs:
        recv_ref[me] = tiles_ref[src_ref[me]]


def start_slots(total, pairs, send, recv):
    me = lax.axis_index("sub")

    def go(peer):
        for k, (_, send_ref, recv_ref) in enumerate(pairs):
            pltpu.make_async_remote_copy(
                src_ref=send_ref.at[peer],
                dst_ref=recv_ref.at[me],
                send_sem=send.at[k],
                recv_sem=recv.at[k],
                device_id={"sub": peer},
                device_id_type=MESH,
            ).start()

    all_peers(total, go)


def await_slots(total, pairs, send, recv):
    for k, (_, send_ref, recv_ref) in enumerate(pairs):
        await_bytes(send_ref.at[pl.ds(0, total - 1)], send.at[k])
        await_bytes(recv_ref.at[pl.ds(0, total - 1)], recv.at[k])


def cross_product(l, pat_ref, hi_ref, lo_ref, c_ref, w_ref, x_ref, xside_ref, out_ref, outside_ref, send, recv):
    panels = lax.axis_size("panel")
    upper = lax.axis_index("panel") // (panels // 2)
    low = upper == 0
    width = c_ref.shape[2] // BLK
    solved = apply_inverse(hi_ref, lo_ref, l, c_ref[l])
    for r in range(width):
        own = w_ref[l, :, r * BLK : (r + 1) * BLK]
        other = solved[:, r * BLK : (r + 1) * BLK]
        tile = mm_tn(jnp.where(low, own, other), jnp.where(low, other, own))
        tile = tile * pat_ref[l * width + r].astype(F32)
        group = l * 2 * width + width * upper + r
        levels, level = to_levels(tile)
        at = l * width + r
        x_ref[group] = jnp.where(low, levels[:HALF], levels[HALF:])
        out_ref[at] = jnp.where(low, levels[HALF:], levels[:HALF])
        xside_ref[group] = level
        outside_ref[at] = level
        to_panel(out_ref.at[at], x_ref.at[group], send.at[0], recv.at[0], panels // 2).start()
        to_panel(
            outside_ref.at[at], xside_ref.at[group], send.at[1], recv.at[1], panels // 2
        ).start()


def whole_kernel(
    src_ref, pat_ref, dindex_ref, xindex_ref, icol_ref, own_diag_ref, f_any, c_any,
    diag_ref, p_ref, inv_ref, pair_ref, col_ref, cols_ref,
    f_ref, c_ref, other_ref, hi_ref, lo_ref, w_ref, s_ref, base_ref, binv_ref,
    d_ref, dside_ref, dsend_ref, dside_send_ref, dgot_ref, dside_got_ref,
    x_ref, xside_ref, out_ref, outside_ref, xsend_ref, xside_send_ref, xgot_ref, xside_got_ref, first_ref, a_ref, b_ref, t_ref,
    local, other_send, other_recv, dslot_send, dslot_recv, slot_send, slot_recv, half_send, half_recv,
    cols_send, cols_recv, first_send, first_recv, pair_send, pair_recv, col_send, col_recv,
):
    total = lax.axis_size("sub")
    panels = lax.axis_size("panel")
    panel = lax.axis_index("panel")
    upper = panel // (panels // 2)
    subs, _, half_width = other_ref.shape
    rows = icol_ref.shape[0]
    ready = greet(total, panels)
    f_copy = pltpu.make_async_copy(f_any, f_ref, local.at[0])
    f_copy.start()
    c_copy = pltpu.make_async_copy(c_any, c_ref, local.at[1])
    c_copy.start()
    for ref in (d_ref, dside_ref, x_ref, xside_ref):
        ref[ref.shape[0] - 1] = jnp.zeros(ref.shape[1:], ref.dtype)
    d_pairs = ((d_ref, dsend_ref, dgot_ref), (dside_ref, dside_send_ref, dside_got_ref))
    x_pairs = ((x_ref, xsend_ref, xgot_ref), (xside_ref, xside_send_ref, xside_got_ref))
    ready()
    at = pl.multiple_of((1 - upper) * half_width, half_width)

    def coupling_copy(l):
        return to_panel(
            c_any.at[l, :, pl.ds(at, half_width)],
            other_ref.at[l],
            other_send.at[l],
            other_recv.at[l],
            panels // 2,
        )

    def start_coupling(l, carry):
        coupling_copy(l).start()
        return carry

    lax.fori_loop(0, subs, start_coupling, 0)
    f_copy.wait()
    base_inverses(f_ref, s_ref, base_ref, binv_ref)
    c_copy.wait()

    def solve(step, carry):
        solve_pair(step * STEP, STEP, f_ref, s_ref, c_ref, hi_ref, lo_ref, w_ref, d_ref, dside_ref)
        return carry

    lax.fori_loop(0, subs // STEP, solve, 0)
    scatter_slots(total, src_ref, d_pairs)
    start_slots(total, d_pairs, dslot_send, dslot_recv)

    def cross(l, carry):
        coupling_copy(l).wait()
        cross_product(
            l, pat_ref, hi_ref, lo_ref, other_ref, w_ref, x_ref, xside_ref, out_ref, outside_ref,
            half_send, half_recv,
        )
        return carry

    lax.fori_loop(0, subs, cross, 0)
    for k, ref in enumerate((out_ref, outside_ref)):
        await_bytes(ref, half_send.at[k])
        await_bytes(ref, half_recv.at[k])
    scatter_slots(total, src_ref, x_pairs)
    start_slots(total, x_pairs, slot_send, slot_recv)
    mine = pl.ds(pl.multiple_of(panel * rows, rows), rows)
    column_copies = [
        to_panel(icol_ref, cols_ref.at[mine], cols_send.at[away - 1], cols_recv, away)
        for away in range(1, panels)
    ]
    for copy in column_copies:
        copy.start()
    cols_ref[mine, :] = icol_ref[...]

    await_slots(total, d_pairs, dslot_send, dslot_recv)
    sum_diagonal(dindex_ref, dgot_ref, dside_got_ref, own_diag_ref, diag_ref)

    @pl.when(panel == 0)
    def _():
        first_ref[...] = diag_ref[0]
        sends = [
            to_panel(first_ref, first_ref, first_send.at[away - 1], first_recv, away)
            for away in range(1, panels)
        ]
        for copy in sends:
            copy.start()
        for copy in sends:
            copy.wait_send()

    @pl.when(panel != 0)
    def _():
        await_bytes(first_ref, first_recv)

    factor_pivot(first_ref, p_ref, inv_ref, a_ref, b_ref, t_ref)
    for copy in column_copies:
        copy.wait_send()
    await_bytes(cols_ref.at[pl.ds(0, (panels - 1) * rows)], cols_recv)
    await_slots(total, x_pairs, slot_send, slot_recv)
    sum_cross(xindex_ref, xgot_ref, xside_got_ref, pair_ref, upper)
    pair = to_panel(pair_ref.at[upper], pair_ref.at[upper], pair_send, pair_recv, panels // 2)
    pair.start()

    @pl.when(panel % 2 == 0)
    def _():
        key = pair_ref.at[upper, pl.ds(0, 2)]
        sends = [
            to_panel(key, col_ref.at[upper], col_send.at[k], col_recv, away)
            for k, away in enumerate((1, panels - 1))
        ]
        for copy in sends:
            copy.start()
        for copy in sends:
            copy.wait_send()
        pair.wait()
        col_ref[...] = pair_ref[:, :2]

    @pl.when(panel % 2 == 1)
    def _():
        pair.wait()
        await_bytes(col_ref, col_recv)


def sum_diagonal(index_ref, recv_ref, side_ref, own_diag_ref, out_ref):
    count = recv_ref.shape[0]
    places = out_ref.shape[0]

    def one(s, sums):
        side = side_ref[s]
        value = from_levels(recv_ref[s], side[1:2])
        diag = side[:1]
        at = index_ref[s]
        return tuple(
            (total + jnp.where(at == r + 1, value, 0.0), line + jnp.where(at == r + 1, diag, 0.0))
            for r, (total, line) in enumerate(sums)
        )

    start = tuple(
        (jnp.zeros((HALF, BLK), F32), own_diag_ref[r : r + 1, :]) for r in range(places)
    )
    sums = lax.fori_loop(0, count, one, start, unroll=2)
    row = iota((HALF, BLK), 0)
    lane = iota((HALF, BLK), 1)
    eye = iota((BLK, BLK), 0) == iota((BLK, BLK), 1)
    for r, (folded, diag) in enumerate(sums):
        low = jnp.where(lane - HALF < row, folded, 0.0)
        high = jnp.where(
            jnp.logical_and(lane > row, lane < HALF), pltpu.roll(folded, HALF, 1), 0.0
        )
        strict = jnp.concatenate([high, low], axis=0)
        out_ref[r] = strict + strict.T + jnp.where(eye, diag, 0.0)


def sum_cross(index_ref, recv_ref, side_ref, out_ref, slot):
    count = recv_ref.shape[0]
    places = out_ref.shape[1]

    def one(s, sums):
        value = from_levels(recv_ref[s], side_ref[s])
        at = index_ref[s]
        return tuple(
            total + jnp.where(at == r + 1, value, 0.0) for r, total in enumerate(sums)
        )

    start = tuple(jnp.zeros((HALF, BLK), F32) for _ in range(places))
    sums = lax.fori_loop(0, count, one, start, unroll=2)
    for r in range(places):
        out_ref[slot, r] = sums[r]


def factor_pivot(tile_ref, p_ref, inv_ref, a_ref, b_ref, t_ref):
    step = 8
    a_ref[...] = tile_ref[...]
    b_ref[...] = jnp.where(iota((BLK, BLK), 0) == iota((BLK, BLK), 1), 1.0, 0.0)
    row = iota((BLK, BLK), 0)
    sub = iota((step, BLK), 0)
    lane = iota((step, BLK), 1)

    def group(g, carry):
        at = pl.ds(pl.multiple_of(g * step, step), step)
        a, b = a_ref[...], b_ref[...]
        rows, right = a_ref[at, :], b_ref[at, :]
        factor_rows, inverse_rows = [], []
        for s in range(step):
            pivot_row, right_row = rows[s : s + 1], right[s : s + 1]
            pivot = jnp.broadcast_to(pivot_row[:, s : s + 1], (1, BLK))
            root = 1.0 / jnp.sqrt(pivot)
            inverse = 1.0 / pivot
            factor_rows.append(pivot_row * root)
            inverse_rows.append(right_row * root)
            scaled, right_scaled = pivot_row * inverse, right_row * inverse
            near = jnp.where(sub > s, rows[:, s : s + 1], 0.0)
            far = jnp.where(row > g * step + s, a[:, s : s + 1], 0.0)
            rows, right = rows - near * scaled, right - near * right_scaled
            a, b = a - far * scaled, b - far * right_scaled
        a_ref[...] = pltpu.roll(a, BLK - step, 1)
        b_ref[...] = b
        block = jnp.concatenate(factor_rows, axis=0)
        block = jnp.where(jnp.logical_and(lane >= sub, lane < BLK - g * step), block, 0.0)
        t_ref[at, :] = pltpu.roll(block, g * step, 1)
        inv_ref[at, :] = jnp.concatenate(inverse_rows, axis=0)
        return carry

    lax.fori_loop(0, BLK // step, group, 0)
    p_ref[...] = t_ref[...].T


def final_kernel(panel_ref, diag_ref, pair_ref, col_ref, icol_ref, p_ref, inv_ref, asm_ref, fac_ref, l_ref):
    panel = panel_ref[0]
    lower = panel < 2
    other = (panel + 2) % 4
    asm_ref[...] = jnp.zeros_like(asm_ref)
    for r in range(2):
        at = pl.multiple_of((panel * 2 + r) * BLK, BLK)
        asm_ref[r * BLK : (r + 1) * BLK, pl.ds(at, BLK)] = diag_ref[r]
    for a in range(2):
        for b in range(2):
            tile = jnp.concatenate([pair_ref[0, a * 2 + b], pair_ref[1, a * 2 + b]], axis=0)
            tile = jnp.where(lower, tile, tile.T)
            row = pl.multiple_of(jnp.where(lower, a, b) * BLK, BLK)
            at = pl.multiple_of((other * 2 + jnp.where(lower, b, a)) * BLK, BLK)
            asm_ref[pl.ds(row, BLK), pl.ds(at, BLK)] = tile
    own = pl.multiple_of(panel * 2 * BLK, BLK)
    off = jnp.logical_or(panel > 0, iota((2 * BLK, BLK), 0) >= BLK)
    asm_ref[:, :BLK] = asm_ref[:, :BLK] + jnp.where(off, icol_ref[pl.ds(own, 2 * BLK), :], 0.0)
    inv_hi, inv_lo = split(inv_ref[...])
    l_ref[:BLK, :] = p_ref[...]
    for r in range(1, OWN):
        key = icol_ref[r * BLK : (r + 1) * BLK, :]
        if r in (4, 5):
            key = key + jnp.concatenate([col_ref[0, r - 4], col_ref[1, r - 4]], axis=0).T
        kh, kl = split(key)
        l_ref[r * BLK : (r + 1) * BLK, :] = mm_nt(kh, inv_hi) + (
            mm_nt(kh, inv_lo) + mm_nt(kl, inv_hi)
        )
    mine = l_ref[pl.ds(own, 2 * BLK), :]
    mh, ml = split(mine)
    fac_ref[:, :BLK] = mine
    for c in range(1, OWN):
        lh, ll = split(l_ref[c * BLK : (c + 1) * BLK, :])
        update = mm_nt(mh, lh) + (mm_nt(mh, ll) + mm_nt(ml, lh))
        fac_ref[:, c * BLK : (c + 1) * BLK] = asm_ref[:, c * BLK : (c + 1) * BLK] - jnp.where(
            off, update, 0.0
        )


def cost(flops, nbytes):
    return pl.CostEstimate(flops=flops, bytes_accessed=nbytes, transcendentals=0)


def whole(count):
    return [pl.BlockSpec(memory_space=VMEM)] * count


SMEM = pl.BlockSpec(memory_space=pltpu.SMEM)


def per_device(
    interior_factor, coupling, interface_diag, interface_column, block_map, pair_pattern
):
    subs, order, width = coupling.shape
    owners_total = lax.axis_size("sub")
    panels = lax.axis_size("panel")
    sub = lax.axis_index("sub")
    panel = lax.axis_index("panel")
    upper = (panel >= panels // 2).astype(jnp.int32)
    panel_s = panel.astype(jnp.int32).reshape(1)
    groups = width // BLK
    half_width = width // 2

    maps = block_map.reshape(owners_total, subs, panels, groups)
    owner = maps[:, :, 0, :] // OWN
    match = (owner == sub).astype(jnp.int32)
    place = maps % 2
    base = panel % 2
    own_place = lax.dynamic_index_in_dim(place, panel, 2, keepdims=False)
    low_place = lax.dynamic_index_in_dim(place, base, 2, keepdims=False)
    high_place = lax.dynamic_index_in_dim(place, base + 2, 2, keepdims=False)
    diag_index = jnp.sum(match * (1 + own_place), axis=(1, 2))
    cross_index = jnp.sum(match * (1 + 2 * low_place + high_place), axis=(1, 2))
    slots = lax.dynamic_index_in_dim(owner, sub, 0, keepdims=False).reshape(-1)
    tiles = subs * groups
    filled = (slots[None, :] == jnp.arange(owners_total, dtype=jnp.int32)[:, None]).astype(jnp.int32)
    source = tiles + jnp.sum(
        filled * (jnp.arange(tiles, dtype=jnp.int32) - tiles)[None, :], axis=1
    )
    pattern = lax.dynamic_slice_in_dim(pair_pattern, base * groups + upper * 2, 2, 1).reshape(-1)

    anywhere = pl.BlockSpec(memory_space=pl.ANY)
    dma = pltpu.SemaphoreType.DMA

    rows = OWN // panels
    diag, pivot, pivot_inverse, pair, col, columns = pl.pallas_call(
        whole_kernel,
        in_specs=[SMEM] * 4 + whole(2) + [anywhere] * 2,
        out_specs=whole(6),
        out_shape=[
            jax.ShapeDtypeStruct((rows, BLK, BLK), F32),
            jax.ShapeDtypeStruct((BLK, BLK), F32),
            jax.ShapeDtypeStruct((BLK, BLK), F32),
            jax.ShapeDtypeStruct((2, rows * rows, HALF, BLK), F32),
            jax.ShapeDtypeStruct((2, 2, HALF, BLK), F32),
            jax.ShapeDtypeStruct((OWN * BLK, BLK), F32),
        ],
        scratch_shapes=[
            VMEM((subs * order, order), F32),
            VMEM((subs, order, width), BF16),
            VMEM((subs, order, half_width), BF16),
            VMEM((subs, order, order), BF16),
            VMEM((subs, order, order), BF16),
            VMEM((subs, order, half_width), BF16),
            VMEM((subs * order // BLK * BASE, BLK), F32),
            VMEM((BASE, BASE, BLK), F32),
            VMEM((BASE, BASE, BLK), F32),
            VMEM((tiles + 1, HALF, BLK), I16),
            VMEM((tiles + 1, 2, BLK), F32),
            VMEM((owners_total, HALF, BLK), I16),
            VMEM((owners_total, 2, BLK), F32),
            VMEM((owners_total, HALF, BLK), I16),
            VMEM((owners_total, 2, BLK), F32),
            VMEM((tiles + 1, HALF, BLK), I16),
            VMEM((tiles + 1, 1, BLK), F32),
            VMEM((tiles // 2, HALF, BLK), I16),
            VMEM((tiles // 2, 1, BLK), F32),
            VMEM((owners_total, HALF, BLK), I16),
            VMEM((owners_total, 1, BLK), F32),
            VMEM((owners_total, HALF, BLK), I16),
            VMEM((owners_total, 1, BLK), F32),
            *[VMEM((BLK, BLK), F32)] * 4,
            dma((2,)),
            dma((subs,)),
            dma((subs,)),
            *[dma((2,))] * 6,
            dma((panels - 1,)),
            dma,
            dma((panels - 1,)),
            *[dma] * 3,
            dma((2,)),
            dma,
        ],
        compiler_params=pltpu.CompilerParams(
            collective_id=1, has_side_effects=True, vmem_limit_bytes=50 * 2**20
        ),
        cost_estimate=cost(10**10, 2**24),
        name="whole",
    )(
        source, pattern, diag_index, cross_index, interface_column,
        interface_diag.reshape(rows, BLK), interior_factor.reshape(subs * order, order), coupling,
    )
    return pl.pallas_call(
        final_kernel,
        in_specs=[SMEM] + whole(6),
        out_specs=whole(2),
        out_shape=[jax.ShapeDtypeStruct((rows * BLK, OWN * BLK), F32)] * 2,
        scratch_shapes=[VMEM((OWN * BLK, BLK), F32)],
        compiler_params=pltpu.CompilerParams(vmem_limit_bytes=16 * 2**20),
        cost_estimate=cost(10**9, 2**22),
        name="final",
    )(panel_s, diag, pair, col, columns, pivot, pivot_inverse)


def solution(mesh):
    return jax.shard_map(
        per_device,
        mesh=mesh,
        in_specs=(
            P("sub", None, None),
            P("sub", None, "panel"),
            P(("sub", "panel")),
            P(("sub", "panel"), None),
            P(),
            P("sub", None),
        ),
        out_specs=(P(("sub", "panel"), None), P(("sub", "panel"), None)),
        check_vma=False,
    )
```

```python
import functools

import jax
import jax.numpy as jnp
from jax import lax
from jax.experimental import pallas as pl
from jax.experimental.pallas import tpu as pltpu
from jax.sharding import PartitionSpec as P

BLK = 128
HALF = BLK // 2
OWN = 8
BASE = 32
LEVELS = 32760.0
AHEAD = 3
STEP = 2
F32 = jnp.float32
BF16 = jnp.bfloat16
I16 = jnp.int16
VMEM = pltpu.VMEM


def split(x):
    hi = x.astype(BF16)
    return hi, (x - hi.astype(F32)).astype(BF16)


def mm(a, b):
    return jnp.dot(a, b, preferred_element_type=F32)


def mm_nt(a, b):
    return lax.dot_general(a, b, (((1,), (1,)), ((), ())), preferred_element_type=F32)


def mm_tn(a, b):
    return lax.dot_general(a, b, (((0,), (0,)), ((), ())), preferred_element_type=F32)


def wide(dot, a, b):
    ah, al = split(a)
    bh, bl = split(b)
    return dot(ah, bh) + (dot(ah, bl) + dot(al, bh))


def packed(a, b):
    size = b.shape[1]
    right = jnp.concatenate(split(b), axis=1)
    both = mm(jnp.concatenate(split(a), axis=1), jnp.concatenate([right, right], axis=0))
    return both[:, :size] + both[:, size:]


def to_levels(tile):
    most = jnp.max(jnp.max(jnp.abs(tile), axis=0, keepdims=True), axis=1, keepdims=True)
    level = jnp.maximum(most, 1e-30) / LEVELS
    levels = jnp.round(tile * (1.0 / level)).astype(jnp.int32).astype(I16)
    return levels, jnp.broadcast_to(level, (1, BLK))


def from_levels(levels, row):
    return levels.astype(jnp.int32).astype(F32) * row


def iota(shape, axis):
    return lax.broadcasted_iota(jnp.int32, shape, axis)


def base_inverses(f_ref, s_ref, a_ref, x_ref):
    order = f_ref.shape[1]
    subs = f_ref.shape[0] // order
    tiles = order // BLK
    per_tile = BLK // BASE
    quarter = iota((BASE, BLK), 1) // BASE

    def pick(parts, where):
        total = parts[-1]
        for q in range(per_tile - 1):
            total = jnp.where(where == q, parts[q], total)
        return total

    def gather(l, carry):
        for t in range(tiles):
            parts = [
                f_ref[
                    pl.ds(pl.multiple_of(l * order + t * BLK + q * BASE, BASE), BASE),
                    t * BLK : (t + 1) * BLK,
                ]
                for q in range(per_tile)
            ]
            start = pl.multiple_of((t * subs + l) * BASE, BASE)
            s_ref[pl.ds(start, BASE), :] = pick(parts, quarter)
        return carry

    lax.fori_loop(0, subs, gather, 0)

    def lanes(g, carry):
        rows = [
            s_ref[pl.ds(g * per_tile + k, subs * tiles, stride=BASE), :] for k in range(per_tile)
        ]
        turned = jnp.concatenate(rows, axis=0).T
        for k in range(per_tile):
            parts = [
                pltpu.roll(turned[q * BASE : (q + 1) * BASE], (q - k) * BASE % BLK, 1)
                if q != k
                else turned[q * BASE : (q + 1) * BASE]
                for q in range(per_tile)
            ]
            a_ref[g * per_tile + k] = pick(parts, quarter)
        return carry

    lax.fori_loop(0, BASE // per_tile, lanes, 0)
    rows = iota((BASE, BLK), 0)
    x_ref[...] = jnp.where(
        iota((BASE, BASE, BLK), 0) == iota((BASE, BASE, BLK), 1), 1.0, 0.0
    ).astype(F32)
    scales = [1.0 / a_ref[i, i : i + 1, :] for i in range(BASE)]
    for k in range(BASE):
        top = 8 * (k // 8 + 1)
        solved = x_ref[k, :top] * scales[k]
        x_ref[k, :top] = solved
        if k + 1 < BASE:
            x_ref[k + 1 :, :top] = x_ref[k + 1 :, :top] - a_ref[k + 1 :, k : k + 1, :] * solved[None]

    def back(g, carry):
        rows = []
        for q in range(per_tile):
            parts = [x_ref[g * per_tile + k] for k in range(per_tile)]
            parts = [
                pltpu.roll(part, (k - q) * BASE % BLK, 1) if q != k else part
                for k, part in enumerate(parts)
            ]
            rows.append(pick(parts, quarter))
        turned = jnp.concatenate(rows, axis=0).T
        for k in range(per_tile):
            s_ref[pl.ds(g * per_tile + k, subs * tiles, stride=BASE), :] = turned[
                k * BASE : (k + 1) * BASE
            ]
        return carry

    lax.fori_loop(0, BASE // per_tile, back, 0)


def full_inverses(first, count, f_ref, s_ref):
    order = f_ref.shape[1]
    subs = f_ref.shape[0] // order
    tiles = order // BLK
    row = iota((BLK, BLK), 0)
    col = iota((BLK, BLK), 1)
    quarter = iota((BASE, BLK), 1) // BASE
    where = [(first + i, t * BLK) for i in range(count) for t in range(tiles)]
    inverse = []
    for l, at in where:
        start = pl.multiple_of((at // BLK * subs + l) * BASE, BASE)
        block = s_ref[pl.ds(start, BASE), :]
        pieces = [jnp.where(quarter == q, block, 0.0) for q in range(BLK // BASE)]
        inverse.append(jnp.concatenate(pieces, axis=0))

    def rows_of(l, start, size):
        return pl.ds(pl.multiple_of(l * order + start, BASE), size)

    size = BASE
    while size < BLK:
        odd = range(size, BLK, 2 * size)
        wanted = jnp.logical_and(row // size % 2 == 1, col // size == row // size - 1)
        mask = jnp.concatenate([wanted[start : start + size] for start in odd], axis=0)
        zero = jnp.zeros((size, BLK), F32)
        strips = []
        for (l, at), known in zip(where, inverse):
            tile = jnp.concatenate(
                [f_ref[rows_of(l, at + start, size), at : at + BLK] for start in odd], axis=0
            )
            strips.append(packed(jnp.where(mask, tile, 0.0), known))
        changes = []
        for strip, known in zip(strips, inverse):
            spread, rows = [], []
            for k, start in enumerate(odd):
                spread += [zero, strip[k * size : (k + 1) * size]]
                rows.append(known[start : start + size])
            changes.append(packed(jnp.concatenate(rows, axis=0), jnp.concatenate(spread, axis=0)))
        for n, (change, known) in enumerate(zip(changes, inverse)):
            pieces = []
            for k, start in enumerate(odd):
                pieces += [
                    known[start - size : start],
                    known[start : start + size] - change[k * size : (k + 1) * size],
                ]
            inverse[n] = jnp.concatenate(pieces, axis=0)
        size *= 2
    while size < order:
        product = packed if size == BLK else functools.partial(wide, mm)
        strips = []
        for n in range(0, len(inverse), 2):
            l, at = where[n]
            below = f_ref[rows_of(l, at + size, size), at : at + size]
            strips.append(product(below, inverse[n]))
        corners = [-product(inverse[2 * n + 1], strip) for n, strip in enumerate(strips)]
        if 2 * size == order:
            return [(inverse[2 * i], corners[i], inverse[2 * i + 1]) for i in range(count)]
        zero = jnp.zeros((size, size), F32)
        inverse = [
            jnp.concatenate(
                [
                    jnp.concatenate([inverse[2 * n], zero], axis=1),
                    jnp.concatenate([corner, inverse[2 * n + 1]], axis=1),
                ],
                axis=0,
            )
            for n, corner in enumerate(corners)
        ]
        where = where[::2]
        size *= 2


def apply_inverse(hi_ref, lo_ref, l, right):
    half = hi_ref.shape[1] // 2
    top = mm(hi_ref[l, :half, :half], right[:half]) + mm(lo_ref[l, :half, :half], right[:half])
    low = mm(hi_ref[l, half:], right) + mm(lo_ref[l, half:], right)
    return jnp.concatenate([top.astype(BF16), low.astype(BF16)], axis=0)


def solve_pair(first, count, f_ref, s_ref, c_ref, hi_ref, lo_ref, w_ref, d_ref, dside_ref):
    order = hi_ref.shape[1]
    half = order // 2
    panels = lax.axis_size("panel")
    upper = lax.axis_index("panel") // (panels // 2)
    groups = c_ref.shape[2] // BLK
    row = iota((HALF, BLK), 0)
    lane = iota((HALF, BLK), 1)
    from_low = lane - HALF < row
    eye = iota((BLK, BLK), 0) == iota((BLK, BLK), 1)
    for i, blocks in enumerate(full_inverses(first, count, f_ref, s_ref)):
        for part, rows, cols in zip(blocks, (0, half, half), (0, 0, half)):
            hi, lo = split(part)
            hi_ref[first + i, rows : rows + half, cols : cols + half] = hi
            lo_ref[first + i, rows : rows + half, cols : cols + half] = lo
    for i in range(count):
        l = first + i
        solved = apply_inverse(hi_ref, lo_ref, l, c_ref[l])
        width = solved.shape[1] // 2
        w_ref[l] = jnp.where(upper == 0, solved[:, :width], solved[:, width:])
        for r in range(groups):
            block = solved[:, r * BLK : (r + 1) * BLK]
            tile = mm_tn(block, block)
            diag = jnp.sum(jnp.where(eye, tile, 0.0), axis=0, keepdims=True)
            tile = jnp.where(eye, 0.0, tile)
            folded = jnp.where(from_low, tile[HALF:], pltpu.roll(tile[:HALF], HALF, 1))
            levels, level = to_levels(folded)
            d_ref[l * groups + r] = levels
            dside_ref[l * groups + r] = jnp.concatenate([diag, level], axis=0)


MESH = pl.DeviceIdType.MESH
SUB_SHAPE = (8, 4, 2)


def sub_peer(step):
    z_total, y_total, cores = SUB_SHAPE
    me = lax.axis_index("sub")
    z, y, core = me // (y_total * cores), (me // cores) % y_total, me % cores
    m = step % z_total
    dz = z_total // 2 + (1 - 2 * (m % 2)) * ((m + 1) // 2)
    rest = step // z_total
    return (
        ((z + dz) % z_total) * y_total + (y + rest // cores) % y_total
    ) * cores + (core + rest) % cores


def all_peers(total, act):
    skip = SUB_SHAPE[0] - 1

    def one(step, carry):
        act(sub_peer(step))
        return carry

    lax.fori_loop(0, skip, one, 0)
    lax.fori_loop(skip + 1, total, one, 0)


def greet(total, panels):
    barrier = pltpu.get_barrier_semaphore()
    panel = lax.axis_index("panel")

    def signal(peer):
        pl.semaphore_signal(barrier, inc=1, device_id={"sub": peer}, device_id_type=MESH)

    all_peers(total, signal)
    for away in range(1, panels):
        pl.semaphore_signal(
            barrier, inc=1, device_id={"panel": (panel + away) % panels}, device_id_type=MESH
        )
    return lambda: pl.semaphore_wait(barrier, total - 1 + panels - 1)


def to_panel(src, dst, send, recv, away):
    panels = lax.axis_size("panel")
    peer = (lax.axis_index("panel") + away) % panels
    return pltpu.make_async_remote_copy(
        src_ref=src,
        dst_ref=dst,
        send_sem=send,
        recv_sem=recv,
        device_id={"panel": peer},
        device_id_type=MESH,
    )


def await_bytes(ref, sem):
    pltpu.make_async_copy(ref, ref, sem).wait()


def scatter_slots(total, src_ref, pairs):
    me = lax.axis_index("sub")

    def one(s, carry):
        at = src_ref[s]
        for tiles_ref, send_ref, _ in pairs:
            send_ref[s] = tiles_ref[at]
        return carry

    lax.fori_loop(0, total, one, 0, unroll=2)
    for tiles_ref, _, recv_ref in pairs:
        recv_ref[me] = tiles_ref[src_ref[me]]


def start_slots(total, pairs, send, recv):
    me = lax.axis_index("sub")

    def go(peer):
        for k, (_, send_ref, recv_ref) in enumerate(pairs):
            pltpu.make_async_remote_copy(
                src_ref=send_ref.at[peer],
                dst_ref=recv_ref.at[me],
                send_sem=send.at[k],
                recv_sem=recv.at[k],
                device_id={"sub": peer},
                device_id_type=MESH,
            ).start()

    all_peers(total, go)


def await_slots(total, pairs, send, recv):
    for k, (_, send_ref, recv_ref) in enumerate(pairs):
        await_bytes(send_ref.at[pl.ds(0, total - 1)], send.at[k])
        await_bytes(recv_ref.at[pl.ds(0, total - 1)], recv.at[k])


def pack_columns(phase, left, right):
    left, right = left.astype(F32), right.astype(F32)
    low = iota(left.shape, 1) < HALF
    if phase == 0:
        return jnp.where(low, left, pltpu.roll(right, HALF, 1)).astype(BF16)
    return jnp.where(low, pltpu.roll(left, HALF, 1), right).astype(BF16)


def cross_product(phase, l, pat_ref, hi_ref, lo_ref, c_ref, w_ref, x_refs, xside_refs, out_ref, outside_ref, send, recv):
    panels = lax.axis_size("panel")
    upper = lax.axis_index("panel") // (panels // 2)
    stay_low = upper == phase
    width = w_ref.shape[2] // BLK
    solved = apply_inverse(hi_ref, lo_ref, l, c_ref[phase, l])
    low = iota((BLK, BLK), 1) < HALF
    narrow = iota((HALF // 2, BLK), 1) < HALF
    for r in range(width):
        tile = mm_tn(w_ref[l, :, r * BLK : (r + 1) * BLK], solved)
        tile = tile * pat_ref[l * width + r].astype(F32)
        tile = jnp.where(low, tile, 0.0) if r == 0 else jnp.where(low, 0.0, tile)
        quarters = []
        for half in range(2):
            top = tile[half * HALF : half * HALF + HALF // 2]
            bottom = tile[half * HALF + HALF // 2 : (half + 1) * HALF]
            if r == 0:
                bottom = pltpu.roll(bottom, HALF, 1)
            else:
                top = pltpu.roll(top, HALF, 1)
            quarters.append(jnp.where(narrow, top, bottom))
        levels, level = to_levels(jnp.concatenate(quarters, axis=0))
        first, second = levels[: HALF // 2], levels[HALF // 2 :]
        group = l * 2 * width + width * upper + r
        at = l * width + r
        x_refs[phase][group] = jnp.where(stay_low, first, second)
        out_ref[phase, at] = jnp.where(stay_low, second, first)
        xside_refs[phase][group] = level
        outside_ref[phase, at] = level
        to_panel(
            out_ref.at[phase, at], x_refs[phase].at[group],
            send.at[2 * phase], recv.at[2 * phase], panels // 2,
        ).start()
        to_panel(
            outside_ref.at[phase, at], xside_refs[phase].at[group],
            send.at[2 * phase + 1], recv.at[2 * phase + 1], panels // 2,
        ).start()


def whole_kernel(
    src_ref, pat_ref, dindex_ref, xindex_ref, icol_ref, own_diag_ref, f_any, c_any,
    diag_ref, p_ref, inv_ref, pair_ref, col_ref, cols_ref,
    f_ref, c_ref, give_ref, other_ref, hi_ref, lo_ref, w_ref, s_ref, base_ref, binv_ref,
    d_ref, dside_ref, dsend_ref, dside_send_ref, dgot_ref, dside_got_ref,
    x0_ref, x1_ref, xside0_ref, xside1_ref, out_ref, outside_ref, xsend_ref, xside_send_ref, xgot_ref, xside_got_ref, part_ref, first_ref, a_ref, b_ref, t_ref,
    local, other_send, other_recv, dslot_send, dslot_recv, slot_send, slot_recv, half_send, half_recv,
    cols_send, cols_recv, first_send, first_recv, pair_send, pair_recv, col_send, col_recv,
):
    total = lax.axis_size("sub")
    panels = lax.axis_size("panel")
    panel = lax.axis_index("panel")
    upper = panel // (panels // 2)
    subs = c_ref.shape[0]
    rows = icol_ref.shape[0]
    ready = greet(total, panels)
    c_copy = pltpu.make_async_copy(c_any, c_ref, local.at[1])
    c_copy.start()
    f_copy = pltpu.make_async_copy(f_any, f_ref, local.at[0])
    f_copy.start()
    x_refs, xside_refs = (x0_ref, x1_ref), (xside0_ref, xside1_ref)
    for ref in (d_ref, dside_ref, *x_refs, *xside_refs):
        ref[ref.shape[0] - 1] = jnp.zeros(ref.shape[1:], ref.dtype)
    d_pairs = ((d_ref, dsend_ref, dgot_ref), (dside_ref, dside_send_ref, dside_got_ref))
    x_pairs = [
        (
            (x_refs[phase], xsend_ref.at[phase], xgot_ref.at[phase]),
            (xside_refs[phase], xside_send_ref.at[phase], xside_got_ref.at[phase]),
        )
        for phase in range(2)
    ]
    c_copy.wait()

    def give(l, carry):
        cols = c_ref[l]
        cols = jnp.where(upper == 0, cols[:, 2 * BLK :], cols[:, : 2 * BLK])
        for phase in range(2):
            give_ref[phase, l] = pack_columns(phase, cols[:, :BLK], cols[:, BLK:])
        return carry

    lax.fori_loop(0, subs, give, 0)
    ready()

    def coupling_copy(phase, l):
        return to_panel(
            give_ref.at[phase, l],
            other_ref.at[phase, l],
            other_send.at[phase, l],
            other_recv.at[phase, l],
            panels // 2,
        )

    def start_coupling(phase, first, last):
        def one(l, carry):
            coupling_copy(phase, l).start()
            return carry

        lax.fori_loop(first, last, one, 0)

    start_coupling(0, 0, subs)
    start_coupling(1, 0, AHEAD)
    f_copy.wait()
    base_inverses(f_ref, s_ref, base_ref, binv_ref)

    def solve(step, carry):
        solve_pair(step * STEP, STEP, f_ref, s_ref, c_ref, hi_ref, lo_ref, w_ref, d_ref, dside_ref)
        return carry

    lax.fori_loop(0, subs // STEP, solve, 0)
    scatter_slots(total, src_ref, d_pairs)
    start_slots(total, d_pairs, dslot_send, dslot_recv)

    def cross(phase, l):
        coupling_copy(phase, l).wait()
        cross_product(
            phase, l, pat_ref, hi_ref, lo_ref, other_ref, w_ref, x_refs, xside_refs, out_ref,
            outside_ref, half_send, half_recv,
        )

    def cross_first(l, carry):
        cross(0, l)
        coupling_copy(1, l + AHEAD).start()
        return carry

    def cross_rest(phase):
        def one(l, carry):
            cross(phase, l)
            return carry

        return one

    for phase in range(2):
        if phase == 0:
            lax.fori_loop(0, subs - AHEAD, cross_first, 0)
            lax.fori_loop(subs - AHEAD, subs, cross_rest(0), 0)
        else:
            lax.fori_loop(0, subs, cross_rest(1), 0)
        for k, ref in enumerate((out_ref, outside_ref)):
            await_bytes(ref.at[phase], half_send.at[2 * phase + k])
            await_bytes(ref.at[phase], half_recv.at[2 * phase + k])
        scatter_slots(total, src_ref, x_pairs[phase])
        start_slots(total, x_pairs[phase], slot_send.at[phase], slot_recv.at[phase])
    mine = pl.ds(pl.multiple_of(panel * rows, rows), rows)
    column_copies = [
        to_panel(icol_ref, cols_ref.at[mine], cols_send.at[away - 1], cols_recv, away)
        for away in range(1, panels)
    ]
    for copy in column_copies:
        copy.start()
    cols_ref[mine, :] = icol_ref[...]

    await_slots(total, d_pairs, dslot_send, dslot_recv)
    sum_diagonal(dindex_ref, dgot_ref, dside_got_ref, own_diag_ref, diag_ref)

    @pl.when(panel == 0)
    def _():
        first_ref[...] = diag_ref[0]
        sends = [
            to_panel(first_ref, first_ref, first_send.at[away - 1], first_recv, away)
            for away in range(1, panels)
        ]
        for copy in sends:
            copy.start()
        for copy in sends:
            copy.wait_send()

    @pl.when(panel != 0)
    def _():
        await_bytes(first_ref, first_recv)

    factor_pivot(first_ref, p_ref, inv_ref, a_ref, b_ref, t_ref)
    for copy in column_copies:
        copy.wait_send()
    await_bytes(cols_ref.at[pl.ds(0, (panels - 1) * rows)], cols_recv)
    for phase in range(2):
        await_slots(total, x_pairs[phase], slot_send.at[phase], slot_recv.at[phase])
        sum_cross(xindex_ref, xgot_ref.at[phase], xside_got_ref.at[phase], part_ref.at[phase])
    join_parts(part_ref, pair_ref, upper)
    pair = to_panel(pair_ref.at[upper], pair_ref.at[upper], pair_send, pair_recv, panels // 2)
    pair.start()

    @pl.when(panel % 2 == 0)
    def _():
        key = pair_ref.at[upper, pl.ds(0, 2)]
        sends = [
            to_panel(key, col_ref.at[upper], col_send.at[k], col_recv, away)
            for k, away in enumerate((1, panels - 1))
        ]
        for copy in sends:
            copy.start()
        for copy in sends:
            copy.wait_send()
        pair.wait()
        col_ref[...] = pair_ref[:, :2]

    @pl.when(panel % 2 == 1)
    def _():
        pair.wait()
        await_bytes(col_ref, col_recv)


def sum_diagonal(index_ref, recv_ref, side_ref, own_diag_ref, out_ref):
    count = recv_ref.shape[0]
    places = out_ref.shape[0]

    def one(s, sums):
        side = side_ref[s]
        value = from_levels(recv_ref[s], side[1:2])
        diag = side[:1]
        at = index_ref[s]
        return tuple(
            (total + jnp.where(at == r + 1, value, 0.0), line + jnp.where(at == r + 1, diag, 0.0))
            for r, (total, line) in enumerate(sums)
        )

    start = tuple(
        (jnp.zeros((HALF, BLK), F32), own_diag_ref[r : r + 1, :]) for r in range(places)
    )
    sums = lax.fori_loop(0, count, one, start, unroll=2)
    row = iota((HALF, BLK), 0)
    lane = iota((HALF, BLK), 1)
    eye = iota((BLK, BLK), 0) == iota((BLK, BLK), 1)
    for r, (folded, diag) in enumerate(sums):
        low = jnp.where(lane - HALF < row, folded, 0.0)
        high = jnp.where(
            jnp.logical_and(lane > row, lane < HALF), pltpu.roll(folded, HALF, 1), 0.0
        )
        strict = jnp.concatenate([high, low], axis=0)
        out_ref[r] = strict + strict.T + jnp.where(eye, diag, 0.0)


def sum_cross(index_ref, recv_ref, side_ref, out_ref):
    count, height, _ = recv_ref.shape
    places = out_ref.shape[0]

    def one(s, sums):
        value = from_levels(recv_ref[s], side_ref[s])
        at = index_ref[s]
        return tuple(
            total + jnp.where(at == r + 1, value, 0.0) for r, total in enumerate(sums)
        )

    start = tuple(jnp.zeros((height, BLK), F32) for _ in range(places))
    sums = lax.fori_loop(0, count, one, start, unroll=2)
    for r in range(places):
        out_ref[r] = sums[r]


def join_parts(part_ref, out_ref, upper):
    places = out_ref.shape[1]
    low = iota((HALF, BLK), 1) < HALF

    def at_low(part):
        return jnp.concatenate([part, pltpu.roll(part, HALF, 1)], axis=0)

    def at_high(part):
        return jnp.concatenate([pltpu.roll(part, HALF, 1), part], axis=0)

    for r in range(places):
        zero, one = part_ref[0, r], part_ref[1, r]
        left, right = jnp.where(upper == 0, zero, one), jnp.where(upper == 0, one, zero)
        straight = jnp.where(low, at_low(left), at_high(right))
        turned = jnp.concatenate(
            [at_low(part_ref[0, places + r]), at_low(part_ref[1, places + r])], axis=0
        ).T[:HALF]
        out_ref[upper, r] = straight + turned


def join_pair(first, second):
    low = iota((HALF, BLK), 1) < HALF
    second = pltpu.roll(second, HALF, 1)
    return jnp.concatenate([jnp.where(low, first, second), jnp.where(low, second, first)], axis=0)


def factor_pivot(tile_ref, p_ref, inv_ref, a_ref, b_ref, t_ref):
    step = 8
    a_ref[...] = tile_ref[...]
    b_ref[...] = jnp.where(iota((BLK, BLK), 0) == iota((BLK, BLK), 1), 1.0, 0.0)
    row = iota((BLK, BLK), 0)
    sub = iota((step, BLK), 0)
    lane = iota((step, BLK), 1)

    def group(g, carry):
        at = pl.ds(pl.multiple_of(g * step, step), step)
        a, b = a_ref[...], b_ref[...]
        rows, right = a_ref[at, :], b_ref[at, :]
        factor_rows, inverse_rows = [], []
        for s in range(step):
            pivot_row, right_row = rows[s : s + 1], right[s : s + 1]
            pivot = jnp.broadcast_to(pivot_row[:, s : s + 1], (1, BLK))
            root = 1.0 / jnp.sqrt(pivot)
            inverse = 1.0 / pivot
            factor_rows.append(pivot_row * root)
            inverse_rows.append(right_row * root)
            scaled, right_scaled = pivot_row * inverse, right_row * inverse
            near = jnp.where(sub > s, rows[:, s : s + 1], 0.0)
            far = jnp.where(row > g * step + s, a[:, s : s + 1], 0.0)
            rows, right = rows - near * scaled, right - near * right_scaled
            a, b = a - far * scaled, b - far * right_scaled
        a_ref[...] = pltpu.roll(a, BLK - step, 1)
        b_ref[...] = b
        block = jnp.concatenate(factor_rows, axis=0)
        block = jnp.where(jnp.logical_and(lane >= sub, lane < BLK - g * step), block, 0.0)
        t_ref[at, :] = pltpu.roll(block, g * step, 1)
        inv_ref[at, :] = jnp.concatenate(inverse_rows, axis=0)
        return carry

    lax.fori_loop(0, BLK // step, group, 0)
    p_ref[...] = t_ref[...].T


def final_kernel(panel_ref, diag_ref, pair_ref, col_ref, icol_ref, p_ref, inv_ref, asm_ref, fac_ref, l_ref):
    panel = panel_ref[0]
    lower = panel < 2
    other = (panel + 2) % 4
    asm_ref[...] = jnp.zeros_like(asm_ref)
    for r in range(2):
        at = pl.multiple_of((panel * 2 + r) * BLK, BLK)
        asm_ref[r * BLK : (r + 1) * BLK, pl.ds(at, BLK)] = diag_ref[r]
    for a in range(2):
        for b in range(2):
            tile = join_pair(pair_ref[0, a * 2 + b], pair_ref[1, a * 2 + b])
            tile = jnp.where(lower, tile, tile.T)
            row = pl.multiple_of(jnp.where(lower, a, b) * BLK, BLK)
            at = pl.multiple_of((other * 2 + jnp.where(lower, b, a)) * BLK, BLK)
            asm_ref[pl.ds(row, BLK), pl.ds(at, BLK)] = tile
    own = pl.multiple_of(panel * 2 * BLK, BLK)
    off = jnp.logical_or(panel > 0, iota((2 * BLK, BLK), 0) >= BLK)
    asm_ref[:, :BLK] = asm_ref[:, :BLK] + jnp.where(off, icol_ref[pl.ds(own, 2 * BLK), :], 0.0)
    inv_hi, inv_lo = split(inv_ref[...])
    l_ref[:BLK, :] = p_ref[...]
    for r in range(1, OWN):
        key = icol_ref[r * BLK : (r + 1) * BLK, :]
        if r in (4, 5):
            key = key + join_pair(col_ref[0, r - 4], col_ref[1, r - 4]).T
        kh, kl = split(key)
        l_ref[r * BLK : (r + 1) * BLK, :] = mm_nt(kh, inv_hi) + (
            mm_nt(kh, inv_lo) + mm_nt(kl, inv_hi)
        )
    mine = l_ref[pl.ds(own, 2 * BLK), :]
    mh, ml = split(mine)
    fac_ref[:, :BLK] = mine
    for c in range(1, OWN):
        lh, ll = split(l_ref[c * BLK : (c + 1) * BLK, :])
        update = mm_nt(mh, lh) + (mm_nt(mh, ll) + mm_nt(ml, lh))
        fac_ref[:, c * BLK : (c + 1) * BLK] = asm_ref[:, c * BLK : (c + 1) * BLK] - jnp.where(
            off, update, 0.0
        )


def cost(flops, nbytes):
    return pl.CostEstimate(flops=flops, bytes_accessed=nbytes, transcendentals=0)


def whole(count):
    return [pl.BlockSpec(memory_space=VMEM)] * count


SMEM = pl.BlockSpec(memory_space=pltpu.SMEM)


def per_device(
    interior_factor, coupling, interface_diag, interface_column, block_map, pair_pattern
):
    subs, order, width = coupling.shape
    owners_total = lax.axis_size("sub")
    panels = lax.axis_size("panel")
    sub = lax.axis_index("sub")
    panel = lax.axis_index("panel")
    upper = (panel >= panels // 2).astype(jnp.int32)
    panel_s = panel.astype(jnp.int32).reshape(1)
    groups = width // BLK
    half_width = width // 2

    maps = block_map.reshape(owners_total, subs, panels, groups)
    owner = maps[:, :, 0, :] // OWN
    match = (owner == sub).astype(jnp.int32)
    place = maps % 2
    base = panel % 2
    own_place = lax.dynamic_index_in_dim(place, panel, 2, keepdims=False)
    low_place = lax.dynamic_index_in_dim(place, base, 2, keepdims=False)
    high_place = lax.dynamic_index_in_dim(place, base + 2, 2, keepdims=False)
    diag_index = jnp.sum(match * (1 + own_place), axis=(1, 2))
    by_upper = (jnp.arange(groups, dtype=jnp.int32) >= groups // 2).astype(jnp.int32)
    cross_index = jnp.sum(
        match * (1 + 2 * low_place + high_place + 4 * by_upper[None, None, :]), axis=(1, 2)
    )
    slots = lax.dynamic_index_in_dim(owner, sub, 0, keepdims=False).reshape(-1)
    tiles = subs * groups
    filled = (slots[None, :] == jnp.arange(owners_total, dtype=jnp.int32)[:, None]).astype(jnp.int32)
    source = tiles + jnp.sum(
        filled * (jnp.arange(tiles, dtype=jnp.int32) - tiles)[None, :], axis=1
    )
    pattern = lax.dynamic_slice_in_dim(pair_pattern, base * groups + upper * 2, 2, 1).reshape(-1)

    anywhere = pl.BlockSpec(memory_space=pl.ANY)
    dma = pltpu.SemaphoreType.DMA

    rows = OWN // panels
    diag, pivot, pivot_inverse, pair, col, columns = pl.pallas_call(
        whole_kernel,
        in_specs=[SMEM] * 4 + whole(2) + [anywhere] * 2,
        out_specs=whole(6),
        out_shape=[
            jax.ShapeDtypeStruct((rows, BLK, BLK), F32),
            jax.ShapeDtypeStruct((BLK, BLK), F32),
            jax.ShapeDtypeStruct((BLK, BLK), F32),
            jax.ShapeDtypeStruct((2, rows * rows, HALF, BLK), F32),
            jax.ShapeDtypeStruct((2, 2, HALF, BLK), F32),
            jax.ShapeDtypeStruct((OWN * BLK, BLK), F32),
        ],
        scratch_shapes=[
            VMEM((subs * order, order), F32),
            VMEM((subs, order, width), BF16),
            VMEM((2, subs, order, BLK), BF16),
            VMEM((2, subs, order, BLK), BF16),
            VMEM((subs, order, order), BF16),
            VMEM((subs, order, order), BF16),
            VMEM((subs, order, half_width), BF16),
            VMEM((subs * order // BLK * BASE, BLK), F32),
            VMEM((BASE, BASE, BLK), F32),
            VMEM((BASE, BASE, BLK), F32),
            VMEM((tiles + 1, HALF, BLK), I16),
            VMEM((tiles + 1, 2, BLK), F32),
            VMEM((owners_total, HALF, BLK), I16),
            VMEM((owners_total, 2, BLK), F32),
            VMEM((owners_total, HALF, BLK), I16),
            VMEM((owners_total, 2, BLK), F32),
            *[VMEM((tiles + 1, HALF // 2, BLK), I16)] * 2,
            *[VMEM((tiles + 1, 1, BLK), F32)] * 2,
            VMEM((2, tiles // 2, HALF // 2, BLK), I16),
            VMEM((2, tiles // 2, 1, BLK), F32),
            VMEM((2, owners_total, HALF // 2, BLK), I16),
            VMEM((2, owners_total, 1, BLK), F32),
            VMEM((2, owners_total, HALF // 2, BLK), I16),
            VMEM((2, owners_total, 1, BLK), F32),
            VMEM((2, 2 * rows * rows, HALF // 2, BLK), F32),
            *[VMEM((BLK, BLK), F32)] * 4,
            dma((2,)),
            dma((2, subs)),
            dma((2, subs)),
            *[dma((2,))] * 2,
            *[dma((2, 2))] * 2,
            *[dma((4,))] * 2,
            dma((panels - 1,)),
            dma,
            dma((panels - 1,)),
            *[dma] * 3,
            dma((2,)),
            dma,
        ],
        compiler_params=pltpu.CompilerParams(
            collective_id=1, has_side_effects=True, vmem_limit_bytes=50 * 2**20
        ),
        cost_estimate=cost(10**10, 2**24),
        name="whole",
    )(
        source, pattern, diag_index, cross_index, interface_column,
        interface_diag.reshape(rows, BLK), interior_factor.reshape(subs * order, order), coupling,
    )
    return pl.pallas_call(
        final_kernel,
        in_specs=[SMEM] + whole(6),
        out_specs=whole(2),
        out_shape=[jax.ShapeDtypeStruct((rows * BLK, OWN * BLK), F32)] * 2,
        scratch_shapes=[VMEM((OWN * BLK, BLK), F32)],
        compiler_params=pltpu.CompilerParams(vmem_limit_bytes=16 * 2**20),
        cost_estimate=cost(10**9, 2**22),
        name="final",
    )(panel_s, diag, pair, col, columns, pivot, pivot_inverse)


def solution(mesh):
    return jax.shard_map(
        per_device,
        mesh=mesh,
        in_specs=(
            P("sub", None, None),
            P("sub", None, "panel"),
            P(("sub", "panel")),
            P(("sub", "panel"), None),
            P(),
            P("sub", None),
        ),
        out_specs=(P(("sub", "panel"), None), P(("sub", "panel"), None)),
        check_vma=False,
    )
```

```python
import functools

import jax
import jax.numpy as jnp
from jax import lax
from jax.experimental import pallas as pl
from jax.experimental.pallas import tpu as pltpu
from jax.sharding import PartitionSpec as P

BLK = 128
HALF = BLK // 2
OWN = 8
BASE = 32
LEVELS = 32760.0
STEP = 2
F32 = jnp.float32
BF16 = jnp.bfloat16
I16 = jnp.int16
VMEM = pltpu.VMEM


def split(x):
    hi = x.astype(BF16)
    return hi, (x - hi.astype(F32)).astype(BF16)


def mm(a, b):
    return jnp.dot(a, b, preferred_element_type=F32)


def mm_nt(a, b):
    return lax.dot_general(a, b, (((1,), (1,)), ((), ())), preferred_element_type=F32)


def mm_tn(a, b):
    return lax.dot_general(a, b, (((0,), (0,)), ((), ())), preferred_element_type=F32)


def wide(dot, a, b):
    ah, al = split(a)
    bh, bl = split(b)
    return dot(ah, bh) + (dot(ah, bl) + dot(al, bh))


def packed(a, b):
    size = b.shape[1]
    right = jnp.concatenate(split(b), axis=1)
    both = mm(jnp.concatenate(split(a), axis=1), jnp.concatenate([right, right], axis=0))
    return both[:, :size] + both[:, size:]


def to_levels(tile):
    most = jnp.max(jnp.max(jnp.abs(tile), axis=0, keepdims=True), axis=1, keepdims=True)
    level = jnp.maximum(most, 1e-30) / LEVELS
    levels = jnp.round(tile * (1.0 / level)).astype(jnp.int32).astype(I16)
    return levels, jnp.broadcast_to(level, (1, BLK))


def from_levels(levels, row):
    return levels.astype(jnp.int32).astype(F32) * row


def iota(shape, axis):
    return lax.broadcasted_iota(jnp.int32, shape, axis)


def base_inverses(f_ref, s_ref, a_ref, x_ref):
    order = f_ref.shape[1]
    subs = f_ref.shape[0] // order
    tiles = order // BLK
    per_tile = BLK // BASE
    quarter = iota((BASE, BLK), 1) // BASE

    def pick(parts, where):
        total = parts[-1]
        for q in range(per_tile - 1):
            total = jnp.where(where == q, parts[q], total)
        return total

    def gather(l, carry):
        for t in range(tiles):
            parts = [
                f_ref[
                    pl.ds(pl.multiple_of(l * order + t * BLK + q * BASE, BASE), BASE),
                    t * BLK : (t + 1) * BLK,
                ]
                for q in range(per_tile)
            ]
            start = pl.multiple_of((t * subs + l) * BASE, BASE)
            s_ref[pl.ds(start, BASE), :] = pick(parts, quarter)
        return carry

    lax.fori_loop(0, subs, gather, 0)

    def lanes(g, carry):
        rows = [
            s_ref[pl.ds(g * per_tile + k, subs * tiles, stride=BASE), :] for k in range(per_tile)
        ]
        turned = jnp.concatenate(rows, axis=0).T
        for k in range(per_tile):
            parts = [
                pltpu.roll(turned[q * BASE : (q + 1) * BASE], (q - k) * BASE % BLK, 1)
                if q != k
                else turned[q * BASE : (q + 1) * BASE]
                for q in range(per_tile)
            ]
            a_ref[g * per_tile + k] = pick(parts, quarter)
        return carry

    lax.fori_loop(0, BASE // per_tile, lanes, 0)
    rows = iota((BASE, BLK), 0)
    x_ref[...] = jnp.where(
        iota((BASE, BASE, BLK), 0) == iota((BASE, BASE, BLK), 1), 1.0, 0.0
    ).astype(F32)
    scales = [1.0 / a_ref[i, i : i + 1, :] for i in range(BASE)]
    for k in range(BASE):
        top = 8 * (k // 8 + 1)
        solved = x_ref[k, :top] * scales[k]
        x_ref[k, :top] = solved
        if k + 1 < BASE:
            x_ref[k + 1 :, :top] = x_ref[k + 1 :, :top] - a_ref[k + 1 :, k : k + 1, :] * solved[None]

    def back(g, carry):
        rows = []
        for q in range(per_tile):
            parts = [x_ref[g * per_tile + k] for k in range(per_tile)]
            parts = [
                pltpu.roll(part, (k - q) * BASE % BLK, 1) if q != k else part
                for k, part in enumerate(parts)
            ]
            rows.append(pick(parts, quarter))
        turned = jnp.concatenate(rows, axis=0).T
        for k in range(per_tile):
            s_ref[pl.ds(g * per_tile + k, subs * tiles, stride=BASE), :] = turned[
                k * BASE : (k + 1) * BASE
            ]
        return carry

    lax.fori_loop(0, BASE // per_tile, back, 0)


def full_inverses(first, count, f_ref, s_ref):
    order = f_ref.shape[1]
    subs = f_ref.shape[0] // order
    tiles = order // BLK
    row = iota((BLK, BLK), 0)
    col = iota((BLK, BLK), 1)
    quarter = iota((BASE, BLK), 1) // BASE
    where = [(first + i, t * BLK) for i in range(count) for t in range(tiles)]
    inverse = []
    for l, at in where:
        start = pl.multiple_of((at // BLK * subs + l) * BASE, BASE)
        block = s_ref[pl.ds(start, BASE), :]
        pieces = [jnp.where(quarter == q, block, 0.0) for q in range(BLK // BASE)]
        inverse.append(jnp.concatenate(pieces, axis=0))

    def rows_of(l, start, size):
        return pl.ds(pl.multiple_of(l * order + start, BASE), size)

    size = BASE
    while size < BLK:
        odd = range(size, BLK, 2 * size)
        wanted = jnp.logical_and(row // size % 2 == 1, col // size == row // size - 1)
        mask = jnp.concatenate([wanted[start : start + size] for start in odd], axis=0)
        zero = jnp.zeros((size, BLK), F32)
        strips = []
        for (l, at), known in zip(where, inverse):
            tile = jnp.concatenate(
                [f_ref[rows_of(l, at + start, size), at : at + BLK] for start in odd], axis=0
            )
            strips.append(packed(jnp.where(mask, tile, 0.0), known))
        changes = []
        for strip, known in zip(strips, inverse):
            spread, rows = [], []
            for k, start in enumerate(odd):
                spread += [zero, strip[k * size : (k + 1) * size]]
                rows.append(known[start : start + size])
            changes.append(packed(jnp.concatenate(rows, axis=0), jnp.concatenate(spread, axis=0)))
        for n, (change, known) in enumerate(zip(changes, inverse)):
            pieces = []
            for k, start in enumerate(odd):
                pieces += [
                    known[start - size : start],
                    known[start : start + size] - change[k * size : (k + 1) * size],
                ]
            inverse[n] = jnp.concatenate(pieces, axis=0)
        size *= 2
    while size < order:
        product = packed if size == BLK else functools.partial(wide, mm)
        strips = []
        for n in range(0, len(inverse), 2):
            l, at = where[n]
            below = f_ref[rows_of(l, at + size, size), at : at + size]
            strips.append(product(below, inverse[n]))
        corners = [-product(inverse[2 * n + 1], strip) for n, strip in enumerate(strips)]
        if 2 * size == order:
            return [(inverse[2 * i], corners[i], inverse[2 * i + 1]) for i in range(count)]
        zero = jnp.zeros((size, size), F32)
        inverse = [
            jnp.concatenate(
                [
                    jnp.concatenate([inverse[2 * n], zero], axis=1),
                    jnp.concatenate([corner, inverse[2 * n + 1]], axis=1),
                ],
                axis=0,
            )
            for n, corner in enumerate(corners)
        ]
        where = where[::2]
        size *= 2


def apply_inverse(hi_ref, lo_ref, l, right):
    half = hi_ref.shape[1] // 2
    top = mm(hi_ref[l, :half, :half], right[:half]) + mm(lo_ref[l, :half, :half], right[:half])
    low = mm(hi_ref[l, half:], right) + mm(lo_ref[l, half:], right)
    return jnp.concatenate([top.astype(BF16), low.astype(BF16)], axis=0)


def solve_pair(first, count, f_ref, s_ref, c_ref, hi_ref, lo_ref, w_ref, d_ref, dside_ref):
    order = hi_ref.shape[1]
    half = order // 2
    panels = lax.axis_size("panel")
    upper = lax.axis_index("panel") // (panels // 2)
    groups = c_ref.shape[2] // BLK
    row = iota((HALF, BLK), 0)
    lane = iota((HALF, BLK), 1)
    from_low = lane - HALF < row
    eye = iota((BLK, BLK), 0) == iota((BLK, BLK), 1)
    for i, blocks in enumerate(full_inverses(first, count, f_ref, s_ref)):
        for part, rows, cols in zip(blocks, (0, half, half), (0, 0, half)):
            hi, lo = split(part)
            hi_ref[first + i, rows : rows + half, cols : cols + half] = hi
            lo_ref[first + i, rows : rows + half, cols : cols + half] = lo
    for i in range(count):
        l = first + i
        solved = apply_inverse(hi_ref, lo_ref, l, c_ref[l])
        width = solved.shape[1] // 2
        w_ref[l] = jnp.where(upper == 0, solved[:, :width], solved[:, width:])
        for r in range(groups):
            block = solved[:, r * BLK : (r + 1) * BLK]
            tile = mm_tn(block, block)
            diag = jnp.sum(jnp.where(eye, tile, 0.0), axis=0, keepdims=True)
            tile = jnp.where(eye, 0.0, tile)
            folded = jnp.where(from_low, tile[HALF:], pltpu.roll(tile[:HALF], HALF, 1))
            levels, level = to_levels(folded)
            d_ref[l * groups + r] = levels
            dside_ref[l * groups + r] = jnp.concatenate([diag, level], axis=0)


MESH = pl.DeviceIdType.MESH
SUB_SHAPE = (8, 4, 2)


def sub_peer(step):
    z_total, y_total, cores = SUB_SHAPE
    me = lax.axis_index("sub")
    z, y, core = me // (y_total * cores), (me // cores) % y_total, me % cores
    m = step % z_total
    dz = z_total // 2 + (1 - 2 * (m % 2)) * ((m + 1) // 2)
    rest = step // z_total
    return (
        ((z + dz) % z_total) * y_total + (y + rest // cores) % y_total
    ) * cores + (core + rest) % cores


def all_peers(total, act):
    skip = SUB_SHAPE[0] - 1

    def one(step, carry):
        act(sub_peer(step))
        return carry

    lax.fori_loop(0, skip, one, 0)
    lax.fori_loop(skip + 1, total, one, 0)


def greet(total, panels):
    barrier = pltpu.get_barrier_semaphore()
    panel = lax.axis_index("panel")

    def signal(peer):
        pl.semaphore_signal(barrier, inc=1, device_id={"sub": peer}, device_id_type=MESH)

    all_peers(total, signal)
    for away in range(1, panels):
        pl.semaphore_signal(
            barrier, inc=1, device_id={"panel": (panel + away) % panels}, device_id_type=MESH
        )
    return lambda: pl.semaphore_wait(barrier, total - 1 + panels - 1)


def to_panel(src, dst, send, recv, away):
    panels = lax.axis_size("panel")
    peer = (lax.axis_index("panel") + away) % panels
    return pltpu.make_async_remote_copy(
        src_ref=src,
        dst_ref=dst,
        send_sem=send,
        recv_sem=recv,
        device_id={"panel": peer},
        device_id_type=MESH,
    )


def await_bytes(ref, sem):
    pltpu.make_async_copy(ref, ref, sem).wait()


def scatter_slots(total, src_ref, pairs):
    me = lax.axis_index("sub")

    def one(s, carry):
        at = src_ref[s]
        for tiles_ref, send_ref, _ in pairs:
            send_ref[s] = tiles_ref[at]
        return carry

    lax.fori_loop(0, total, one, 0, unroll=8)
    for tiles_ref, _, recv_ref in pairs:
        recv_ref[me] = tiles_ref[src_ref[me]]


def start_slots(total, pairs, send, recv):
    me = lax.axis_index("sub")

    def go(peer):
        for k, (_, send_ref, recv_ref) in enumerate(pairs):
            pltpu.make_async_remote_copy(
                src_ref=send_ref.at[peer],
                dst_ref=recv_ref.at[me],
                send_sem=send.at[k],
                recv_sem=recv.at[k],
                device_id={"sub": peer},
                device_id_type=MESH,
            ).start()

    all_peers(total, go)


def await_slots(total, pairs, send, recv):
    for k, (_, send_ref, recv_ref) in enumerate(pairs):
        await_bytes(send_ref.at[pl.ds(0, total - 1)], send.at[k])
        await_bytes(recv_ref.at[pl.ds(0, total - 1)], recv.at[k])


def cross_product(l, pat_ref, hi_ref, lo_ref, c_ref, w_ref, x_ref, xside_ref, out_ref, outside_ref, send, recv):
    panels = lax.axis_size("panel")
    upper = lax.axis_index("panel") // (panels // 2)
    low = upper == 0
    width = c_ref.shape[2] // BLK
    solved = apply_inverse(hi_ref, lo_ref, l, c_ref[l])
    for r in range(width):
        own = w_ref[l, :, r * BLK : (r + 1) * BLK]
        other = solved[:, r * BLK : (r + 1) * BLK]
        tile = mm_tn(jnp.where(low, own, other), jnp.where(low, other, own))
        tile = tile * pat_ref[l * width + r].astype(F32)
        group = l * 2 * width + width * upper + r
        levels, level = to_levels(tile)
        at = l * width + r
        x_ref[group] = jnp.where(low, levels[:HALF], levels[HALF:])
        out_ref[at] = jnp.where(low, levels[HALF:], levels[:HALF])
        xside_ref[group] = level
        outside_ref[at] = level
        to_panel(out_ref.at[at], x_ref.at[group], send.at[0], recv.at[0], panels // 2).start()
        to_panel(
            outside_ref.at[at], xside_ref.at[group], send.at[1], recv.at[1], panels // 2
        ).start()


def whole_kernel(
    src_ref, pat_ref, dindex_ref, xindex_ref, icol_ref, own_diag_ref, f_any, c_any,
    diag_ref, p_ref, inv_ref, pair_ref, col_ref, cols_ref,
    f_ref, c_ref, other_ref, hi_ref, lo_ref, w_ref, s_ref, base_ref, binv_ref,
    d_ref, dside_ref, dsend_ref, dside_send_ref, dgot_ref, dside_got_ref,
    x_ref, xside_ref, out_ref, outside_ref, xsend_ref, xside_send_ref, xgot_ref, xside_got_ref,
    half_ref, halfside_ref, key_ref, keyside_ref, first_ref, a_ref, b_ref, t_ref,
    local, other_send, other_recv, dslot_send, dslot_recv, slot_send, slot_recv, half_send, half_recv,
    cols_send, cols_recv, first_send, first_recv, pair_send, pair_recv, col_send, col_recv,
):
    total = lax.axis_size("sub")
    panels = lax.axis_size("panel")
    panel = lax.axis_index("panel")
    upper = panel // (panels // 2)
    subs, _, half_width = other_ref.shape
    rows = icol_ref.shape[0]
    ready = greet(total, panels)
    f_copy = pltpu.make_async_copy(f_any, f_ref, local.at[0])
    f_copy.start()
    c_copy = pltpu.make_async_copy(c_any, c_ref, local.at[1])
    c_copy.start()
    for ref in (d_ref, dside_ref, x_ref, xside_ref):
        ref[ref.shape[0] - 1] = jnp.zeros(ref.shape[1:], ref.dtype)
    d_pairs = ((d_ref, dsend_ref, dgot_ref), (dside_ref, dside_send_ref, dside_got_ref))
    x_pairs = ((x_ref, xsend_ref, xgot_ref), (xside_ref, xside_send_ref, xside_got_ref))
    ready()
    at = pl.multiple_of((1 - upper) * half_width, half_width)

    def coupling_copy(l):
        return to_panel(
            c_any.at[l, :, pl.ds(at, half_width)],
            other_ref.at[l],
            other_send.at[l],
            other_recv.at[l],
            panels // 2,
        )

    def start_coupling(l, carry):
        coupling_copy(l).start()
        return carry

    lax.fori_loop(0, subs, start_coupling, 0)
    f_copy.wait()
    base_inverses(f_ref, s_ref, base_ref, binv_ref)
    c_copy.wait()

    def solve(step, carry):
        solve_pair(step * STEP, STEP, f_ref, s_ref, c_ref, hi_ref, lo_ref, w_ref, d_ref, dside_ref)
        return carry

    lax.fori_loop(0, subs // STEP, solve, 0)
    scatter_slots(total, src_ref, d_pairs)
    start_slots(total, d_pairs, dslot_send, dslot_recv)

    def cross(l, carry):
        coupling_copy(l).wait()
        cross_product(
            l, pat_ref, hi_ref, lo_ref, other_ref, w_ref, x_ref, xside_ref, out_ref, outside_ref,
            half_send, half_recv,
        )
        return carry

    lax.fori_loop(0, subs, cross, 0)
    for k, ref in enumerate((out_ref, outside_ref)):
        await_bytes(ref, half_send.at[k])
        await_bytes(ref, half_recv.at[k])
    scatter_slots(total, src_ref, x_pairs)
    start_slots(total, x_pairs, slot_send, slot_recv)
    mine = pl.ds(pl.multiple_of(panel * rows, rows), rows)
    column_copies = [
        to_panel(icol_ref, cols_ref.at[mine], cols_send.at[away - 1], cols_recv, away)
        for away in range(1, panels)
    ]
    for copy in column_copies:
        copy.start()
    cols_ref[mine, :] = icol_ref[...]

    await_slots(total, d_pairs, dslot_send, dslot_recv)
    sum_diagonal(dindex_ref, dgot_ref, dside_got_ref, own_diag_ref, diag_ref)

    @pl.when(panel == 0)
    def _():
        first_ref[...] = diag_ref[0]
        sends = [
            to_panel(first_ref, first_ref, first_send.at[away - 1], first_recv, away)
            for away in range(1, panels)
        ]
        for copy in sends:
            copy.start()
        for copy in sends:
            copy.wait_send()

    @pl.when(panel != 0)
    def _():
        await_bytes(first_ref, first_recv)

    factor_pivot(first_ref, p_ref, inv_ref, a_ref, b_ref, t_ref)
    for copy in column_copies:
        copy.wait_send()
    await_bytes(cols_ref.at[pl.ds(0, (panels - 1) * rows)], cols_recv)
    await_slots(total, x_pairs, slot_send, slot_recv)
    sum_cross(xindex_ref, xgot_ref, xside_got_ref, pair_ref, upper)
    places = pair_ref.shape[1]
    for r in range(places):
        levels, level = to_levels(pair_ref[upper, r])
        half_ref[upper, r] = levels
        halfside_ref[upper, r] = level
    pair = [
        to_panel(ref.at[upper], ref.at[upper], pair_send.at[k], pair_recv.at[k], panels // 2)
        for k, ref in enumerate((half_ref, halfside_ref))
    ]
    for copy in pair:
        copy.start()

    def take_pair():
        for copy in pair:
            copy.wait()
        for r in range(places):
            pair_ref[1 - upper, r] = from_levels(
                half_ref[1 - upper, r], halfside_ref[1 - upper, r]
            )

    @pl.when(panel % 2 == 0)
    def _():
        sends = [
            to_panel(
                src.at[upper, pl.ds(0, 2)], dst.at[upper], col_send.at[2 * k + n], col_recv.at[n], away
            )
            for k, away in enumerate((1, panels - 1))
            for n, (src, dst) in enumerate(((half_ref, key_ref), (halfside_ref, keyside_ref)))
        ]
        for copy in sends:
            copy.start()
        for copy in sends:
            copy.wait_send()
        take_pair()
        col_ref[...] = pair_ref[:, :2]

    @pl.when(panel % 2 == 1)
    def _():
        take_pair()
        await_bytes(key_ref, col_recv.at[0])
        await_bytes(keyside_ref, col_recv.at[1])
        for n in range(2):
            for r in range(2):
                col_ref[n, r] = from_levels(key_ref[n, r], keyside_ref[n, r])


def sum_diagonal(index_ref, recv_ref, side_ref, own_diag_ref, out_ref):
    count = recv_ref.shape[0]
    places = out_ref.shape[0]

    def one(s, sums):
        side = side_ref[s]
        value = from_levels(recv_ref[s], side[1:2])
        diag = side[:1]
        at = index_ref[s]
        return tuple(
            (total + jnp.where(at == r + 1, value, 0.0), line + jnp.where(at == r + 1, diag, 0.0))
            for r, (total, line) in enumerate(sums)
        )

    start = tuple(
        (jnp.zeros((HALF, BLK), F32), own_diag_ref[r : r + 1, :]) for r in range(places)
    )
    sums = lax.fori_loop(0, count, one, start, unroll=2)
    row = iota((HALF, BLK), 0)
    lane = iota((HALF, BLK), 1)
    eye = iota((BLK, BLK), 0) == iota((BLK, BLK), 1)
    for r, (folded, diag) in enumerate(sums):
        low = jnp.where(lane - HALF < row, folded, 0.0)
        high = jnp.where(
            jnp.logical_and(lane > row, lane < HALF), pltpu.roll(folded, HALF, 1), 0.0
        )
        strict = jnp.concatenate([high, low], axis=0)
        out_ref[r] = strict + strict.T + jnp.where(eye, diag, 0.0)


def sum_cross(index_ref, recv_ref, side_ref, out_ref, slot):
    count = recv_ref.shape[0]
    places = out_ref.shape[1]

    def one(s, sums):
        value = from_levels(recv_ref[s], side_ref[s])
        at = index_ref[s]
        return tuple(
            total + jnp.where(at == r + 1, value, 0.0) for r, total in enumerate(sums)
        )

    start = tuple(jnp.zeros((HALF, BLK), F32) for _ in range(places))
    sums = lax.fori_loop(0, count, one, start, unroll=2)
    for r in range(places):
        out_ref[slot, r] = sums[r]


def factor_pivot(tile_ref, p_ref, inv_ref, a_ref, b_ref, t_ref):
    step = 8
    a_ref[...] = tile_ref[...]
    b_ref[...] = jnp.where(iota((BLK, BLK), 0) == iota((BLK, BLK), 1), 1.0, 0.0)
    row = iota((BLK, BLK), 0)
    sub = iota((step, BLK), 0)
    lane = iota((step, BLK), 1)

    def group(g, carry):
        at = pl.ds(pl.multiple_of(g * step, step), step)
        a, b = a_ref[...], b_ref[...]
        rows, right = a_ref[at, :], b_ref[at, :]
        factor_rows, inverse_rows = [], []
        for s in range(step):
            pivot_row, right_row = rows[s : s + 1], right[s : s + 1]
            pivot = jnp.broadcast_to(pivot_row[:, s : s + 1], (1, BLK))
            root = 1.0 / jnp.sqrt(pivot)
            inverse = 1.0 / pivot
            factor_rows.append(pivot_row * root)
            inverse_rows.append(right_row * root)
            scaled, right_scaled = pivot_row * inverse, right_row * inverse
            near = jnp.where(sub > s, rows[:, s : s + 1], 0.0)
            far = jnp.where(row > g * step + s, a[:, s : s + 1], 0.0)
            rows, right = rows - near * scaled, right - near * right_scaled
            a, b = a - far * scaled, b - far * right_scaled
        a_ref[...] = pltpu.roll(a, BLK - step, 1)
        b_ref[...] = b
        block = jnp.concatenate(factor_rows, axis=0)
        block = jnp.where(jnp.logical_and(lane >= sub, lane < BLK - g * step), block, 0.0)
        t_ref[at, :] = pltpu.roll(block, g * step, 1)
        inv_ref[at, :] = jnp.concatenate(inverse_rows, axis=0)
        return carry

    lax.fori_loop(0, BLK // step, group, 0)
    p_ref[...] = t_ref[...].T


def final_kernel(panel_ref, diag_ref, pair_ref, col_ref, icol_ref, p_ref, inv_ref, asm_ref, fac_ref, l_ref):
    panel = panel_ref[0]
    lower = panel < 2
    other = (panel + 2) % 4
    asm_ref[...] = jnp.zeros_like(asm_ref)
    for r in range(2):
        at = pl.multiple_of((panel * 2 + r) * BLK, BLK)
        asm_ref[r * BLK : (r + 1) * BLK, pl.ds(at, BLK)] = diag_ref[r]
    for a in range(2):
        for b in range(2):
            tile = jnp.concatenate([pair_ref[0, a * 2 + b], pair_ref[1, a * 2 + b]], axis=0)
            tile = jnp.where(lower, tile, tile.T)
            row = pl.multiple_of(jnp.where(lower, a, b) * BLK, BLK)
            at = pl.multiple_of((other * 2 + jnp.where(lower, b, a)) * BLK, BLK)
            asm_ref[pl.ds(row, BLK), pl.ds(at, BLK)] = tile
    own = pl.multiple_of(panel * 2 * BLK, BLK)
    off = jnp.logical_or(panel > 0, iota((2 * BLK, BLK), 0) >= BLK)
    asm_ref[:, :BLK] = asm_ref[:, :BLK] + jnp.where(off, icol_ref[pl.ds(own, 2 * BLK), :], 0.0)
    inv_hi, inv_lo = split(inv_ref[...])
    l_ref[:BLK, :] = p_ref[...]
    for r in range(1, OWN):
        key = icol_ref[r * BLK : (r + 1) * BLK, :]
        if r in (4, 5):
            key = key + jnp.concatenate([col_ref[0, r - 4], col_ref[1, r - 4]], axis=0).T
        kh, kl = split(key)
        l_ref[r * BLK : (r + 1) * BLK, :] = mm_nt(kh, inv_hi) + (
            mm_nt(kh, inv_lo) + mm_nt(kl, inv_hi)
        )
    mine = l_ref[pl.ds(own, 2 * BLK), :]
    mh, ml = split(mine)
    fac_ref[:, :BLK] = mine
    for c in range(1, OWN):
        lh, ll = split(l_ref[c * BLK : (c + 1) * BLK, :])
        update = mm_nt(mh, lh) + (mm_nt(mh, ll) + mm_nt(ml, lh))
        fac_ref[:, c * BLK : (c + 1) * BLK] = asm_ref[:, c * BLK : (c + 1) * BLK] - jnp.where(
            off, update, 0.0
        )


def cost(flops, nbytes):
    return pl.CostEstimate(flops=flops, bytes_accessed=nbytes, transcendentals=0)


def whole(count):
    return [pl.BlockSpec(memory_space=VMEM)] * count


SMEM = pl.BlockSpec(memory_space=pltpu.SMEM)


def per_device(
    interior_factor, coupling, interface_diag, interface_column, block_map, pair_pattern
):
    subs, order, width = coupling.shape
    owners_total = lax.axis_size("sub")
    panels = lax.axis_size("panel")
    sub = lax.axis_index("sub")
    panel = lax.axis_index("panel")
    upper = (panel >= panels // 2).astype(jnp.int32)
    panel_s = panel.astype(jnp.int32).reshape(1)
    groups = width // BLK
    half_width = width // 2

    maps = block_map.reshape(owners_total, subs, panels, groups)
    owner = maps[:, :, 0, :] // OWN
    match = (owner == sub).astype(jnp.int32)
    place = maps % 2
    base = panel % 2
    own_place = lax.dynamic_index_in_dim(place, panel, 2, keepdims=False)
    low_place = lax.dynamic_index_in_dim(place, base, 2, keepdims=False)
    high_place = lax.dynamic_index_in_dim(place, base + 2, 2, keepdims=False)
    diag_index = jnp.sum(match * (1 + own_place), axis=(1, 2))
    cross_index = jnp.sum(match * (1 + 2 * low_place + high_place), axis=(1, 2))
    slots = lax.dynamic_index_in_dim(owner, sub, 0, keepdims=False).reshape(-1)
    tiles = subs * groups
    filled = (slots[None, :] == jnp.arange(owners_total, dtype=jnp.int32)[:, None]).astype(jnp.int32)
    source = tiles + jnp.sum(
        filled * (jnp.arange(tiles, dtype=jnp.int32) - tiles)[None, :], axis=1
    )
    pattern = lax.dynamic_slice_in_dim(pair_pattern, base * groups + upper * 2, 2, 1).reshape(-1)

    anywhere = pl.BlockSpec(memory_space=pl.ANY)
    dma = pltpu.SemaphoreType.DMA

    rows = OWN // panels
    diag, pivot, pivot_inverse, pair, col, columns = pl.pallas_call(
        whole_kernel,
        in_specs=[SMEM] * 4 + whole(2) + [anywhere] * 2,
        out_specs=whole(6),
        out_shape=[
            jax.ShapeDtypeStruct((rows, BLK, BLK), F32),
            jax.ShapeDtypeStruct((BLK, BLK), F32),
            jax.ShapeDtypeStruct((BLK, BLK), F32),
            jax.ShapeDtypeStruct((2, rows * rows, HALF, BLK), F32),
            jax.ShapeDtypeStruct((2, 2, HALF, BLK), F32),
            jax.ShapeDtypeStruct((OWN * BLK, BLK), F32),
        ],
        scratch_shapes=[
            VMEM((subs * order, order), F32),
            VMEM((subs, order, width), BF16),
            VMEM((subs, order, half_width), BF16),
            VMEM((subs, order, order), BF16),
            VMEM((subs, order, order), BF16),
            VMEM((subs, order, half_width), BF16),
            VMEM((subs * order // BLK * BASE, BLK), F32),
            VMEM((BASE, BASE, BLK), F32),
            VMEM((BASE, BASE, BLK), F32),
            VMEM((tiles + 1, HALF, BLK), I16),
            VMEM((tiles + 1, 2, BLK), F32),
            VMEM((owners_total, HALF, BLK), I16),
            VMEM((owners_total, 2, BLK), F32),
            VMEM((owners_total, HALF, BLK), I16),
            VMEM((owners_total, 2, BLK), F32),
            VMEM((tiles + 1, HALF, BLK), I16),
            VMEM((tiles + 1, 1, BLK), F32),
            VMEM((tiles // 2, HALF, BLK), I16),
            VMEM((tiles // 2, 1, BLK), F32),
            VMEM((owners_total, HALF, BLK), I16),
            VMEM((owners_total, 1, BLK), F32),
            VMEM((owners_total, HALF, BLK), I16),
            VMEM((owners_total, 1, BLK), F32),
            VMEM((2, rows * rows, HALF, BLK), I16),
            VMEM((2, rows * rows, 1, BLK), F32),
            VMEM((2, 2, HALF, BLK), I16),
            VMEM((2, 2, 1, BLK), F32),
            *[VMEM((BLK, BLK), F32)] * 4,
            dma((2,)),
            dma((subs,)),
            dma((subs,)),
            *[dma((2,))] * 6,
            dma((panels - 1,)),
            dma,
            dma((panels - 1,)),
            dma,
            *[dma((2,))] * 2,
            dma((4,)),
            dma((2,)),
        ],
        compiler_params=pltpu.CompilerParams(
            collective_id=1, has_side_effects=True, vmem_limit_bytes=50 * 2**20
        ),
        cost_estimate=cost(10**10, 2**24),
        name="whole",
    )(
        source, pattern, diag_index, cross_index, interface_column,
        interface_diag.reshape(rows, BLK), interior_factor.reshape(subs * order, order), coupling,
    )
    return pl.pallas_call(
        final_kernel,
        in_specs=[SMEM] + whole(6),
        out_specs=whole(2),
        out_shape=[jax.ShapeDtypeStruct((rows * BLK, OWN * BLK), F32)] * 2,
        scratch_shapes=[VMEM((OWN * BLK, BLK), F32)],
        compiler_params=pltpu.CompilerParams(vmem_limit_bytes=16 * 2**20),
        cost_estimate=cost(10**9, 2**22),
        name="final",
    )(panel_s, diag, pair, col, columns, pivot, pivot_inverse)


def solution(mesh):
    return jax.shard_map(
        per_device,
        mesh=mesh,
        in_specs=(
            P("sub", None, None),
            P("sub", None, "panel"),
            P(("sub", "panel")),
            P(("sub", "panel"), None),
            P(),
            P("sub", None),
        ),
        out_specs=(P(("sub", "panel"), None), P(("sub", "panel"), None)),
        check_vma=False,
    )
```

```python
import functools

import jax
import jax.numpy as jnp
from jax import lax
from jax.experimental import pallas as pl
from jax.experimental.pallas import tpu as pltpu
from jax.sharding import PartitionSpec as P

BLK = 128
HALF = BLK // 2
OWN = 8
BASE = 32
LEVELS = 32760.0
STEP = 2
F32 = jnp.float32
BF16 = jnp.bfloat16
I16 = jnp.int16
VMEM = pltpu.VMEM


def split(x):
    hi = x.astype(BF16)
    return hi, (x - hi.astype(F32)).astype(BF16)


def mm(a, b):
    return jnp.dot(a, b, preferred_element_type=F32)


def mm_nt(a, b):
    return lax.dot_general(a, b, (((1,), (1,)), ((), ())), preferred_element_type=F32)


def mm_tn(a, b):
    return lax.dot_general(a, b, (((0,), (0,)), ((), ())), preferred_element_type=F32)


def wide(dot, a, b):
    ah, al = split(a)
    bh, bl = split(b)
    return dot(ah, bh) + (dot(ah, bl) + dot(al, bh))


def packed(a, b):
    size = b.shape[1]
    right = jnp.concatenate(split(b), axis=1)
    both = mm(jnp.concatenate(split(a), axis=1), jnp.concatenate([right, right], axis=0))
    return both[:, :size] + both[:, size:]


def to_levels(tile):
    most = jnp.max(jnp.max(jnp.abs(tile), axis=0, keepdims=True), axis=1, keepdims=True)
    level = jnp.maximum(most, 1e-30) / LEVELS
    levels = jnp.round(tile * (1.0 / level)).astype(jnp.int32).astype(I16)
    return levels, jnp.broadcast_to(level, (1, BLK))


def from_levels(levels, row):
    return levels.astype(jnp.int32).astype(F32) * row


def iota(shape, axis):
    return lax.broadcasted_iota(jnp.int32, shape, axis)


def base_inverses(f_ref, s_ref, a_ref, x_ref):
    order = f_ref.shape[1]
    subs = f_ref.shape[0] // order
    tiles = order // BLK
    per_tile = BLK // BASE
    quarter = iota((BASE, BLK), 1) // BASE

    def pick(parts, where):
        total = parts[-1]
        for q in range(per_tile - 1):
            total = jnp.where(where == q, parts[q], total)
        return total

    def gather(l, carry):
        for t in range(tiles):
            parts = [
                f_ref[
                    pl.ds(pl.multiple_of(l * order + t * BLK + q * BASE, BASE), BASE),
                    t * BLK : (t + 1) * BLK,
                ]
                for q in range(per_tile)
            ]
            start = pl.multiple_of((t * subs + l) * BASE, BASE)
            s_ref[pl.ds(start, BASE), :] = pick(parts, quarter)
        return carry

    lax.fori_loop(0, subs, gather, 0)

    def lanes(g, carry):
        rows = [
            s_ref[pl.ds(g * per_tile + k, subs * tiles, stride=BASE), :] for k in range(per_tile)
        ]
        turned = jnp.concatenate(rows, axis=0).T
        for k in range(per_tile):
            parts = [
                pltpu.roll(turned[q * BASE : (q + 1) * BASE], (q - k) * BASE % BLK, 1)
                if q != k
                else turned[q * BASE : (q + 1) * BASE]
                for q in range(per_tile)
            ]
            a_ref[g * per_tile + k] = pick(parts, quarter)
        return carry

    lax.fori_loop(0, BASE // per_tile, lanes, 0)
    rows = iota((BASE, BLK), 0)
    x_ref[...] = jnp.where(
        iota((BASE, BASE, BLK), 0) == iota((BASE, BASE, BLK), 1), 1.0, 0.0
    ).astype(F32)
    scales = [1.0 / a_ref[i, i : i + 1, :] for i in range(BASE)]
    for k in range(BASE):
        top = 8 * (k // 8 + 1)
        solved = x_ref[k, :top] * scales[k]
        x_ref[k, :top] = solved
        if k + 1 < BASE:
            x_ref[k + 1 :, :top] = x_ref[k + 1 :, :top] - a_ref[k + 1 :, k : k + 1, :] * solved[None]

    def back(g, carry):
        rows = []
        for q in range(per_tile):
            parts = [x_ref[g * per_tile + k] for k in range(per_tile)]
            parts = [
                pltpu.roll(part, (k - q) * BASE % BLK, 1) if q != k else part
                for k, part in enumerate(parts)
            ]
            rows.append(pick(parts, quarter))
        turned = jnp.concatenate(rows, axis=0).T
        for k in range(per_tile):
            s_ref[pl.ds(g * per_tile + k, subs * tiles, stride=BASE), :] = turned[
                k * BASE : (k + 1) * BASE
            ]
        return carry

    lax.fori_loop(0, BASE // per_tile, back, 0)


def full_inverses(first, count, f_ref, s_ref):
    order = f_ref.shape[1]
    subs = f_ref.shape[0] // order
    tiles = order // BLK
    row = iota((BLK, BLK), 0)
    col = iota((BLK, BLK), 1)
    quarter = iota((BASE, BLK), 1) // BASE
    where = [(first + i, t * BLK) for i in range(count) for t in range(tiles)]
    inverse = []
    for l, at in where:
        start = pl.multiple_of((at // BLK * subs + l) * BASE, BASE)
        block = s_ref[pl.ds(start, BASE), :]
        pieces = [jnp.where(quarter == q, block, 0.0) for q in range(BLK // BASE)]
        inverse.append(jnp.concatenate(pieces, axis=0))

    def rows_of(l, start, size):
        return pl.ds(pl.multiple_of(l * order + start, BASE), size)

    size = BASE
    while size < BLK:
        odd = range(size, BLK, 2 * size)
        wanted = jnp.logical_and(row // size % 2 == 1, col // size == row // size - 1)
        mask = jnp.concatenate([wanted[start : start + size] for start in odd], axis=0)
        zero = jnp.zeros((size, BLK), F32)
        strips = []
        for (l, at), known in zip(where, inverse):
            tile = jnp.concatenate(
                [f_ref[rows_of(l, at + start, size), at : at + BLK] for start in odd], axis=0
            )
            strips.append(packed(jnp.where(mask, tile, 0.0), known))
        changes = []
        for strip, known in zip(strips, inverse):
            spread, rows = [], []
            for k, start in enumerate(odd):
                spread += [zero, strip[k * size : (k + 1) * size]]
                rows.append(known[start : start + size])
            changes.append(packed(jnp.concatenate(rows, axis=0), jnp.concatenate(spread, axis=0)))
        for n, (change, known) in enumerate(zip(changes, inverse)):
            pieces = []
            for k, start in enumerate(odd):
                pieces += [
                    known[start - size : start],
                    known[start : start + size] - change[k * size : (k + 1) * size],
                ]
            inverse[n] = jnp.concatenate(pieces, axis=0)
        size *= 2
    while size < order:
        product = packed if size == BLK else functools.partial(wide, mm)
        strips = []
        for n in range(0, len(inverse), 2):
            l, at = where[n]
            below = f_ref[rows_of(l, at + size, size), at : at + size]
            strips.append(product(below, inverse[n]))
        corners = [-product(inverse[2 * n + 1], strip) for n, strip in enumerate(strips)]
        if 2 * size == order:
            return [(inverse[2 * i], corners[i], inverse[2 * i + 1]) for i in range(count)]
        zero = jnp.zeros((size, size), F32)
        inverse = [
            jnp.concatenate(
                [
                    jnp.concatenate([inverse[2 * n], zero], axis=1),
                    jnp.concatenate([corner, inverse[2 * n + 1]], axis=1),
                ],
                axis=0,
            )
            for n, corner in enumerate(corners)
        ]
        where = where[::2]
        size *= 2


def apply_inverse(hi_ref, lo_ref, l, right):
    half = hi_ref.shape[1] // 2
    top = mm(hi_ref[l, :half, :half], right[:half]) + mm(lo_ref[l, :half, :half], right[:half])
    low = mm(hi_ref[l, half:], right) + mm(lo_ref[l, half:], right)
    return jnp.concatenate([top.astype(BF16), low.astype(BF16)], axis=0)


def solve_pair(first, count, f_ref, s_ref, c_ref, hi_ref, lo_ref, w_ref, d_ref, dside_ref):
    order = hi_ref.shape[1]
    half = order // 2
    panels = lax.axis_size("panel")
    upper = lax.axis_index("panel") // (panels // 2)
    groups = c_ref.shape[2] // BLK
    row = iota((HALF, BLK), 0)
    lane = iota((HALF, BLK), 1)
    from_low = lane - HALF < row
    eye = iota((BLK, BLK), 0) == iota((BLK, BLK), 1)
    for i, blocks in enumerate(full_inverses(first, count, f_ref, s_ref)):
        for part, rows, cols in zip(blocks, (0, half, half), (0, 0, half)):
            hi, lo = split(part)
            hi_ref[first + i, rows : rows + half, cols : cols + half] = hi
            lo_ref[first + i, rows : rows + half, cols : cols + half] = lo
    for i in range(count):
        l = first + i
        solved = apply_inverse(hi_ref, lo_ref, l, c_ref[l])
        width = solved.shape[1] // 2
        w_ref[l] = jnp.where(upper == 0, solved[:, :width], solved[:, width:])
        for r in range(groups):
            block = solved[:, r * BLK : (r + 1) * BLK]
            tile = mm_tn(block, block)
            diag = jnp.sum(jnp.where(eye, tile, 0.0), axis=0, keepdims=True)
            tile = jnp.where(eye, 0.0, tile)
            folded = jnp.where(from_low, tile[HALF:], pltpu.roll(tile[:HALF], HALF, 1))
            levels, level = to_levels(folded)
            d_ref[l * groups + r] = levels
            dside_ref[l * groups + r] = jnp.concatenate([diag, level], axis=0)


MESH = pl.DeviceIdType.MESH
SUB_SHAPE = (8, 4, 2)


def sub_peer(step):
    z_total, y_total, cores = SUB_SHAPE
    me = lax.axis_index("sub")
    z, y, core = me // (y_total * cores), (me // cores) % y_total, me % cores
    m = step % z_total
    dz = z_total // 2 + (1 - 2 * (m % 2)) * ((m + 1) // 2)
    rest = step // z_total
    return (
        ((z + dz) % z_total) * y_total + (y + rest // cores) % y_total
    ) * cores + (core + rest) % cores


def all_peers(total, act):
    skip = SUB_SHAPE[0] - 1

    def one(step, carry):
        act(sub_peer(step))
        return carry

    lax.fori_loop(0, skip, one, 0, unroll=7)
    lax.fori_loop(skip + 1, total, one, 0, unroll=8)


def greet(total, panels):
    barrier = pltpu.get_barrier_semaphore()
    panel = lax.axis_index("panel")

    def signal(peer):
        pl.semaphore_signal(barrier, inc=1, device_id={"sub": peer}, device_id_type=MESH)

    all_peers(total, signal)
    for away in range(1, panels):
        pl.semaphore_signal(
            barrier, inc=1, device_id={"panel": (panel + away) % panels}, device_id_type=MESH
        )
    return lambda: pl.semaphore_wait(barrier, total - 1 + panels - 1)


def to_panel(src, dst, send, recv, away):
    panels = lax.axis_size("panel")
    peer = (lax.axis_index("panel") + away) % panels
    return pltpu.make_async_remote_copy(
        src_ref=src,
        dst_ref=dst,
        send_sem=send,
        recv_sem=recv,
        device_id={"panel": peer},
        device_id_type=MESH,
    )


def await_bytes(ref, sem):
    pltpu.make_async_copy(ref, ref, sem).wait()


def scatter_slots(total, src_ref, pairs):
    me = lax.axis_index("sub")

    def one(s, carry):
        at = src_ref[s]
        for tiles_ref, send_ref, _ in pairs:
            send_ref[s] = tiles_ref[at]
        return carry

    lax.fori_loop(0, total, one, 0, unroll=8)
    for tiles_ref, _, recv_ref in pairs:
        recv_ref[me] = tiles_ref[src_ref[me]]


def start_slots(total, pairs, send, recv):
    me = lax.axis_index("sub")

    def go(peer):
        for k, (_, send_ref, recv_ref) in enumerate(pairs):
            pltpu.make_async_remote_copy(
                src_ref=send_ref.at[peer],
                dst_ref=recv_ref.at[me],
                send_sem=send.at[k],
                recv_sem=recv.at[k],
                device_id={"sub": peer},
                device_id_type=MESH,
            ).start()

    all_peers(total, go)


def await_slots(total, pairs, send, recv):
    for k, (_, send_ref, recv_ref) in enumerate(pairs):
        await_bytes(send_ref.at[pl.ds(0, total - 1)], send.at[k])
        await_bytes(recv_ref.at[pl.ds(0, total - 1)], recv.at[k])


def cross_product(l, pat_ref, hi_ref, lo_ref, c_ref, w_ref, x_ref, xside_ref, out_ref, outside_ref, send, recv):
    panels = lax.axis_size("panel")
    upper = lax.axis_index("panel") // (panels // 2)
    low = upper == 0
    width = c_ref.shape[2] // BLK
    solved = apply_inverse(hi_ref, lo_ref, l, c_ref[l])
    for r in range(width):
        own = w_ref[l, :, r * BLK : (r + 1) * BLK]
        other = solved[:, r * BLK : (r + 1) * BLK]
        tile = mm_tn(jnp.where(low, own, other), jnp.where(low, other, own))
        tile = tile * pat_ref[l * width + r].astype(F32)
        group = l * 2 * width + width * upper + r
        levels, level = to_levels(tile)
        at = l * width + r
        x_ref[group] = jnp.where(low, levels[:HALF], levels[HALF:])
        out_ref[at] = jnp.where(low, levels[HALF:], levels[:HALF])
        xside_ref[group] = level
        outside_ref[at] = level
        to_panel(out_ref.at[at], x_ref.at[group], send.at[0], recv.at[0], panels // 2).start()
        to_panel(
            outside_ref.at[at], xside_ref.at[group], send.at[1], recv.at[1], panels // 2
        ).start()


def whole_kernel(
    src_ref, pat_ref, dindex_ref, xindex_ref, icol_ref, own_diag_ref, f_any, c_any,
    diag_ref, p_ref, inv_ref, pair_ref, col_ref, cols_ref,
    f_ref, c_ref, other_ref, hi_ref, lo_ref, w_ref, s_ref, base_ref, binv_ref,
    d_ref, dside_ref, dsend_ref, dside_send_ref, dgot_ref, dside_got_ref,
    x_ref, xside_ref, out_ref, outside_ref, xsend_ref, xside_send_ref, xgot_ref, xside_got_ref,
    half_ref, halfside_ref, key_ref, keyside_ref, first_ref, a_ref, b_ref, t_ref,
    local, other_send, other_recv, dslot_send, dslot_recv, slot_send, slot_recv, half_send, half_recv,
    cols_send, cols_recv, first_send, first_recv, pair_send, pair_recv, col_send, col_recv,
):
    total = lax.axis_size("sub")
    panels = lax.axis_size("panel")
    panel = lax.axis_index("panel")
    upper = panel // (panels // 2)
    subs, _, half_width = other_ref.shape
    rows = icol_ref.shape[0]
    ready = greet(total, panels)
    f_copy = pltpu.make_async_copy(f_any, f_ref, local.at[0])
    f_copy.start()
    c_copy = pltpu.make_async_copy(c_any, c_ref, local.at[1])
    c_copy.start()
    for ref in (d_ref, dside_ref, x_ref, xside_ref):
        ref[ref.shape[0] - 1] = jnp.zeros(ref.shape[1:], ref.dtype)
    d_pairs = ((d_ref, dsend_ref, dgot_ref), (dside_ref, dside_send_ref, dside_got_ref))
    x_pairs = ((x_ref, xsend_ref, xgot_ref), (xside_ref, xside_send_ref, xside_got_ref))
    ready()
    at = pl.multiple_of((1 - upper) * half_width, half_width)

    def coupling_copy(l):
        return to_panel(
            c_any.at[l, :, pl.ds(at, half_width)],
            other_ref.at[l],
            other_send.at[l],
            other_recv.at[l],
            panels // 2,
        )

    def start_coupling(l, carry):
        coupling_copy(l).start()
        return carry

    lax.fori_loop(0, subs, start_coupling, 0)
    f_copy.wait()
    base_inverses(f_ref, s_ref, base_ref, binv_ref)
    c_copy.wait()

    def solve(step, carry):
        solve_pair(step * STEP, STEP, f_ref, s_ref, c_ref, hi_ref, lo_ref, w_ref, d_ref, dside_ref)
        return carry

    lax.fori_loop(0, subs // STEP, solve, 0)
    scatter_slots(total, src_ref, d_pairs)
    start_slots(total, d_pairs, dslot_send, dslot_recv)

    def cross(l, carry):
        coupling_copy(l).wait()
        cross_product(
            l, pat_ref, hi_ref, lo_ref, other_ref, w_ref, x_ref, xside_ref, out_ref, outside_ref,
            half_send, half_recv,
        )
        return carry

    lax.fori_loop(0, subs, cross, 0)
    for k, ref in enumerate((out_ref, outside_ref)):
        await_bytes(ref, half_send.at[k])
        await_bytes(ref, half_recv.at[k])
    scatter_slots(total, src_ref, x_pairs)
    start_slots(total, x_pairs, slot_send, slot_recv)
    mine = pl.ds(pl.multiple_of(panel * rows, rows), rows)
    column_copies = [
        to_panel(icol_ref, cols_ref.at[mine], cols_send.at[away - 1], cols_recv, away)
        for away in range(1, panels)
    ]
    for copy in column_copies:
        copy.start()
    cols_ref[mine, :] = icol_ref[...]

    await_slots(total, d_pairs, dslot_send, dslot_recv)
    sum_diagonal(dindex_ref, dgot_ref, dside_got_ref, own_diag_ref, diag_ref)

    @pl.when(panel == 0)
    def _():
        first_ref[...] = diag_ref[0]
        sends = [
            to_panel(first_ref, first_ref, first_send.at[away - 1], first_recv, away)
            for away in range(1, panels)
        ]
        for copy in sends:
            copy.start()
        for copy in sends:
            copy.wait_send()

    @pl.when(panel != 0)
    def _():
        await_bytes(first_ref, first_recv)

    factor_pivot(first_ref, p_ref, inv_ref, a_ref, b_ref, t_ref)
    for copy in column_copies:
        copy.wait_send()
    await_bytes(cols_ref.at[pl.ds(0, (panels - 1) * rows)], cols_recv)
    await_slots(total, x_pairs, slot_send, slot_recv)
    sum_cross(xindex_ref, xgot_ref, xside_got_ref, pair_ref, upper)
    places = pair_ref.shape[1]
    for r in range(places):
        levels, level = to_levels(pair_ref[upper, r])
        half_ref[upper, r] = levels
        halfside_ref[upper, r] = level
    pair = [
        to_panel(ref.at[upper], ref.at[upper], pair_send.at[k], pair_recv.at[k], panels // 2)
        for k, ref in enumerate((half_ref, halfside_ref))
    ]
    for copy in pair:
        copy.start()

    def take_pair():
        for copy in pair:
            copy.wait()
        for r in range(places):
            pair_ref[1 - upper, r] = from_levels(
                half_ref[1 - upper, r], halfside_ref[1 - upper, r]
            )

    @pl.when(panel % 2 == 0)
    def _():
        sends = [
            to_panel(
                src.at[upper, pl.ds(0, 2)], dst.at[upper], col_send.at[2 * k + n], col_recv.at[n], away
            )
            for k, away in enumerate((1, panels - 1))
            for n, (src, dst) in enumerate(((half_ref, key_ref), (halfside_ref, keyside_ref)))
        ]
        for copy in sends:
            copy.start()
        for copy in sends:
            copy.wait_send()
        take_pair()
        col_ref[...] = pair_ref[:, :2]

    @pl.when(panel % 2 == 1)
    def _():
        take_pair()
        await_bytes(key_ref, col_recv.at[0])
        await_bytes(keyside_ref, col_recv.at[1])
        for n in range(2):
            for r in range(2):
                col_ref[n, r] = from_levels(key_ref[n, r], keyside_ref[n, r])


def sum_diagonal(index_ref, recv_ref, side_ref, own_diag_ref, out_ref):
    count = recv_ref.shape[0]
    places = out_ref.shape[0]

    def one(s, sums):
        side = side_ref[s]
        value = from_levels(recv_ref[s], side[1:2])
        diag = side[:1]
        at = index_ref[s]
        return tuple(
            (total + jnp.where(at == r + 1, value, 0.0), line + jnp.where(at == r + 1, diag, 0.0))
            for r, (total, line) in enumerate(sums)
        )

    start = tuple(
        (jnp.zeros((HALF, BLK), F32), own_diag_ref[r : r + 1, :]) for r in range(places)
    )
    sums = lax.fori_loop(0, count, one, start, unroll=2)
    row = iota((HALF, BLK), 0)
    lane = iota((HALF, BLK), 1)
    eye = iota((BLK, BLK), 0) == iota((BLK, BLK), 1)
    for r, (folded, diag) in enumerate(sums):
        low = jnp.where(lane - HALF < row, folded, 0.0)
        high = jnp.where(
            jnp.logical_and(lane > row, lane < HALF), pltpu.roll(folded, HALF, 1), 0.0
        )
        strict = jnp.concatenate([high, low], axis=0)
        out_ref[r] = strict + strict.T + jnp.where(eye, diag, 0.0)


def sum_cross(index_ref, recv_ref, side_ref, out_ref, slot):
    count = recv_ref.shape[0]
    places = out_ref.shape[1]

    def one(s, sums):
        value = from_levels(recv_ref[s], side_ref[s])
        at = index_ref[s]
        return tuple(
            total + jnp.where(at == r + 1, value, 0.0) for r, total in enumerate(sums)
        )

    start = tuple(jnp.zeros((HALF, BLK), F32) for _ in range(places))
    sums = lax.fori_loop(0, count, one, start, unroll=2)
    for r in range(places):
        out_ref[slot, r] = sums[r]


def factor_pivot(tile_ref, p_ref, inv_ref, a_ref, b_ref, t_ref):
    step = 8
    a_ref[...] = tile_ref[...]
    b_ref[...] = jnp.where(iota((BLK, BLK), 0) == iota((BLK, BLK), 1), 1.0, 0.0)
    row = iota((BLK, BLK), 0)
    sub = iota((step, BLK), 0)
    lane = iota((step, BLK), 1)

    def group(g, carry):
        at = pl.ds(pl.multiple_of(g * step, step), step)
        a, b = a_ref[...], b_ref[...]
        rows, right = a_ref[at, :], b_ref[at, :]
        factor_rows, inverse_rows = [], []
        for s in range(step):
            pivot_row, right_row = rows[s : s + 1], right[s : s + 1]
            pivot = jnp.broadcast_to(pivot_row[:, s : s + 1], (1, BLK))
            root = 1.0 / jnp.sqrt(pivot)
            inverse = 1.0 / pivot
            factor_rows.append(pivot_row * root)
            inverse_rows.append(right_row * root)
            scaled, right_scaled = pivot_row * inverse, right_row * inverse
            near = jnp.where(sub > s, rows[:, s : s + 1], 0.0)
            far = jnp.where(row > g * step + s, a[:, s : s + 1], 0.0)
            rows, right = rows - near * scaled, right - near * right_scaled
            a, b = a - far * scaled, b - far * right_scaled
        a_ref[...] = pltpu.roll(a, BLK - step, 1)
        b_ref[...] = b
        block = jnp.concatenate(factor_rows, axis=0)
        block = jnp.where(jnp.logical_and(lane >= sub, lane < BLK - g * step), block, 0.0)
        t_ref[at, :] = pltpu.roll(block, g * step, 1)
        inv_ref[at, :] = jnp.concatenate(inverse_rows, axis=0)
        return carry

    lax.fori_loop(0, BLK // step, group, 0)
    p_ref[...] = t_ref[...].T


def final_kernel(panel_ref, diag_ref, pair_ref, col_ref, icol_ref, p_ref, inv_ref, asm_ref, fac_ref, l_ref):
    panel = panel_ref[0]
    lower = panel < 2
    other = (panel + 2) % 4
    asm_ref[...] = jnp.zeros_like(asm_ref)
    for r in range(2):
        at = pl.multiple_of((panel * 2 + r) * BLK, BLK)
        asm_ref[r * BLK : (r + 1) * BLK, pl.ds(at, BLK)] = diag_ref[r]
    for a in range(2):
        for b in range(2):
            tile = jnp.concatenate([pair_ref[0, a * 2 + b], pair_ref[1, a * 2 + b]], axis=0)
            tile = jnp.where(lower, tile, tile.T)
            row = pl.multiple_of(jnp.where(lower, a, b) * BLK, BLK)
            at = pl.multiple_of((other * 2 + jnp.where(lower, b, a)) * BLK, BLK)
            asm_ref[pl.ds(row, BLK), pl.ds(at, BLK)] = tile
    own = pl.multiple_of(panel * 2 * BLK, BLK)
    off = jnp.logical_or(panel > 0, iota((2 * BLK, BLK), 0) >= BLK)
    asm_ref[:, :BLK] = asm_ref[:, :BLK] + jnp.where(off, icol_ref[pl.ds(own, 2 * BLK), :], 0.0)
    inv_hi, inv_lo = split(inv_ref[...])
    l_ref[:BLK, :] = p_ref[...]
    for r in range(1, OWN):
        key = icol_ref[r * BLK : (r + 1) * BLK, :]
        if r in (4, 5):
            key = key + jnp.concatenate([col_ref[0, r - 4], col_ref[1, r - 4]], axis=0).T
        kh, kl = split(key)
        l_ref[r * BLK : (r + 1) * BLK, :] = mm_nt(kh, inv_hi) + (
            mm_nt(kh, inv_lo) + mm_nt(kl, inv_hi)
        )
    mine = l_ref[pl.ds(own, 2 * BLK), :]
    mh, ml = split(mine)
    fac_ref[:, :BLK] = mine
    for c in range(1, OWN):
        lh, ll = split(l_ref[c * BLK : (c + 1) * BLK, :])
        update = mm_nt(mh, lh) + (mm_nt(mh, ll) + mm_nt(ml, lh))
        fac_ref[:, c * BLK : (c + 1) * BLK] = asm_ref[:, c * BLK : (c + 1) * BLK] - jnp.where(
            off, update, 0.0
        )


def cost(flops, nbytes):
    return pl.CostEstimate(flops=flops, bytes_accessed=nbytes, transcendentals=0)


def whole(count):
    return [pl.BlockSpec(memory_space=VMEM)] * count


SMEM = pl.BlockSpec(memory_space=pltpu.SMEM)


def per_device(
    interior_factor, coupling, interface_diag, interface_column, block_map, pair_pattern
):
    subs, order, width = coupling.shape
    owners_total = lax.axis_size("sub")
    panels = lax.axis_size("panel")
    sub = lax.axis_index("sub")
    panel = lax.axis_index("panel")
    upper = (panel >= panels // 2).astype(jnp.int32)
    panel_s = panel.astype(jnp.int32).reshape(1)
    groups = width // BLK
    half_width = width // 2

    maps = block_map.reshape(owners_total, subs, panels, groups)
    owner = maps[:, :, 0, :] // OWN
    match = (owner == sub).astype(jnp.int32)
    place = maps % 2
    base = panel % 2
    own_place = lax.dynamic_index_in_dim(place, panel, 2, keepdims=False)
    low_place = lax.dynamic_index_in_dim(place, base, 2, keepdims=False)
    high_place = lax.dynamic_index_in_dim(place, base + 2, 2, keepdims=False)
    diag_index = jnp.sum(match * (1 + own_place), axis=(1, 2))
    cross_index = jnp.sum(match * (1 + 2 * low_place + high_place), axis=(1, 2))
    slots = lax.dynamic_index_in_dim(owner, sub, 0, keepdims=False).reshape(-1)
    tiles = subs * groups
    filled = (slots[None, :] == jnp.arange(owners_total, dtype=jnp.int32)[:, None]).astype(jnp.int32)
    source = tiles + jnp.sum(
        filled * (jnp.arange(tiles, dtype=jnp.int32) - tiles)[None, :], axis=1
    )
    pattern = lax.dynamic_slice_in_dim(pair_pattern, base * groups + upper * 2, 2, 1).reshape(-1)

    anywhere = pl.BlockSpec(memory_space=pl.ANY)
    dma = pltpu.SemaphoreType.DMA

    rows = OWN // panels
    diag, pivot, pivot_inverse, pair, col, columns = pl.pallas_call(
        whole_kernel,
        in_specs=[SMEM] * 4 + whole(2) + [anywhere] * 2,
        out_specs=whole(6),
        out_shape=[
            jax.ShapeDtypeStruct((rows, BLK, BLK), F32),
            jax.ShapeDtypeStruct((BLK, BLK), F32),
            jax.ShapeDtypeStruct((BLK, BLK), F32),
            jax.ShapeDtypeStruct((2, rows * rows, HALF, BLK), F32),
            jax.ShapeDtypeStruct((2, 2, HALF, BLK), F32),
            jax.ShapeDtypeStruct((OWN * BLK, BLK), F32),
        ],
        scratch_shapes=[
            VMEM((subs * order, order), F32),
            VMEM((subs, order, width), BF16),
            VMEM((subs, order, half_width), BF16),
            VMEM((subs, order, order), BF16),
            VMEM((subs, order, order), BF16),
            VMEM((subs, order, half_width), BF16),
            VMEM((subs * order // BLK * BASE, BLK), F32),
            VMEM((BASE, BASE, BLK), F32),
            VMEM((BASE, BASE, BLK), F32),
            VMEM((tiles + 1, HALF, BLK), I16),
            VMEM((tiles + 1, 2, BLK), F32),
            VMEM((owners_total, HALF, BLK), I16),
            VMEM((owners_total, 2, BLK), F32),
            VMEM((owners_total, HALF, BLK), I16),
            VMEM((owners_total, 2, BLK), F32),
            VMEM((tiles + 1, HALF, BLK), I16),
            VMEM((tiles + 1, 1, BLK), F32),
            VMEM((tiles // 2, HALF, BLK), I16),
            VMEM((tiles // 2, 1, BLK), F32),
            VMEM((owners_total, HALF, BLK), I16),
            VMEM((owners_total, 1, BLK), F32),
            VMEM((owners_total, HALF, BLK), I16),
            VMEM((owners_total, 1, BLK), F32),
            VMEM((2, rows * rows, HALF, BLK), I16),
            VMEM((2, rows * rows, 1, BLK), F32),
            VMEM((2, 2, HALF, BLK), I16),
            VMEM((2, 2, 1, BLK), F32),
            *[VMEM((BLK, BLK), F32)] * 4,
            dma((2,)),
            dma((subs,)),
            dma((subs,)),
            *[dma((2,))] * 6,
            dma((panels - 1,)),
            dma,
            dma((panels - 1,)),
            dma,
            *[dma((2,))] * 2,
            dma((4,)),
            dma((2,)),
        ],
        compiler_params=pltpu.CompilerParams(
            collective_id=1, has_side_effects=True, vmem_limit_bytes=50 * 2**20
        ),
        cost_estimate=cost(10**10, 2**24),
        name="whole",
    )(
        source, pattern, diag_index, cross_index, interface_column,
        interface_diag.reshape(rows, BLK), interior_factor.reshape(subs * order, order), coupling,
    )
    return pl.pallas_call(
        final_kernel,
        in_specs=[SMEM] + whole(6),
        out_specs=whole(2),
        out_shape=[jax.ShapeDtypeStruct((rows * BLK, OWN * BLK), F32)] * 2,
        scratch_shapes=[VMEM((OWN * BLK, BLK), F32)],
        compiler_params=pltpu.CompilerParams(vmem_limit_bytes=16 * 2**20),
        cost_estimate=cost(10**9, 2**22),
        name="final",
    )(panel_s, diag, pair, col, columns, pivot, pivot_inverse)


def solution(mesh):
    return jax.shard_map(
        per_device,
        mesh=mesh,
        in_specs=(
            P("sub", None, None),
            P("sub", None, "panel"),
            P(("sub", "panel")),
            P(("sub", "panel"), None),
            P(),
            P("sub", None),
        ),
        out_specs=(P(("sub", "panel"), None), P(("sub", "panel"), None)),
        check_vma=False,
    )
```
